128 devices in a mesh: gx: 16 (over z, y_lo, core), gy: 4 (over x), gz: 2 (over y_hi).
Axes of the slice: x: 4, y: 4 (y_hi: 2, y_lo: 2; y = y_hi * 2 + y_lo), z: 4, core: 2. Of those that a mesh axis runs over, the one named last changes fastest.
Arguments:
- models: float32 [2, 256, 128, 256], P(None, 'gx', 'gy', 'gz'), may hold values from -6 to 6
- targets: float32 [2, 256, 128, 256], P(None, 'gx', 'gy', 'gz'), may hold values from -6 to 6
- weights: float32 [2, 256, 128, 256], P(None, 'gx', 'gy', 'gz'), may hold values from 0.5 to 12, as said below
Outputs:
- updated: float32 [2, 256, 128, 256], P(None, 'gx', 'gy', 'gz')
- applied_last: float32 [2, 256, 128, 256], P(None, 'gx', 'gy', 'gz')
The draws below stay inside these ranges and needn't reach their ends.
Inputs may be any that keep to these rules, and one draw needn't show every extreme that they name: Positive data weights.
All inputs are finite; a program needn't handle non-finite values.
Results may differ from the reference program's by a relative error of at most 0.00016.
Values sent between devices are 32-bit elements; how exact they have to be, the bound alone decides.
A program may use at most 128 MiB of HBM per device.

```python
import math
import jax
import jax.numpy as jnp
from jax import lax

ITERS = 3
NX = 256
NY = 128
NZ = 256


def draw_weights(key, part):
    base_key = jax.random.fold_in(key, 11)
    base = jnp.exp(jax.random.uniform(base_key, (2, NX, NY, NZ), jnp.float32, math.log(0.5), math.log(4.0)))
    ramp = 1.0 + 2.0 * jnp.arange(NX, dtype=jnp.float32) / max(NX - 1, 1)
    return base * ramp[None, :, None, None]


def levels(stream_key, extent, shards, least, high):
    loudness, own = 1.0, jax.random.fold_in(stream_key, 6)
    for dim, parts in shards:
        heights = jnp.exp(jax.random.uniform(jax.random.fold_in(own, dim), (parts,), jnp.float32, least / len(shards), high / len(shards)))
        loudness = loudness * jnp.repeat(heights, extent[dim] // parts).reshape([-1 if axis == dim else 1 for axis in range(len(extent))])
    return loudness


def normal_values(key, shape, width, reach, shards=(), held_as=jnp.bfloat16):
    drawn = jax.random.normal(key, shape, jnp.float32) * width
    if len(shards) > 0:
        drawn = levels(key, shape, shards, -0.22, 0.18) * drawn
    return jnp.clip(drawn, min=-reach, max=reach).astype(held_as)


def setup_inputs(seed: int = 0) -> dict:
    splits = jax.random.split(jax.random.key(seed), 4)
    models = normal_values(splits[0], (2, NX, NY, NZ), 1.0, 6.0, ((1, 16), (2, 4), (3, 2)), jnp.float32)
    targets = normal_values(splits[1], (2, NX, NY, NZ), 1.0, 6.0, ((1, 16), (2, 4), (3, 2)), jnp.float32)
    weights = draw_weights(jax.random.fold_in(splits[3], 71), 0)
    return dict(models=models, targets=targets, weights=weights)


def central(field, which):
    length = field.shape[which]
    widths = [(1, 1) if k == which else (0, 0) for k in range(3)]
    padded = jnp.pad(field, widths)
    upper = lax.slice_in_dim(padded, 2, length + 2, axis=which)
    lower = lax.slice_in_dim(padded, 0, length, axis=which)
    return 0.5 * (upper - lower)


def laplace(field):
    summed = 6.0 * field
    for which in range(3):
        length = field.shape[which]
        widths = [(1, 1) if k == which else (0, 0) for k in range(3)]
        padded = jnp.pad(field, widths)
        summed = summed - lax.slice_in_dim(padded, 2, length + 2, axis=which) - lax.slice_in_dim(padded, 0, length, axis=which)
    return summed


def vector_cross(first_vec, second_vec):
    return (first_vec[1] * second_vec[2] - first_vec[2] * second_vec[1],
            first_vec[2] * second_vec[0] - first_vec[0] * second_vec[2],
            first_vec[0] * second_vec[1] - first_vec[1] * second_vec[0])


def reference(models, targets, weights):
    current = models
    applied = jnp.zeros_like(models)
    for iteration in range(ITERS):
        first_grad = [central(current[0], k) for k in range(3)]
        second_grad = [central(current[1], k) for k in range(3)]
        crossed = vector_cross(first_grad, second_grad)
        first_flux = vector_cross(second_grad, crossed)
        second_flux = vector_cross(crossed, first_grad)
        first_coupling = -2.0 * (central(first_flux[0], 0) + central(first_flux[1], 1) + central(first_flux[2], 2))
        second_coupling = -2.0 * (central(second_flux[0], 0) + central(second_flux[1], 1) + central(second_flux[2], 2))
        smooth = jnp.stack([laplace(current[0]), laplace(current[1])])
        coupling = jnp.stack([first_coupling, second_coupling])
        gradient = weights * (current - targets) + 1.0 * smooth + 0.05 * coupling
        grad_norm = jnp.sum(gradient * gradient)
        applied = weights * gradient + 1.0 * jnp.stack([laplace(gradient[0]), laplace(gradient[1])])
        curvature = jnp.sum(gradient * applied)
        current = current - (grad_norm / curvature) * gradient
    return (current, applied)
```

```python
import functools

import jax
import jax.numpy as jnp
from jax import lax
from jax.experimental import pallas as pl
from jax.experimental.pallas import tpu as pltpu
from jax.sharding import PartitionSpec as P

ITERS = 3
MESH = pl.DeviceIdType.MESH
MODELS = 2
XO = 2
YO = 8
UNROLL = 4
KAPPA = 0.05 * -2.0 * 0.5 * 0.125


def kernel(sizes, models, targets, weights, updated, applied_out,
           field, tgt, wgt, base, flux0, flux1, flux2, ghost2, near, far, far_rows,
           own1, got1, own2, got2, out_c, out_a,
           load_sem, store_sem, send_sem, recv_sem, send1, recv1, send2, recv2):
    nx, ny, nz = sizes
    _, cx, cy, cz = tgt.shape
    tiles = cy // 8
    gx, gy, gz = lax.axis_index("gx"), lax.axis_index("gy"), lax.axis_index("gz")

    offsets = [(0, 0, 1), (1, 0, 1), (-1, 0, 1), (0, 1, 1), (0, -1, 1),
               (1, 0, 0), (-1, 0, 0), (0, 1, 0), (0, -1, 0),
               (1, 1, 0), (1, -1, 0), (-1, 1, 0), (-1, -1, 0)]

    def there(ox, oy):
        ok = None
        for place, step, count in ((gx, ox, nx), (gy, oy, ny)):
            if step != 0:
                here = place < count - 1 if step > 0 else place > 0
                ok = here if ok is None else jnp.logical_and(ok, here)
        return ok

    def guarded(ok, action):
        if ok is None:
            action()
        else:
            pl.when(ok)(action)

    def face(k, ox, oy, depth):
        x_src = {1: pl.ds(XO + cx - depth, depth), -1: pl.ds(XO, depth), 0: pl.ds(XO, cx)}[ox]
        x_dst = {1: pl.ds(XO - depth, depth), -1: pl.ds(XO + cx, depth), 0: pl.ds(XO, cx)}[ox]
        y_src = {1: pl.ds(YO + cy - depth, depth), -1: pl.ds(YO, depth), 0: pl.ds(YO, cy)}[oy]
        y_dst = {1: pl.ds(YO - depth, depth), -1: pl.ds(YO + cy, depth), 0: pl.ds(YO, cy)}[oy]
        return field.at[k, x_src, :, y_src, :], field.at[k, x_dst, :, y_dst, :]

    def message(k, j, last):
        ox, oy, oz = offsets[j]
        if oz:
            src, dst = near.at[k], far.at[k, j]
        else:
            depth = 1 if last or (ox and oy) else 2
            src, dst = face(k, ox, oy, depth)
        return pltpu.make_async_remote_copy(
            src_ref=src, dst_ref=dst, send_sem=send_sem.at[k, j], recv_sem=recv_sem.at[k, j],
            device_id={"gx": gx + ox, "gy": gy + oy, "gz": gz + oz - 2 * oz * gz}, device_id_type=MESH)

    def used(last):
        return [j for j, (ox, oy, oz) in enumerate(offsets) if not last or abs(ox) + abs(oy) + oz == 1]

    def start_exchange(k, last=False):
        for j in used(last):
            guarded(there(offsets[j][0], offsets[j][1]), lambda j=j: message(k, j, last).start())

    def wait_exchange(k, last=False):
        for j in used(last):
            guarded(there(-offsets[j][0], -offsets[j][1]), lambda j=j: message(k, j, last).wait_recv())

    def wait_sends(k, last=False):
        for j in used(last):
            guarded(there(offsets[j][0], offsets[j][1]), lambda j=j: message(k, j, last).wait_send())

    group1 = [(c, s) for s in range(ny) for c in range(2) if (c, s) != (0, 0)]
    group2 = [(h, s) for s in range(nz) for h in range(nx // 2) if (h, s) != (0, 0)]

    def peer1(j):
        c, s = group1[j]
        core = lax.rem(gx, 2)
        return {"gx": gx + c - 2 * c * core, "gy": lax.rem(gy + s, ny), "gz": gz}

    def peer2(j):
        h, s = group2[j]
        return {"gx": lax.rem(gx + 2 * h, nx), "gy": gy, "gz": gz + s - 2 * s * gz}

    def stage(k, peers, peer, own, got, sends, recvs):
        return [pltpu.make_async_remote_copy(
            src_ref=own.at[k], dst_ref=got.at[k, j], send_sem=sends.at[k, j], recv_sem=recvs.at[k, j],
            device_id=peer(j), device_id_type=MESH) for j in range(len(peers))]

    loads = []
    for m in range(MODELS):
        loads.append(pltpu.make_async_copy(models.at[m], field.at[0, pl.ds(XO, cx), m, pl.ds(YO, cy), :], load_sem.at[m]))
    loads.append(pltpu.make_async_copy(targets, tgt, load_sem.at[2]))
    loads.append(pltpu.make_async_copy(weights, wgt, load_sem.at[3]))
    for copy in loads:
        copy.start()

    zero = jnp.zeros((8, cz), jnp.float32)
    rows = field.shape[3]

    def clear_planes(start):
        for k in range(ITERS + 1):
            for x in range(start, start + XO):
                for m in range(MODELS):
                    for r in range(0, rows, 8):
                        field[k, x, m, pl.ds(r, 8), :] = zero

    def clear_rows(start):
        def clear(x, _):
            for k in range(ITERS + 1):
                for m in range(MODELS):
                    field[k, x, m, pl.ds(start, 8), :] = zero
            return 0

        lax.fori_loop(0, cx + 2 * XO, clear, 0)

    def clear_far(j):
        for k in range(ITERS + 1):
            for m in range(MODELS):
                far[k, j, m] = zero

    pl.when(gx == 0)(lambda: (clear_planes(0), clear_far(1))[0])
    pl.when(gx == nx - 1)(lambda: (clear_planes(XO + cx), clear_far(2))[0])
    pl.when(gy == 0)(lambda: (clear_rows(0), clear_far(3))[0])
    pl.when(gy == ny - 1)(lambda: (clear_rows(rows - 8), clear_far(4))[0])

    barrier = pltpu.get_barrier_semaphore()
    expected = len(group1) + len(group2)
    for ox, oy, oz in offsets:
        ok = there(ox, oy)
        guarded(ok, lambda ox=ox, oy=oy, oz=oz: pl.semaphore_signal(
            barrier, 1, device_id={"gx": gx + ox, "gy": gy + oy, "gz": gz + oz - 2 * oz * gz}, device_id_type=MESH))
        expected = expected + (1 if ok is None else ok.astype(jnp.int32))
    for j in range(len(group1)):
        pl.semaphore_signal(barrier, 1, device_id=peer1(j), device_id_type=MESH)
    for j in range(len(group2)):
        pl.semaphore_signal(barrier, 1, device_id=peer2(j), device_id_type=MESH)


    lane = lax.broadcasted_iota(jnp.int32, (8, cz), 1)
    row = lax.broadcasted_iota(jnp.int32, (8, cz), 0)
    first, last_lane = lane == 0, lane == cz - 1
    ghost_lane = lane == jnp.where(gz == 0, 0, cz - 1)

    def turn(v, shift):
        if isinstance(shift, int):
            shift = shift % cz
            return v if shift == 0 else pltpu.roll(v, shift, 1)
        return pltpu.roll(v, shift, 1)

    def edge(packed, at):
        back = (2 * cz - at - 2 * gz) % cz if not isinstance(at, int) else lax.rem(2 * cz - at - 2 * gz, cz)
        return jnp.where(ghost_lane, turn(packed, back), 0.0)

    def z_pair(v, e):
        return turn(jnp.where(first, e, v), cz - 1), turn(jnp.where(last_lane, e, v), 1)

    def pack(acc, v, t, x):
        put = lax.rem(2 * cx * t + 2 * x + 2 - 2 * gz, cz)
        return jnp.where(lax.div(lane, 2) == cx * t + x, turn(v, put), acc)

    def at(k, x, m, r):
        return field[k, x + XO, m, pl.ds(YO + r, 8), :]

    def over_x(body, carry):
        def block(b, carry):
            for u in range(UNROLL):
                carry = body(b * UNROLL + u, carry)
            return carry

        return lax.fori_loop(0, cx // UNROLL, block, carry)

    def cross_part(a, b, i):
        j, l = (i + 1) % 3, (i + 2) % 3
        return a[j] * b[l] - a[l] * b[j]

    def flux_part(g1, g2, which):
        crossed = [None, None, None]
        for i in range(3):
            if which is None or i != which:
                crossed[i] = cross_part(g1, g2, i)
        parts = range(3) if which is None else [which]
        return [(cross_part(g2, crossed, i), cross_part(crossed, g1, i)) for i in parts]

    for copy in loads[:MODELS]:
        copy.wait()
    empty = (zero,) * MODELS

    def pack_plane(x, acc):
        acc = list(acc)
        for m in range(MODELS):
            for t in range(tiles):
                acc[m] = pack(acc[m], at(0, x, m, 8 * t), t, x)
        return tuple(acc)

    packed = over_x(pack_plane, empty)
    for m in range(MODELS):
        near[0, m] = packed[m]
    pl.semaphore_wait(barrier, expected)
    start_exchange(0)
    for copy in loads[MODELS:]:
        copy.wait()
    wait_exchange(0)

    for k in range(1, ITERS + 1):
        final = k == ITERS
        for x, keep, j in ((-1, gx > 0, 1), (cx, gx < nx - 1, 2)):
            for t in range(tiles):
                grads = []
                for m in range(MODELS):
                    up, down = z_pair(at(0, x, m, 8 * t), edge(far[0, j, m], 2 * cx * t + (2 * cx - 2 if x < 0 else 0)))
                    grads.append([at(0, x + 1, m, 8 * t) - at(0, x - 1, m, 8 * t),
                                  at(0, x, m, 8 * t + 1) - at(0, x, m, 8 * t - 1), up - down])
                parts = flux_part(grads[0], grads[1], 0)[0]
                for m in range(MODELS):
                    flux0[x + 1, m, pl.ds(8 * t, 8), :] = jnp.where(keep, parts[m], 0.0)

        top = row == 0
        for m in range(MODELS):
            below = turn(far[0, 3, m], 2 * cx)
            for t in range(tiles):
                tile = jnp.where(lane < 2 * cx, turn(far[0, 0, m], -2 * cx * t),
                                 jnp.where(lane < 4 * cx, turn(far[0, 2, m], 2 * cx - 2 * cx * t),
                                           turn(far[0, 1, m], -2 * cx * t - 2 * cx)))
                far_rows[m, pl.ds(YO + 8 * t, 8), :] = tile
            far_rows[m, pl.ds(YO - 1, 1), :] = below[7:8]
            far_rows[m, pl.ds(YO + cy, 1), :] = far[0, 4, m][0:1]

        sign = (1 - 2 * gz).astype(jnp.float32)
        for t in range(tiles):
            grads = []
            for m in range(MODELS):
                here = far_rows[m, pl.ds(YO + 8 * t, 8), :]
                inner = turn(near[0, m], -2 * cx * t)
                grads.append([turn(here, -2) - turn(here, 2),
                              far_rows[m, pl.ds(YO + 8 * t + 1, 8), :] - far_rows[m, pl.ds(YO + 8 * t - 1, 8), :],
                              sign * turn(here - inner, jnp.where(gz == 0, cz - 1, 1))])
            parts = flux_part(grads[0], grads[1], 2)[0]
            for m in range(MODELS):
                ghost2[m, pl.ds(8 * t, 8), :] = parts[m]

        beside = [jnp.where(top, far_rows[m, pl.ds(YO - 1, 8), :],
                            far_rows[m, pl.ds(YO + cy - 1, 8), :]) for m in range(MODELS)]
        keep_low, keep_high = gy > 0, gy < ny - 1

        def fluxes(x, carry):
            def ends(dx, m, dy):
                return jnp.where(top, at(0, x + dx, m, dy - 1), at(0, x + dx, m, cy - 1 + dy))

            grads = []
            for m in range(MODELS):
                up, down = z_pair(ends(0, m, 0), edge(beside[m], 2 * x))
                grads.append([ends(1, m, 0) - ends(-1, m, 0), ends(0, m, 1) - ends(0, m, -1), up - down])
            parts = flux_part(grads[0], grads[1], 1)[0]
            for m in range(MODELS):
                flux1[x, m, pl.ds(YO - 1, 1), :] = jnp.where(keep_low, parts[m][0:1], 0.0)
                flux1[x, m, pl.ds(YO + cy, 1), :] = jnp.where(keep_high, parts[m][1:2], 0.0)
            for t in range(tiles):
                grads = []
                for m in range(MODELS):
                    here = at(0, x, m, 8 * t)
                    up, down = z_pair(here, edge(far[0, 0, m], 2 * cx * t + 2 * x))
                    xp, xm = at(0, x + 1, m, 8 * t), at(0, x - 1, m, 8 * t)
                    yp, ym = at(0, x, m, 8 * t + 1), at(0, x, m, 8 * t - 1)
                    grads.append([xp - xm, yp - ym, up - down])
                    smooth = 6.0 * here - ((xp + xm) + (yp + ym) + (up + down))
                    misfit = wgt[m, x, pl.ds(8 * t, 8), :] * (here - tgt[m, x, pl.ds(8 * t, 8), :])
                    base[m, x, pl.ds(8 * t, 8), :] = misfit + smooth
                parts = flux_part(grads[0], grads[1], None)
                for m in range(MODELS):
                    flux0[x + 1, m, pl.ds(8 * t, 8), :] = parts[0][m]
                    flux1[x, m, pl.ds(YO + 8 * t, 8), :] = parts[1][m]
                    flux2[x, m, pl.ds(8 * t, 8), :] = parts[2][m]
            return carry

        over_x(fluxes, 0)

        def gradients(x, carry):
            norm, acc = carry[0], list(carry[1:])
            for t in range(tiles):
                for m in range(MODELS):
                    here = flux2[x, m, pl.ds(8 * t, 8), :]
                    up, down = z_pair(here, edge(ghost2[m, pl.ds(8 * t, 8), :], 2 * x))
                    div = (flux0[x + 2, m, pl.ds(8 * t, 8), :] - flux0[x, m, pl.ds(8 * t, 8), :]
                           + (flux1[x, m, pl.ds(YO + 8 * t + 1, 8), :] - flux1[x, m, pl.ds(YO + 8 * t - 1, 8), :])
                           + (up - down))
                    grad = base[m, x, pl.ds(8 * t, 8), :] + KAPPA * div
                    field[k, x + XO, m, pl.ds(YO + 8 * t, 8), :] = grad
                    norm = norm + grad * grad
                    acc[m] = pack(acc[m], grad, t, x)
            return (norm, *acc)

        norm, *packed = over_x(gradients, (zero, *empty))
        for m in range(MODELS):
            near[k, m] = packed[m]
        start_exchange(k, final)
        wait_exchange(k, final)

        def applies(x, curve):
            for t in range(tiles):
                for m in range(MODELS):
                    here = at(k, x, m, 8 * t)
                    up, down = z_pair(here, edge(far[k, 0, m], 2 * cx * t + 2 * x))
                    around = ((at(k, x + 1, m, 8 * t) + at(k, x - 1, m, 8 * t))
                              + (at(k, x, m, 8 * t + 1) + at(k, x, m, 8 * t - 1)) + (up + down))
                    applied = wgt[m, x, pl.ds(8 * t, 8), :] * here + (6.0 * here - around)
                    curve = curve + here * applied
                    if final:
                        out_a[m, x, pl.ds(8 * t, 8), :] = applied
            return curve

        curve = over_x(applies, zero)
        if final:
            store_a = pltpu.make_async_copy(out_a, applied_out, store_sem.at[0])
            store_a.start()

        def fold(v):
            return jnp.sum(v, axis=0, keepdims=True)

        own1[k - 1, pl.ds(0, 1), :] = fold(norm)
        own1[k - 1, pl.ds(1, 1), :] = fold(curve)
        copies1 = stage(k - 1, group1, peer1, own1, got1, send1, recv1)
        for copy in copies1:
            copy.start()
        total = own1[k - 1]
        for j, copy in enumerate(copies1):
            copy.wait_recv()
            total = total + got1[k - 1, j]
        own2[k - 1] = total
        copies2 = stage(k - 1, group2, peer2, own2, got2, send2, recv2)
        for copy in copies2:
            copy.start()
        for j, copy in enumerate(copies2):
            copy.wait_recv()
            total = total + got2[k - 1, j]
        sums = jnp.sum(total, axis=1, keepdims=True)
        alpha = jnp.broadcast_to(sums[0:1] / sums[1:2], (8, cz))

        if k == 1:
            wait_sends(0)
        wait_sends(k, final)
        for copy in copies1 + copies2:
            copy.wait_send()

        if final:
            def step(x, carry):
                for m in range(MODELS):
                    for t in range(tiles):
                        out_c[m, x, pl.ds(8 * t, 8), :] = at(0, x, m, 8 * t) - alpha * at(k, x, m, 8 * t)
                return carry

            over_x(step, 0)
        else:
            def step(x, carry):
                for m in range(MODELS):
                    for r in range(0, rows, 8):
                        field[0, x, m, pl.ds(r, 8), :] = (
                            field[0, x, m, pl.ds(r, 8), :] - alpha * field[k, x, m, pl.ds(r, 8), :])
                return carry

            lax.fori_loop(0, cx + 2 * XO, step, 0)
            for m in range(MODELS):
                near[0, m] = near[0, m] - alpha * near[k, m]
                for j in range(5):
                    far[0, j, m] = far[0, j, m] - alpha * far[k, j, m]

    store_c = pltpu.make_async_copy(out_c, updated, store_sem.at[1])
    store_c.start()
    store_a.wait()
    store_c.wait()


def solution(mesh):
    sizes = (mesh.shape["gx"], mesh.shape["gy"], mesh.shape["gz"])
    nx, ny, nz = sizes

    def local(models, targets, weights):
        _, cx, cy, cz = models.shape
        assert nz == 2 and nx % 2 == 0 and 2 * cx * (cy // 8) == cz
        f32 = jnp.float32
        block = (MODELS, cx, cy, cz)
        rows = YO + cy + 8
        peers1, peers2 = 2 * ny - 1, nx // 2 * nz - 1
        return pl.pallas_call(
            functools.partial(kernel, sizes),
            out_shape=[jax.ShapeDtypeStruct(models.shape, f32)] * 2,
            in_specs=[pl.BlockSpec(memory_space=pl.ANY)] * 3,
            out_specs=[pl.BlockSpec(memory_space=pl.ANY)] * 2,
            scratch_shapes=[
                pltpu.VMEM((ITERS + 1, cx + 2 * XO, MODELS, rows, cz), f32),
                pltpu.VMEM(block, f32),
                pltpu.VMEM(block, f32),
                pltpu.VMEM(block, f32),
                pltpu.VMEM((cx + 2, MODELS, cy, cz), f32),
                pltpu.VMEM((cx, MODELS, rows, cz), f32),
                pltpu.VMEM((cx, MODELS, cy, cz), f32),
                pltpu.VMEM((MODELS, cy, cz), f32),
                pltpu.VMEM((ITERS + 1, MODELS, 8, cz), f32),
                pltpu.VMEM((ITERS + 1, 5, MODELS, 8, cz), f32),
                pltpu.VMEM((MODELS, rows, cz), f32),
                pltpu.VMEM((ITERS, 2, cz), f32),
                pltpu.VMEM((ITERS, peers1, 2, cz), f32),
                pltpu.VMEM((ITERS, 2, cz), f32),
                pltpu.VMEM((ITERS, peers2, 2, cz), f32),
                pltpu.VMEM(block, f32),
                pltpu.VMEM(block, f32),
                pltpu.SemaphoreType.DMA((4,)),
                pltpu.SemaphoreType.DMA((2,)),
                pltpu.SemaphoreType.DMA((ITERS + 1, 13)),
                pltpu.SemaphoreType.DMA((ITERS + 1, 13)),
                pltpu.SemaphoreType.DMA((ITERS, peers1)),
                pltpu.SemaphoreType.DMA((ITERS, peers1)),
                pltpu.SemaphoreType.DMA((ITERS, peers2)),
                pltpu.SemaphoreType.DMA((ITERS, peers2)),
            ],
            compiler_params=pltpu.CompilerParams(
                collective_id=0, has_side_effects=True, vmem_limit_bytes=60 * 2**20),
        )(models, targets, weights)

    spec = P(None, "gx", "gy", "gz")
    return jax.shard_map(local, mesh=mesh, in_specs=(spec,) * 3, out_specs=(spec,) * 2, check_vma=False)
```

```python
import functools

import jax
import jax.numpy as jnp
from jax import lax
from jax.experimental import pallas as pl
from jax.experimental.pallas import tpu as pltpu
from jax.sharding import PartitionSpec as P

ITERS = 3
MESH = pl.DeviceIdType.MESH
MODELS = 2
XO = 2
YO = 8
UNROLL = 4
KAPPA = 0.05 * -2.0 * 0.5 * 0.125


def kernel(sizes, models, targets, weights, updated, applied_out,
           field, tgt, wgt, base, flux0, flux1, flux2, ghost2, near, far, far_rows,
           own, got,
           load_sem, send_sem, recv_sem, sum_send, sum_recv, enter_sem):
    nx, ny, nz = sizes
    _, cx, cy, cz = tgt.shape
    tiles = cy // 8
    gx, gy, gz = lax.axis_index("gx"), lax.axis_index("gy"), lax.axis_index("gz")

    offsets = [(0, 0, 1), (1, 0, 1), (-1, 0, 1), (0, 1, 1), (0, -1, 1),
               (1, 0, 0), (-1, 0, 0), (0, 1, 0), (0, -1, 0),
               (1, 1, 0), (1, -1, 0), (-1, 1, 0), (-1, -1, 0)]

    def there(ox, oy):
        ok = None
        for place, step, count in ((gx, ox, nx), (gy, oy, ny)):
            if step != 0:
                here = place < count - 1 if step > 0 else place > 0
                ok = here if ok is None else jnp.logical_and(ok, here)
        return ok

    def guarded(ok, action):
        if ok is None:
            action()
        else:
            pl.when(ok)(action)

    def face(k, ox, oy, depth):
        x_src = {1: pl.ds(XO + cx - depth, depth), -1: pl.ds(XO, depth), 0: pl.ds(XO, cx)}[ox]
        x_dst = {1: pl.ds(XO - depth, depth), -1: pl.ds(XO + cx, depth), 0: pl.ds(XO, cx)}[ox]
        y_src = {1: pl.ds(YO + cy - depth, depth), -1: pl.ds(YO, depth), 0: pl.ds(YO, cy)}[oy]
        y_dst = {1: pl.ds(YO - depth, depth), -1: pl.ds(YO + cy, depth), 0: pl.ds(YO, cy)}[oy]
        return field.at[k, x_src, :, y_src, :], field.at[k, x_dst, :, y_dst, :]

    def message(k, j, last):
        ox, oy, oz = offsets[j]
        if oz:
            src, dst = near.at[k], far.at[k, j]
        else:
            depth = 1 if last or (ox and oy) else 2
            src, dst = face(k, ox, oy, depth)
        return pltpu.make_async_remote_copy(
            src_ref=src, dst_ref=dst, send_sem=send_sem.at[k, j], recv_sem=recv_sem.at[k, j],
            device_id={"gx": gx + ox, "gy": gy + oy, "gz": gz + oz - 2 * oz * gz}, device_id_type=MESH)

    def used(last):
        return [j for j, (ox, oy, oz) in enumerate(offsets) if not last or abs(ox) + abs(oy) + oz == 1]

    def start_exchange(k, last=False):
        for j in used(last):
            guarded(there(offsets[j][0], offsets[j][1]), lambda j=j: message(k, j, last).start())

    def wait_exchange(k, last=False):
        for j in used(last):
            guarded(there(-offsets[j][0], -offsets[j][1]), lambda j=j: message(k, j, last).wait_recv())

    def wait_sends(k, last=False):
        for j in used(last):
            guarded(there(offsets[j][0], offsets[j][1]), lambda j=j: message(k, j, last).wait_send())

    others = [(x, y, z) for z in range(nz) for y in range(ny) for x in range(nx) if (x, y, z) != (0, 0, 0)]

    def peer(x, y, z):
        return {"gx": lax.rem(gx + x, nx) if x else gx, "gy": lax.rem(gy + y, ny) if y else gy,
                "gz": lax.rem(gz + z, nz) if z else gz}

    def start_sum(k):
        for j, offset in enumerate(others):
            pltpu.make_async_remote_copy(
                src_ref=own.at[k], dst_ref=got.at[k, j], send_sem=sum_send.at[k], recv_sem=sum_recv.at[k],
                device_id=peer(*offset), device_id_type=MESH).start()

    def whole_sum(k):
        return pltpu.make_async_remote_copy(
            src_ref=got.at[k], dst_ref=got.at[k], send_sem=sum_send.at[k], recv_sem=sum_recv.at[k],
            device_id=peer(1, 0, 0), device_id_type=MESH)

    def on_line(x, y, z):
        return {"gx": x, "gy": y, "gz": z}

    pair, quad, chip_z = lax.rem(gx, 2), lax.rem(lax.div(gx, 2), 2), lax.div(gx, 4)
    line_x = [on_line(gx + c - 2 * c * pair, lax.rem(gy + s, ny), gz)
              for s in range(ny) for c in range(2) if (c, s) != (0, 0)]
    line_y = [on_line(gx + 2 * h - 4 * h * quad, gy, gz + s - 2 * s * gz)
              for s in range(nz) for h in range(2) if (h, s) != (0, 0)]
    line_z = [on_line(lax.rem(gx + 4 * s, nx), gy, gz) for s in range(1, nx // 4)]

    def tell(sem, line):
        for device in line:
            pl.semaphore_signal(sem, 1, device_id=device, device_id_type=MESH)

    loads = []
    for m in range(MODELS):
        loads.append(pltpu.make_async_copy(models.at[m], field.at[0, pl.ds(XO, cx), m, pl.ds(YO, cy), :], load_sem.at[m]))
    loads.append(pltpu.make_async_copy(targets, tgt, load_sem.at[2]))
    loads.append(pltpu.make_async_copy(weights, wgt, load_sem.at[3]))
    for copy in loads:
        copy.start()

    zero = jnp.zeros((8, cz), jnp.float32)
    rows = field.shape[3]

    def clear_planes(start):
        for k in range(ITERS + 1):
            for x in range(start, start + XO):
                for m in range(MODELS):
                    for r in range(0, rows, 8):
                        field[k, x, m, pl.ds(r, 8), :] = zero

    def clear_rows(start):
        def clear(x, _):
            for k in range(ITERS + 1):
                for m in range(MODELS):
                    field[k, x, m, pl.ds(start, 8), :] = zero
            return 0

        lax.fori_loop(0, cx + 2 * XO, clear, 0)

    def clear_far(j):
        for k in range(ITERS + 1):
            for m in range(MODELS):
                far[k, j, m] = zero

    pl.when(gx == 0)(lambda: (clear_planes(0), clear_far(1))[0])
    pl.when(gx == nx - 1)(lambda: (clear_planes(XO + cx), clear_far(2))[0])
    pl.when(gy == 0)(lambda: (clear_rows(0), clear_far(3))[0])
    pl.when(gy == ny - 1)(lambda: (clear_rows(rows - 8), clear_far(4))[0])

    barrier = pltpu.get_barrier_semaphore()
    expected = len(line_x) + len(line_y) + len(line_z)
    for ox, oy, oz in offsets:
        ok = there(ox, oy)
        guarded(ok, lambda ox=ox, oy=oy, oz=oz: pl.semaphore_signal(
            barrier, 1, device_id={"gx": gx + ox, "gy": gy + oy, "gz": gz + oz - 2 * oz * gz}, device_id_type=MESH))
        expected = expected + (1 if ok is None else ok.astype(jnp.int32))
    for line in (line_x, line_y, line_z):
        tell(barrier, line)

    lane = lax.broadcasted_iota(jnp.int32, (8, cz), 1)
    row = lax.broadcasted_iota(jnp.int32, (8, cz), 0)
    first, last_lane = lane == 0, lane == cz - 1
    ghost_lane = lane == jnp.where(gz == 0, 0, cz - 1)

    def turn(v, shift):
        if isinstance(shift, int):
            shift = shift % cz
            return v if shift == 0 else pltpu.roll(v, shift, 1)
        return pltpu.roll(v, shift, 1)

    def edge(packed, at):
        back = (2 * cz - at - 2 * gz) % cz if not isinstance(at, int) else lax.rem(2 * cz - at - 2 * gz, cz)
        return jnp.where(ghost_lane, turn(packed, back), 0.0)

    def z_pair(v, e):
        return turn(jnp.where(first, e, v), cz - 1), turn(jnp.where(last_lane, e, v), 1)

    def pack(acc, v, t, x):
        put = lax.rem(2 * cx * t + 2 * x + 2 - 2 * gz, cz)
        return jnp.where(lax.div(lane, 2) == cx * t + x, turn(v, put), acc)

    def at(k, x, m, r):
        return field[k, x + XO, m, pl.ds(YO + r, 8), :]

    def over_x(body, carry):
        def block(b, carry):
            for u in range(UNROLL):
                carry = body(b * UNROLL + u, carry)
            return carry

        return lax.fori_loop(0, cx // UNROLL, block, carry)

    def cross_part(a, b, i):
        j, l = (i + 1) % 3, (i + 2) % 3
        return a[j] * b[l] - a[l] * b[j]

    def flux_part(g1, g2, which):
        crossed = [None, None, None]
        for i in range(3):
            if which is None or i != which:
                crossed[i] = cross_part(g1, g2, i)
        parts = range(3) if which is None else [which]
        return [(cross_part(g2, crossed, i), cross_part(crossed, g1, i)) for i in parts]

    for copy in loads[:MODELS]:
        copy.wait()
    empty = (zero,) * MODELS

    def pack_plane(x, acc):
        acc = list(acc)
        for m in range(MODELS):
            for t in range(tiles):
                acc[m] = pack(acc[m], at(0, x, m, 8 * t), t, x)
        return tuple(acc)

    packed = over_x(pack_plane, empty)
    for m in range(MODELS):
        near[0, m] = packed[m]
    pl.semaphore_wait(barrier, expected)
    start_exchange(0)
    tell(enter_sem.at[0], line_y)
    for copy in loads[MODELS:]:
        copy.wait()
    wait_exchange(0)
    pl.semaphore_wait(enter_sem.at[0], len(line_y))
    tell(enter_sem.at[1], line_z)

    for k in range(1, ITERS + 1):
        final = k == ITERS
        for x, keep, j in ((-1, gx > 0, 1), (cx, gx < nx - 1, 2)):
            for t in range(tiles):
                grads = []
                for m in range(MODELS):
                    up, down = z_pair(at(0, x, m, 8 * t), edge(far[0, j, m], 2 * cx * t + (2 * cx - 2 if x < 0 else 0)))
                    grads.append([at(0, x + 1, m, 8 * t) - at(0, x - 1, m, 8 * t),
                                  at(0, x, m, 8 * t + 1) - at(0, x, m, 8 * t - 1), up - down])
                parts = flux_part(grads[0], grads[1], 0)[0]
                for m in range(MODELS):
                    flux0[x + 1, m, pl.ds(8 * t, 8), :] = jnp.where(keep, parts[m], 0.0)

        top = row == 0
        for m in range(MODELS):
            below = turn(far[0, 3, m], 2 * cx)
            for t in range(tiles):
                tile = jnp.where(lane < 2 * cx, turn(far[0, 0, m], -2 * cx * t),
                                 jnp.where(lane < 4 * cx, turn(far[0, 2, m], 2 * cx - 2 * cx * t),
                                           turn(far[0, 1, m], -2 * cx * t - 2 * cx)))
                far_rows[m, pl.ds(YO + 8 * t, 8), :] = tile
            far_rows[m, pl.ds(YO - 1, 1), :] = below[7:8]
            far_rows[m, pl.ds(YO + cy, 1), :] = far[0, 4, m][0:1]

        sign = (1 - 2 * gz).astype(jnp.float32)
        for t in range(tiles):
            grads = []
            for m in range(MODELS):
                here = far_rows[m, pl.ds(YO + 8 * t, 8), :]
                inner = turn(near[0, m], -2 * cx * t)
                grads.append([turn(here, -2) - turn(here, 2),
                              far_rows[m, pl.ds(YO + 8 * t + 1, 8), :] - far_rows[m, pl.ds(YO + 8 * t - 1, 8), :],
                              sign * turn(here - inner, jnp.where(gz == 0, cz - 1, 1))])
            parts = flux_part(grads[0], grads[1], 2)[0]
            for m in range(MODELS):
                ghost2[m, pl.ds(8 * t, 8), :] = parts[m]

        beside = [jnp.where(top, far_rows[m, pl.ds(YO - 1, 8), :],
                            far_rows[m, pl.ds(YO + cy - 1, 8), :]) for m in range(MODELS)]
        keep_low, keep_high = gy > 0, gy < ny - 1

        def fluxes(x, carry):
            def ends(dx, m, dy):
                return jnp.where(top, at(0, x + dx, m, dy - 1), at(0, x + dx, m, cy - 1 + dy))

            grads = []
            for m in range(MODELS):
                up, down = z_pair(ends(0, m, 0), edge(beside[m], 2 * x))
                grads.append([ends(1, m, 0) - ends(-1, m, 0), ends(0, m, 1) - ends(0, m, -1), up - down])
            parts = flux_part(grads[0], grads[1], 1)[0]
            for m in range(MODELS):
                flux1[x, m, pl.ds(YO - 1, 1), :] = jnp.where(keep_low, parts[m][0:1], 0.0)
                flux1[x, m, pl.ds(YO + cy, 1), :] = jnp.where(keep_high, parts[m][1:2], 0.0)
            for t in range(tiles):
                grads = []
                for m in range(MODELS):
                    here = at(0, x, m, 8 * t)
                    up, down = z_pair(here, edge(far[0, 0, m], 2 * cx * t + 2 * x))
                    xp, xm = at(0, x + 1, m, 8 * t), at(0, x - 1, m, 8 * t)
                    yp, ym = at(0, x, m, 8 * t + 1), at(0, x, m, 8 * t - 1)
                    grads.append([xp - xm, yp - ym, up - down])
                    smooth = 6.0 * here - ((xp + xm) + (yp + ym) + (up + down))
                    misfit = wgt[m, x, pl.ds(8 * t, 8), :] * (here - tgt[m, x, pl.ds(8 * t, 8), :])
                    base[m, x, pl.ds(8 * t, 8), :] = misfit + smooth
                parts = flux_part(grads[0], grads[1], None)
                for m in range(MODELS):
                    flux0[x + 1, m, pl.ds(8 * t, 8), :] = parts[0][m]
                    flux1[x, m, pl.ds(YO + 8 * t, 8), :] = parts[1][m]
                    flux2[x, m, pl.ds(8 * t, 8), :] = parts[2][m]
            return carry

        over_x(fluxes, 0)

        def gradients(x, carry):
            norm, acc = carry[0], list(carry[1:])
            for t in range(tiles):
                for m in range(MODELS):
                    here = flux2[x, m, pl.ds(8 * t, 8), :]
                    up, down = z_pair(here, edge(ghost2[m, pl.ds(8 * t, 8), :], 2 * x))
                    div = (flux0[x + 2, m, pl.ds(8 * t, 8), :] - flux0[x, m, pl.ds(8 * t, 8), :]
                           + (flux1[x, m, pl.ds(YO + 8 * t + 1, 8), :] - flux1[x, m, pl.ds(YO + 8 * t - 1, 8), :])
                           + (up - down))
                    grad = base[m, x, pl.ds(8 * t, 8), :] + KAPPA * div
                    field[k, x + XO, m, pl.ds(YO + 8 * t, 8), :] = grad
                    norm = norm + grad * grad
                    acc[m] = pack(acc[m], grad, t, x)
            return (norm, *acc)

        norm, *packed = over_x(gradients, (zero, *empty))
        for m in range(MODELS):
            near[k, m] = packed[m]
        start_exchange(k, final)
        wait_exchange(k, final)

        def applies(x, curve):
            for t in range(tiles):
                for m in range(MODELS):
                    here = at(k, x, m, 8 * t)
                    up, down = z_pair(here, edge(far[k, 0, m], 2 * cx * t + 2 * x))
                    around = ((at(k, x + 1, m, 8 * t) + at(k, x - 1, m, 8 * t))
                              + (at(k, x, m, 8 * t + 1) + at(k, x, m, 8 * t - 1)) + (up + down))
                    applied = wgt[m, x, pl.ds(8 * t, 8), :] * here + (6.0 * here - around)
                    curve = curve + here * applied
                    if final:
                        applied_out[m, x, pl.ds(8 * t, 8), :] = applied
            return curve

        curve = over_x(applies, zero)

        def fold(v):
            return jnp.sum(v, axis=0, keepdims=True)

        own[k - 1, pl.ds(0, 1), :] = fold(norm)
        own[k - 1, pl.ds(1, 1), :] = fold(curve)
        if k == 1:
            pl.semaphore_wait(enter_sem.at[1], len(line_z))
        start_sum(k - 1)
        whole_sum(k - 1).wait_recv()
        partial = [own[k - 1]] + [got[k - 1, j] for j in range(len(others))]
        while len(partial) > 1:
            partial = [sum(partial[i:i + 2]) for i in range(0, len(partial), 2)]
        total = partial[0]
        sums = jnp.sum(total, axis=1, keepdims=True)
        alpha = jnp.broadcast_to(sums[0:1] / sums[1:2], (8, cz))

        if k == 1:
            wait_sends(0)
        wait_sends(k, final)
        whole_sum(k - 1).wait_send()

        if final:
            def step(x, carry):
                for m in range(MODELS):
                    for t in range(tiles):
                        updated[m, x, pl.ds(8 * t, 8), :] = at(0, x, m, 8 * t) - alpha * at(k, x, m, 8 * t)
                return carry

            over_x(step, 0)
        else:
            def step(x, carry):
                for m in range(MODELS):
                    for r in range(0, rows, 8):
                        field[0, x, m, pl.ds(r, 8), :] = (
                            field[0, x, m, pl.ds(r, 8), :] - alpha * field[k, x, m, pl.ds(r, 8), :])
                return carry

            lax.fori_loop(0, cx + 2 * XO, step, 0)
            for m in range(MODELS):
                near[0, m] = near[0, m] - alpha * near[k, m]
                for j in range(5):
                    far[0, j, m] = far[0, j, m] - alpha * far[k, j, m]


def solution(mesh):
    sizes = (mesh.shape["gx"], mesh.shape["gy"], mesh.shape["gz"])
    nx, ny, nz = sizes

    def local(models, targets, weights):
        _, cx, cy, cz = models.shape
        assert nz == 2 and nx % 4 == 0 and 2 * cx * (cy // 8) == cz
        f32 = jnp.float32
        block = (MODELS, cx, cy, cz)
        rows = YO + cy + 8
        others = nx * ny * nz - 1
        return pl.pallas_call(
            functools.partial(kernel, sizes),
            out_shape=[jax.ShapeDtypeStruct(models.shape, f32)] * 2,
            in_specs=[pl.BlockSpec(memory_space=pltpu.HBM)] * 3,
            out_specs=[pl.BlockSpec(memory_space=pltpu.VMEM)] * 2,
            scratch_shapes=[
                pltpu.VMEM((ITERS + 1, cx + 2 * XO, MODELS, rows, cz), f32),
                pltpu.VMEM(block, f32),
                pltpu.VMEM(block, f32),
                pltpu.VMEM(block, f32),
                pltpu.VMEM((cx + 2, MODELS, cy, cz), f32),
                pltpu.VMEM((cx, MODELS, rows, cz), f32),
                pltpu.VMEM((cx, MODELS, cy, cz), f32),
                pltpu.VMEM((MODELS, cy, cz), f32),
                pltpu.VMEM((ITERS + 1, MODELS, 8, cz), f32),
                pltpu.VMEM((ITERS + 1, 5, MODELS, 8, cz), f32),
                pltpu.VMEM((MODELS, rows, cz), f32),
                pltpu.VMEM((ITERS, 2, cz), f32),
                pltpu.VMEM((ITERS, others, 2, cz), f32),
                pltpu.SemaphoreType.DMA((4,)),
                pltpu.SemaphoreType.DMA((ITERS + 1, 13)),
                pltpu.SemaphoreType.DMA((ITERS + 1, 13)),
                pltpu.SemaphoreType.DMA((ITERS,)),
                pltpu.SemaphoreType.DMA((ITERS,)),
                pltpu.SemaphoreType.REGULAR((2,)),
            ],
            compiler_params=pltpu.CompilerParams(
                collective_id=0, has_side_effects=True, vmem_limit_bytes=24 * 2**20),
        )(*[pltpu.with_memory_space_constraint(a, pltpu.HBM) for a in (models, targets, weights)])

    spec = P(None, "gx", "gy", "gz")
    return jax.shard_map(local, mesh=mesh, in_specs=(spec,) * 3, out_specs=(spec,) * 2, check_vma=False)
```

```python
import functools

import jax
import jax.numpy as jnp
from jax import lax
from jax.experimental import pallas as pl
from jax.experimental.pallas import tpu as pltpu
from jax.sharding import PartitionSpec as P

ITERS = 3
MESH = pl.DeviceIdType.MESH
MODELS = 2
XO = 2
YO = 8
LOW, HIGH = 2, 3
SPAN = 5
UNROLL = 4
KAPPA = 0.05 * -2.0 * 0.5 * 0.125


def kernel(sizes, models, targets, weights, updated, applied_out,
           field, tgt, wgt, base, flux0, flux1, flux2, z_own, z_got, z_field, z_flux, z_grad, z_fixed,
           x_own, x_got, corner, own, got,
           load_sem, send_sem, recv_sem, fixed_send, fixed_recv, sum_send, sum_recv, enter_sem):
    nx, ny, nz = sizes
    _, cx, cy, cz = updated.shape
    tiles = cy // 8
    rows = field.shape[3]
    wide = tiles + 1
    gx, gy, gz = lax.axis_index("gx"), lax.axis_index("gy"), lax.axis_index("gz")

    faces = [(1, 0, 0), (-1, 0, 0), (0, 1, 0), (0, -1, 0), (1, 1, 0), (1, -1, 0), (-1, 1, 0), (-1, -1, 0)]
    z_faces = [(0, 0, 1), (1, 0, 0), (-1, 0, 0), (1, 0, 1), (-1, 0, 1), (0, 1, 0), (0, -1, 0), (0, 1, 1), (0, -1, 1),
               (1, 1, 1), (1, -1, 1), (-1, 1, 1), (-1, -1, 1)]
    corners = z_faces[9:]

    def there(ox, oy):
        ok = None
        for place, step, count in ((gx, ox, nx), (gy, oy, ny)):
            if step != 0:
                here = place < count - 1 if step > 0 else place > 0
                ok = here if ok is None else jnp.logical_and(ok, here)
        return ok

    def guarded(ok, action):
        if ok is None:
            action()
        else:
            pl.when(ok)(action)

    def device(ox, oy, oz):
        return {"gx": gx + ox, "gy": gy + oy, "gz": gz + oz - 2 * oz * gz}

    def slices(step, offset, count, skip, depth):
        if step > 0:
            return pl.ds(offset + count - LOW, LOW), pl.ds(offset - LOW, LOW)
        if step < 0:
            return pl.ds(offset + skip, depth - skip), pl.ds(offset + count + skip, depth - skip)
        return pl.ds(offset, count), pl.ds(offset, count)

    def message(k, j, last=False):
        if j < len(faces):
            ox, oy, oz = faces[j]
            if last:
                x_src, x_dst = (pl.ds(XO + cx - 1, 1), pl.ds(XO - 1, 1)) if ox else (pl.ds(XO, cx),) * 2
                y_src, y_dst = (pl.ds(YO + cy - 1, 1), pl.ds(YO - 1, 1)) if oy else (pl.ds(YO, cy),) * 2
            else:
                edge_of = ox != 0 and oy != 0
                skip, depth = (0, 2) if edge_of else (0 if k == 0 else 1, HIGH)
                x_src, x_dst = slices(ox, XO, cx, skip, depth)
                y_src, y_dst = slices(oy, YO, cy, skip, depth)
            src, dst = field.at[k, x_src, :, y_src, :], field.at[k, x_dst, :, y_dst, :]
        else:
            ox, oy, oz = offset = z_faces[j - len(faces)]
            y_src, y_dst = slices(oy, YO, cy, 0, 2)
            into = z_got if oz else z_own
            if ox and oy:
                line = YO + cy - 1 if oy > 0 else YO
                src, dst = z_own.at[k, :, pl.ds(line, 1), :], corner.at[k, corners.index(offset), :, pl.ds(0, 1), :]
            elif ox:
                src, dst = x_own.at[k, 0 if ox > 0 else 1], x_got.at[k, 0 if ox > 0 else 1, oz]
            else:
                src, dst = z_own.at[k, :, y_src, :], into.at[k, :, y_dst, :]
        return pltpu.make_async_remote_copy(
            src_ref=src, dst_ref=dst, send_sem=send_sem.at[k, j], recv_sem=recv_sem.at[k, j],
            device_id=device(ox, oy, oz), device_id_type=MESH)

    everything = faces + z_faces
    plain = list(range(len(faces)))
    through_z = list(range(len(faces), len(everything)))

    def start_copies(k, which, last=False):
        for j in which:
            guarded(there(*everything[j][:2]), lambda j=j: message(k, j, last).start())

    def wait_copies(k, which, last=False):
        for j in which:
            ox, oy, _ = everything[j]
            guarded(there(-ox, -oy), lambda j=j: message(k, j, last).wait_recv())

    def wait_sent(k, which, last=False):
        for j in which:
            guarded(there(*everything[j][:2]), lambda j=j: message(k, j, last).wait_send())

    def fixed_message(j):
        array = (wgt, tgt)[j % 2]
        if j < 2:
            ox, oy, oz = -1, 0, 0
            src, dst = array.at[:, pl.ds(0, 1), pl.ds(YO, cy), :], array.at[:, pl.ds(cx, 1), pl.ds(YO, cy), :]
        elif j < 4:
            ox, oy, oz = 0, -1, 0
            src, dst = array.at[:, pl.ds(0, cx), pl.ds(YO, 1), :], array.at[:, pl.ds(0, cx), pl.ds(YO + cy, 1), :]
        else:
            ox, oy, oz = 0, 0, 1
            src, dst = z_fixed.at[0], z_fixed.at[1]
        return pltpu.make_async_remote_copy(
            src_ref=src, dst_ref=dst, send_sem=fixed_send.at[j], recv_sem=fixed_recv.at[j],
            device_id=device(ox, oy, oz), device_id_type=MESH), there(ox, oy), there(-ox, -oy)

    others = [(x, y, z) for z in range(nz) for y in range(ny) for x in range(nx) if (x, y, z) != (0, 0, 0)]

    def peer(x, y, z):
        return {"gx": lax.rem(gx + x, nx) if x else gx, "gy": lax.rem(gy + y, ny) if y else gy,
                "gz": lax.rem(gz + z, nz) if z else gz}

    def start_sum(k):
        for j, offset in enumerate(others):
            pltpu.make_async_remote_copy(
                src_ref=own.at[k], dst_ref=got.at[k, j], send_sem=sum_send.at[k], recv_sem=sum_recv.at[k],
                device_id=peer(*offset), device_id_type=MESH).start()

    def whole_sum(k):
        return pltpu.make_async_remote_copy(
            src_ref=got.at[k], dst_ref=got.at[k], send_sem=sum_send.at[k], recv_sem=sum_recv.at[k],
            device_id=peer(1, 0, 0), device_id_type=MESH)

    def on_line(x, y, z):
        return {"gx": x, "gy": y, "gz": z}

    pair, quad, chip_z = lax.rem(gx, 2), lax.rem(lax.div(gx, 2), 2), lax.div(gx, 4)
    line_x = [on_line(gx + c - 2 * c * pair, lax.rem(gy + s, ny), gz)
              for s in range(ny) for c in range(2) if (c, s) != (0, 0)]
    line_y = [on_line(gx + 2 * h - 4 * h * quad, gy, gz + s - 2 * s * gz)
              for s in range(nz) for h in range(2) if (h, s) != (0, 0)]
    line_z = [on_line(lax.rem(gx + 4 * s, nx), gy, gz) for s in range(1, nx // 4)]

    def tell(sem, line):
        for device in line:
            pl.semaphore_signal(sem, 1, device_id=device, device_id_type=MESH)

    inner = pl.ds(YO, cy)
    loads = [pltpu.make_async_copy(models.at[m], field.at[0, pl.ds(XO, cx), m, inner, :], load_sem.at[m]) for m in range(MODELS)]
    loads.append(pltpu.make_async_copy(targets, tgt.at[:, pl.ds(0, cx), inner, :], load_sem.at[2]))
    loads.append(pltpu.make_async_copy(weights, wgt.at[:, pl.ds(0, cx), inner, :], load_sem.at[3]))
    for copy in loads:
        copy.start()

    zero = jnp.zeros((8, cz), jnp.float32)

    def clear_planes(start, count, side):
        for k in range(ITERS + 1):
            for x in range(start, start + count):
                for m in range(MODELS):
                    for r in range(0, rows, 8):
                        field[k, x, m, pl.ds(r, 8), :] = zero
            for oz in range(2):
                x_got[k, side, oz] = zero

    def clear_rows(start):
        def clear(x, _):
            for k in range(ITERS + 1):
                for m in range(MODELS):
                    field[k, x, m, pl.ds(start, 8), :] = zero
            return 0

        lax.fori_loop(0, cx + LOW + HIGH, clear, 0)
        for k in range(ITERS + 1):
            for m in range(MODELS):
                z_own[k, m, pl.ds(start, 8), :] = zero
                z_got[k, m, pl.ds(start, 8), :] = zero

    def clear_corner(j):
        for k in range(ITERS + 1):
            for m in range(MODELS):
                corner[k, j, m] = zero

    for j, (ox, oy, _) in enumerate(corners):
        pl.when(jnp.logical_not(there(-ox, -oy)))(functools.partial(clear_corner, j))
    pl.when(gx == 0)(lambda: clear_planes(0, LOW, 0))
    pl.when(gx == nx - 1)(lambda: clear_planes(XO + cx, HIGH, 1))
    pl.when(gy == 0)(lambda: clear_rows(0))
    pl.when(gy == ny - 1)(lambda: clear_rows(rows - 8))

    barrier = pltpu.get_barrier_semaphore()
    expected = len(line_x) + len(line_y) + len(line_z)
    for ox, oy, oz in dict.fromkeys(everything):
        ok = there(ox, oy)
        guarded(ok, lambda ox=ox, oy=oy, oz=oz: pl.semaphore_signal(
            barrier, 1, device_id=device(ox, oy, oz), device_id_type=MESH))
        expected = expected + (1 if ok is None else ok.astype(jnp.int32))
    for line in (line_x, line_y, line_z):
        tell(barrier, line)

    lane = lax.broadcasted_iota(jnp.int32, (8, cz), 1)
    first, last_lane = lane == 0, lane == cz - 1
    ghost_lane = lane == jnp.where(gz == 0, 0, cz - 1)
    upward = 1 - 2 * gz
    beyond = (lax.rem(lane, SPAN) - 2) * upward >= 0
    beyond_x = (lax.rem(lax.rem(lane, 16), SPAN) - 2) * upward >= 0
    to_own = jnp.where(gz == 0, cz - 1, 1)

    def turn(v, shift):
        if isinstance(shift, int):
            shift = shift % cz
            return v if shift == 0 else pltpu.roll(v, shift, 1)
        return pltpu.roll(v, shift, 1)

    def edge(lines, x):
        return jnp.where(ghost_lane, turn(lines, lax.rem(2 * cz - SPAN * (x + 2) - 2 - gz, cz)), 0.0)

    def z_pair(v, e):
        return turn(jnp.where(first, e, v), cz - 1), turn(jnp.where(last_lane, e, v), 1)

    def pack(acc, v, x):
        return jnp.where(lax.div(lane, SPAN) == x + 2, turn(v, lax.rem(SPAN * (x + 2) + 3 - gz, cz)), acc)

    def tile_of(k, x, m, r):
        return field[k, x + XO, m, pl.ds(YO + r, 8), :]

    def over_x(body, carry):
        def block(b, carry):
            for u in range(UNROLL):
                carry = body(b * UNROLL + u, carry)
            return carry

        return lax.fori_loop(0, cx // UNROLL, block, carry)

    def pack_all(read, write):
        def planes(x, acc):
            return tuple(pack(a, read(x, m, t), x) for a, (m, t) in zip(acc, order))

        order = [(m, t) for m in range(MODELS) for t in range(tiles)]
        for a, (m, t) in zip(over_x(planes, (zero,) * len(order)), order):
            write(m, t, a)

    def pack_field(k):
        def write(m, t, v):
            z_own[k, m, pl.ds(YO + 8 * t, 8), :] = v

        pack_all(lambda x, m, t: tile_of(k, x, m, 8 * t), write)
        high, low = zero, zero
        for m in range(MODELS):
            for t in range(tiles):
                i = m * tiles + t
                v, mine = z_own[k, m, pl.ds(YO + 8 * t, 8), :], lax.div(lane, 16) == i
                high = jnp.where(mine, turn(v, 16 * i - SPAN * cx), high)
                low = jnp.where(mine, turn(v, 16 * i - 2 * SPAN), low)
        x_own[k, 0] = high
        x_own[k, 1] = low

    def join_z(k):
        low, high = [jnp.where(beyond_x, x_got[k, side, 1], turn(x_got[k, side, 0], to_own)) for side in range(2)]

        def inside(m, r):
            return jnp.where(beyond, z_got[k, m, pl.ds(r, 8), :], turn(z_own[k, m, pl.ds(r, 8), :], to_own))

        def with_x(v, before, after):
            return jnp.where(lane < 2 * SPAN, before, jnp.where(lane < SPAN * (cx + 2), v, after))

        for m in range(MODELS):
            for t in range(tiles):
                i = m * tiles + t
                z_field[min(k, 1), m, pl.ds(YO + 8 * t, 8), :] = with_x(
                    inside(m, YO + 8 * t), turn(low, -16 * i), turn(high, SPAN * (cx + 2) - 16 * i))
            for r, oy in ((0, 1), (YO + cy, -1)):
                before, after = [turn(jnp.broadcast_to(corner[k, corners.index((ox, oy, 1)), m, pl.ds(0, 1), :], (8, cz)),
                                      -ox * SPAN * cx) for ox in (1, -1)]
                z_field[min(k, 1), m, pl.ds(r, 8), :] = with_x(inside(m, r), before, after)

    def cross_part(a, b, i):
        j, l = (i + 1) % 3, (i + 2) % 3
        return a[j] * b[l] - a[l] * b[j]

    def flux_part(g1, g2, which):
        crossed = [None if i == which else cross_part(g1, g2, i) for i in range(3)]
        return [(cross_part(g2, crossed, i), cross_part(crossed, g1, i)) for i in (range(3) if which is None else [which])]

    for copy in loads[:MODELS]:
        copy.wait()
    pack_field(0)
    pl.semaphore_wait(barrier, expected)
    start_copies(0, through_z)
    start_copies(0, plain)
    tell(enter_sem.at[0], line_y)
    for copy in loads[MODELS:]:
        copy.wait()
    for a, array in enumerate((wgt, tgt)):
        def write(m, t, v, a=a):
            z_fixed[0, a, m, pl.ds(8 * t, 8), :] = v

        pack_all(lambda x, m, t, array=array: array[m, x, pl.ds(YO + 8 * t, 8), :], write)
    fixed = [fixed_message(j) for j in range(5)]
    for copy, sends, _ in fixed:
        guarded(sends, copy.start)
    wait_copies(0, through_z)
    join_z(0)
    wait_copies(0, plain)
    pl.semaphore_wait(enter_sem.at[0], len(line_y))
    tell(enter_sem.at[1], line_z)
    for copy, _, receives in fixed:
        guarded(receives, copy.wait_recv)

    for k in range(1, ITERS + 1):
        final = k == ITERS
        for j in range(wide):
            grads = []
            for m in range(MODELS):
                here = z_field[0, m, pl.ds(YO - 1 + 8 * j, 8), :]
                grads.append([turn(here, -SPAN) - turn(here, SPAN),
                              z_field[0, m, pl.ds(YO + 8 * j, 8), :] - z_field[0, m, pl.ds(YO - 2 + 8 * j, 8), :],
                              turn(here, -1) - turn(here, 1)])
            for i, parts in enumerate(flux_part(grads[0], grads[1], None)):
                for m in range(MODELS):
                    z_flux[i, m, pl.ds(YO - 1 + 8 * j, 8), :] = parts[m]

        for x in (-1, cx + 1):
            for j in range(wide):
                grads = []
                for m in range(MODELS):
                    here = tile_of(0, x, m, 8 * j - 1)
                    up, down = z_pair(here, edge(z_field[0, m, pl.ds(YO - 1 + 8 * j, 8), :], x))
                    grads.append([tile_of(0, x + 1, m, 8 * j - 1) - tile_of(0, x - 1, m, 8 * j - 1),
                                  tile_of(0, x, m, 8 * j) - tile_of(0, x, m, 8 * j - 2), up - down])
                parts = flux_part(grads[0], grads[1], 0)[0]
                for m in range(MODELS):
                    flux0[x + 1, m, pl.ds(YO - 1 + 8 * j, 8), :] = parts[m]

        def fluxes(x, carry):
            for j in range(wide):
                grads = []
                at = pl.ds(YO - 1 + 8 * j, 8)
                for m in range(MODELS):
                    here = tile_of(0, x, m, 8 * j - 1)
                    up, down = z_pair(here, edge(z_field[0, m, at, :], x))
                    xp, xm = tile_of(0, x + 1, m, 8 * j - 1), tile_of(0, x - 1, m, 8 * j - 1)
                    yp, ym = tile_of(0, x, m, 8 * j), tile_of(0, x, m, 8 * j - 2)
                    grads.append([xp - xm, yp - ym, up - down])
                    smooth = 6.0 * here - ((xp + xm) + (yp + ym) + (up + down))
                    base[m, x, at, :] = wgt[m, x, at, :] * (here - tgt[m, x, at, :]) + smooth
                parts = flux_part(grads[0], grads[1], None)
                for m in range(MODELS):
                    flux0[x + 1, m, at, :] = parts[0][m]
                    flux1[x, m, at, :] = parts[1][m]
                    flux2[x, m, at, :] = parts[2][m]
            return carry

        over_x(fluxes, 0)
        fluxes(cx, 0)

        def no_plane(x):
            for m in range(MODELS):
                for r in range(0, rows, 8):
                    flux0[x + 1, m, pl.ds(r, 8), :] = zero

        def no_row(y):
            for x in range(cx + 1):
                for m in range(MODELS):
                    flux1[x, m, pl.ds(YO + y, 1), :] = zero[0:1]

        pl.when(gx == 0)(lambda: no_plane(-1))
        pl.when(gx == nx - 1)(lambda: no_plane(cx))
        pl.when(gy == 0)(lambda: no_row(-1))
        pl.when(gy == ny - 1)(lambda: no_row(cy))

        def gradient(x, m, r):
            at = pl.ds(YO + r, 8)
            here = flux2[x, m, at, :]
            up, down = z_pair(here, edge(z_flux[2, m, at, :], x))
            div = (flux0[x + 2, m, at, :] - flux0[x, m, at, :]
                   + (flux1[x, m, pl.ds(YO + r + 1, 8), :] - flux1[x, m, pl.ds(YO + r - 1, 8), :]) + (up - down))
            return base[m, x, at, :] + KAPPA * div

        def gradients(x, norm):
            for t in range(tiles):
                for m in range(MODELS):
                    grad = gradient(x, m, 8 * t)
                    field[k, x + XO, m, pl.ds(YO + 8 * t, 8), :] = grad
                    norm = norm + grad * grad
            return norm

        norm = over_x(gradients, zero)

        def x_face():
            for t in range(tiles):
                for m in range(MODELS):
                    field[k, cx + XO, m, pl.ds(YO + 8 * t, 8), :] = gradient(cx, m, 8 * t)

        def y_face():
            def row_of(x, carry):
                for m in range(MODELS):
                    field[k, x + XO, m, pl.ds(YO + cy, 1), :] = gradient(x, m, cy)[0:1]
                return carry

            over_x(row_of, 0)

        pl.when(gx < nx - 1)(x_face)
        pl.when(gy < ny - 1)(y_face)
        start_copies(k, [0, 2] if final else plain, final)

        for t in range(tiles):
            for m in range(MODELS):
                def shifted(ref, i, dy=0):
                    return ref[i, m, pl.ds(YO + 8 * t + dy, 8), :]

                here, f0, f2 = shifted(z_field, 0), shifted(z_flux, 0), shifted(z_flux, 2)
                div = (turn(f0, -SPAN) - turn(f0, SPAN) + (shifted(z_flux, 1, 1) - shifted(z_flux, 1, -1))
                       + (turn(f2, -1) - turn(f2, 1)))
                around = ((turn(here, -SPAN) + turn(here, SPAN)) + (shifted(z_field, 0, 1) + shifted(z_field, 0, -1))
                          + (turn(here, -1) + turn(here, 1)))
                misfit = z_fixed[1, 0, m, pl.ds(8 * t, 8), :] * (here - z_fixed[1, 1, m, pl.ds(8 * t, 8), :])
                z_grad[m, pl.ds(YO + 8 * t, 8), :] = misfit + (6.0 * here - around) + KAPPA * div

        inside_up = (gz == 0).astype(jnp.float32)

        def curves(x, curve):
            for t in range(tiles):
                for m in range(MODELS):
                    here = tile_of(k, x, m, 8 * t)
                    e = edge(z_grad[m, pl.ds(YO + 8 * t, 8), :], x) * inside_up
                    up = turn(jnp.where(first, e, here), cz - 1)
                    pairs = tile_of(k, x + 1, m, 8 * t) + tile_of(k, x, m, 8 * t + 1) + up
                    curve = curve + here * ((wgt[m, x, pl.ds(YO + 8 * t, 8), :] + 6.0) * here - 2.0 * pairs)
            return curve

        curve = over_x(curves, zero)

        def fold(v):
            return jnp.sum(v, axis=0, keepdims=True)

        own[k - 1, pl.ds(0, 1), :] = fold(norm)
        own[k - 1, pl.ds(1, 1), :] = fold(curve)
        if k == 1:
            pl.semaphore_wait(enter_sem.at[1], len(line_z))
        start_sum(k - 1)
        if final:
            wait_copies(k, [0, 2], True)

            def applies(x, carry):
                for t in range(tiles):
                    for m in range(MODELS):
                        here = tile_of(k, x, m, 8 * t)
                        up, down = z_pair(here, edge(z_grad[m, pl.ds(YO + 8 * t, 8), :], x))
                        around = ((tile_of(k, x + 1, m, 8 * t) + tile_of(k, x - 1, m, 8 * t))
                                  + (tile_of(k, x, m, 8 * t + 1) + tile_of(k, x, m, 8 * t - 1)) + (up + down))
                        applied_out[m, x, pl.ds(8 * t, 8), :] = (
                            wgt[m, x, pl.ds(YO + 8 * t, 8), :] * here + (6.0 * here - around))
                return carry

            over_x(applies, 0)
        else:
            pack_field(k)
            start_copies(k, through_z)
            wait_copies(k, through_z)
            join_z(k)
            wait_copies(k, plain)
        whole_sum(k - 1).wait_recv()
        partial = [own[k - 1]] + [got[k - 1, j] for j in range(len(others))]
        while len(partial) > 1:
            partial = [sum(partial[i:i + 2]) for i in range(0, len(partial), 2)]
        sums = jnp.sum(partial[0], axis=1, keepdims=True)
        alpha = jnp.broadcast_to(sums[0:1] / sums[1:2], (8, cz))

        if k == 1:
            wait_sent(0, plain + through_z)
            for copy, sends, _ in fixed:
                guarded(sends, copy.wait_send)
        if final:
            wait_sent(k, [0, 2], True)
        else:
            wait_sent(k, plain + through_z)
        whole_sum(k - 1).wait_send()

        if final:
            def step(x, carry):
                for m in range(MODELS):
                    for t in range(tiles):
                        updated[m, x, pl.ds(8 * t, 8), :] = tile_of(0, x, m, 8 * t) - alpha * tile_of(k, x, m, 8 * t)
                return carry

            over_x(step, 0)
        else:
            def step(x, carry):
                for m in range(MODELS):
                    for r in range(0, rows, 8):
                        field[0, x, m, pl.ds(r, 8), :] = (
                            field[0, x, m, pl.ds(r, 8), :] - alpha * field[k, x, m, pl.ds(r, 8), :])
                return carry

            lax.fori_loop(0, cx + LOW + HIGH, step, 0)
            for m in range(MODELS):
                for r in range(0, rows, 8):
                    z_field[0, m, pl.ds(r, 8), :] = z_field[0, m, pl.ds(r, 8), :] - alpha * z_field[1, m, pl.ds(r, 8), :]


def solution(mesh):
    sizes = (mesh.shape["gx"], mesh.shape["gy"], mesh.shape["gz"])
    nx, ny, nz = sizes

    def local(models, targets, weights):
        _, cx, cy, cz = models.shape
        assert nz == 2 and nx % 4 == 0 and cy % 8 == 0
        assert SPAN * (cx + 4) <= cz and 16 * MODELS * (cy // 8) <= cz
        f32 = jnp.float32
        rows = YO + cy + 8
        others = nx * ny * nz - 1

        def vmem(*shape):
            return pltpu.VMEM(shape, f32)

        return pl.pallas_call(
            functools.partial(kernel, sizes),
            out_shape=[jax.ShapeDtypeStruct(models.shape, f32)] * 2,
            in_specs=[pl.BlockSpec(memory_space=pltpu.HBM)] * 3,
            out_specs=[pl.BlockSpec(memory_space=pltpu.VMEM)] * 2,
            scratch_shapes=[
                vmem(ITERS + 1, cx + LOW + HIGH, MODELS, rows, cz),
                vmem(MODELS, cx + 1, rows, cz),
                vmem(MODELS, cx + 1, rows, cz),
                vmem(MODELS, cx + 1, rows, cz),
                vmem(cx + 3, MODELS, rows, cz),
                vmem(cx + 1, MODELS, rows + 8, cz),
                vmem(cx + 1, MODELS, rows, cz),
                vmem(ITERS + 1, MODELS, rows, cz),
                vmem(ITERS + 1, MODELS, rows, cz),
                vmem(2, MODELS, rows, cz),
                vmem(3, MODELS, rows, cz),
                vmem(MODELS, rows, cz),
                vmem(2, 2, MODELS, cy, cz),
                vmem(ITERS + 1, 2, 8, cz),
                vmem(ITERS + 1, 2, 2, 8, cz),
                vmem(ITERS + 1, 4, MODELS, 8, cz),
                vmem(ITERS, 2, cz),
                vmem(ITERS, others, 2, cz),
                pltpu.SemaphoreType.DMA((4,)),
                pltpu.SemaphoreType.DMA((ITERS + 1, 21)),
                pltpu.SemaphoreType.DMA((ITERS + 1, 21)),
                pltpu.SemaphoreType.DMA((5,)),
                pltpu.SemaphoreType.DMA((5,)),
                pltpu.SemaphoreType.DMA((ITERS,)),
                pltpu.SemaphoreType.DMA((ITERS,)),
                pltpu.SemaphoreType.REGULAR((2,)),
            ],
            compiler_params=pltpu.CompilerParams(
                collective_id=0, has_side_effects=True, vmem_limit_bytes=24 * 2**20),
        )(*[pltpu.with_memory_space_constraint(a, pltpu.HBM) for a in (models, targets, weights)])

    spec = P(None, "gx", "gy", "gz")
    return jax.shard_map(local, mesh=mesh, in_specs=(spec,) * 3, out_specs=(spec,) * 2, check_vma=False)
```

```python
import functools

import jax
import jax.numpy as jnp
from jax import lax
from jax.experimental import pallas as pl
from jax.experimental.pallas import tpu as pltpu
from jax.sharding import PartitionSpec as P

ITERS = 3
MESH = pl.DeviceIdType.MESH
MODELS = 2
XO = 2
YO = 8
LOW, HIGH = 2, 3
SPAN = 5
FLUX, GRADIENT, CURVE, PACK, APPLY, STEP = 4, 4, 8, 4, 4, 4
KAPPA = 0.05 * -2.0 * 0.5 * 0.125


def kernel(sizes, models, targets, weights, updated, applied_out,
           field, tgt, wgt, base, flux0, flux1, flux2, z_own, z_got, z_field, z_flux, z_grad, z_fixed,
           x_own, x_got, corner, own, got,
           load_sem, send_sem, recv_sem, fixed_send, fixed_recv, sum_send, sum_recv, enter_sem):
    nx, ny, nz = sizes
    _, cx, cy, cz = updated.shape
    tiles = cy // 8
    rows = field.shape[3]
    wide = tiles + 1
    gx, gy, gz = lax.axis_index("gx"), lax.axis_index("gy"), lax.axis_index("gz")

    faces = [(1, 0, 0), (-1, 0, 0), (0, 1, 0), (0, -1, 0), (1, 1, 0), (1, -1, 0), (-1, 1, 0), (-1, -1, 0)]
    z_faces = [(0, 0, 1), (1, 0, 0), (-1, 0, 0), (1, 0, 1), (-1, 0, 1), (0, 1, 0), (0, -1, 0), (0, 1, 1), (0, -1, 1),
               (1, 1, 1), (1, -1, 1), (-1, 1, 1), (-1, -1, 1)]
    corners = z_faces[9:]

    def there(ox, oy):
        ok = None
        for place, step, count in ((gx, ox, nx), (gy, oy, ny)):
            if step != 0:
                here = place < count - 1 if step > 0 else place > 0
                ok = here if ok is None else jnp.logical_and(ok, here)
        return ok

    def guarded(ok, action):
        if ok is None:
            action()
        else:
            pl.when(ok)(action)

    def device(ox, oy, oz):
        return {"gx": gx + ox, "gy": gy + oy, "gz": gz + oz - 2 * oz * gz}

    def slices(step, offset, count, skip, depth):
        if step > 0:
            return pl.ds(offset + count - LOW, LOW), pl.ds(offset - LOW, LOW)
        if step < 0:
            return pl.ds(offset + skip, depth - skip), pl.ds(offset + count + skip, depth - skip)
        return pl.ds(offset, count), pl.ds(offset, count)

    def message(k, j, last=False):
        if j < len(faces):
            ox, oy, oz = faces[j]
            if last:
                x_src, x_dst = (pl.ds(XO + cx - 1, 1), pl.ds(XO - 1, 1)) if ox else (pl.ds(XO, cx),) * 2
                y_src, y_dst = (pl.ds(YO + cy - 1, 1), pl.ds(YO - 1, 1)) if oy else (pl.ds(YO, cy),) * 2
            else:
                edge_of = ox != 0 and oy != 0
                skip, depth = (0, 2) if edge_of else (0 if k == 0 else 1, HIGH)
                x_src, x_dst = slices(ox, XO, cx, skip, depth)
                y_src, y_dst = slices(oy, YO, cy, skip, depth)
            src, dst = field.at[k, x_src, :, y_src, :], field.at[k, x_dst, :, y_dst, :]
        else:
            ox, oy, oz = offset = z_faces[j - len(faces)]
            y_src, y_dst = slices(oy, YO, cy, 0, 2)
            into = z_got if oz else z_own
            if ox and oy:
                line = YO + cy - 1 if oy > 0 else YO
                src, dst = z_own.at[k, :, pl.ds(line, 1), :], corner.at[k, corners.index(offset), :, pl.ds(0, 1), :]
            elif ox:
                src, dst = x_own.at[k, 0 if ox > 0 else 1], x_got.at[k, 0 if ox > 0 else 1, oz]
            else:
                src, dst = z_own.at[k, :, y_src, :], into.at[k, :, y_dst, :]
        return pltpu.make_async_remote_copy(
            src_ref=src, dst_ref=dst, send_sem=send_sem.at[k, j], recv_sem=recv_sem.at[k, j],
            device_id=device(ox, oy, oz), device_id_type=MESH)

    everything = faces + z_faces
    plain = list(range(len(faces)))
    through_z = list(range(len(faces), len(everything)))

    def start_copies(k, which, last=False):
        for j in which:
            guarded(there(*everything[j][:2]), lambda j=j: message(k, j, last).start())

    def wait_copies(k, which, last=False):
        for j in which:
            ox, oy, _ = everything[j]
            guarded(there(-ox, -oy), lambda j=j: message(k, j, last).wait_recv())

    def wait_sent(k, which, last=False):
        for j in which:
            guarded(there(*everything[j][:2]), lambda j=j: message(k, j, last).wait_send())

    def fixed_message(j):
        array = (wgt, tgt)[j % 2]
        if j < 2:
            ox, oy, oz = -1, 0, 0
            src, dst = array.at[:, pl.ds(0, 1), pl.ds(YO, cy), :], array.at[:, pl.ds(cx, 1), pl.ds(YO, cy), :]
        elif j < 4:
            ox, oy, oz = 0, -1, 0
            src, dst = array.at[:, pl.ds(0, cx), pl.ds(YO, 1), :], array.at[:, pl.ds(0, cx), pl.ds(YO + cy, 1), :]
        else:
            ox, oy, oz = 0, 0, 1
            src, dst = z_fixed.at[0], z_fixed.at[1]
        return pltpu.make_async_remote_copy(
            src_ref=src, dst_ref=dst, send_sem=fixed_send.at[j], recv_sem=fixed_recv.at[j],
            device_id=device(ox, oy, oz), device_id_type=MESH), there(ox, oy), there(-ox, -oy)

    pair, quad, chip_z = lax.rem(gx, 2), lax.rem(lax.div(gx, 2), 2), lax.div(gx, 4)
    turns_z = nx // 4

    def hops(offset):
        x, z, h, q, c = offset
        return min(x, ny - x) + min(z, turns_z - z) + (1 if q else 2 * h), c

    others = [(x, z, h, q, c) for x in range(ny) for z in range(turns_z) for h in range(nz) for q in range(2) for c in range(2)]
    others = sorted(others, key=hops, reverse=True)[:-1]
    place_x = [lax.rem(gy + x, ny) if x else gy for x in range(ny)]
    place_h = [gz, 1 - gz]
    place_gx = {(z, q, c): 4 * (lax.rem(chip_z + z, turns_z) if z else chip_z) + 2 * (1 - quad if q else quad) + (1 - pair if c else pair)
                for z in range(turns_z) for q in range(2) for c in range(2)}

    def start_sum(k):
        for j, (x, z, h, q, c) in enumerate(others):
            pltpu.make_async_remote_copy(
                src_ref=own.at[k], dst_ref=got.at[k, pl.ds(j, 1)], send_sem=sum_send.at[k], recv_sem=sum_recv.at[k],
                device_id={"gx": place_gx[z, q, c], "gy": place_x[x], "gz": place_h[h]}, device_id_type=MESH).start()

    def whole_sum(k):
        landed = got.at[k, pl.ds(0, len(others))]
        return pltpu.make_async_remote_copy(
            src_ref=landed, dst_ref=landed, send_sem=sum_send.at[k], recv_sem=sum_recv.at[k],
            device_id={"gx": gx, "gy": gy, "gz": 1 - gz}, device_id_type=MESH)

    def on_line(x, y, z):
        return {"gx": x, "gy": y, "gz": z}

    line_x = [on_line(gx + c - 2 * c * pair, lax.rem(gy + s, ny), gz)
              for s in range(ny) for c in range(2) if (c, s) != (0, 0)]
    line_y = [on_line(gx + 2 * h - 4 * h * quad, gy, gz + s - 2 * s * gz)
              for s in range(nz) for h in range(2) if (h, s) != (0, 0)]
    line_z = [on_line(lax.rem(gx + 4 * s, nx), gy, gz) for s in range(1, nx // 4)]

    def tell(sem, line):
        for device in line:
            pl.semaphore_signal(sem, 1, device_id=device, device_id_type=MESH)

    inner = pl.ds(YO, cy)
    loads = [pltpu.make_async_copy(models.at[m], field.at[0, pl.ds(XO, cx), m, inner, :], load_sem.at[m]) for m in range(MODELS)]
    loads.append(pltpu.make_async_copy(targets, tgt.at[:, pl.ds(0, cx), inner, :], load_sem.at[2]))
    loads.append(pltpu.make_async_copy(weights, wgt.at[:, pl.ds(0, cx), inner, :], load_sem.at[3]))
    for copy in loads:
        copy.start()

    zero = jnp.zeros((8, cz), jnp.float32)

    def clear_planes(start, count, side):
        for k in range(ITERS + 1):
            for x in range(start, start + count):
                for m in range(MODELS):
                    for r in range(0, rows, 8):
                        field[k, x, m, pl.ds(r, 8), :] = zero
            for oz in range(2):
                x_got[k, side, oz] = zero

    def clear_rows(start):
        def clear(x, _):
            for k in range(ITERS + 1):
                for m in range(MODELS):
                    field[k, x, m, pl.ds(start, 8), :] = zero
            return 0

        lax.fori_loop(0, cx + LOW + HIGH, clear, 0)
        for k in range(ITERS + 1):
            for m in range(MODELS):
                z_own[k, m, pl.ds(start, 8), :] = zero
                z_got[k, m, pl.ds(start, 8), :] = zero

    def clear_corner(j):
        for k in range(ITERS + 1):
            for m in range(MODELS):
                corner[k, j, m] = zero

    for j, (ox, oy, _) in enumerate(corners):
        pl.when(jnp.logical_not(there(-ox, -oy)))(functools.partial(clear_corner, j))
    pl.when(gx == 0)(lambda: clear_planes(0, LOW, 0))
    pl.when(gx == nx - 1)(lambda: clear_planes(XO + cx, HIGH, 1))
    pl.when(gy == 0)(lambda: clear_rows(0))
    pl.when(gy == ny - 1)(lambda: clear_rows(rows - 8))

    barrier = pltpu.get_barrier_semaphore()
    expected = len(line_x) + len(line_y) + len(line_z)
    for ox, oy, oz in dict.fromkeys(everything):
        ok = there(ox, oy)
        guarded(ok, lambda ox=ox, oy=oy, oz=oz: pl.semaphore_signal(
            barrier, 1, device_id=device(ox, oy, oz), device_id_type=MESH))
        expected = expected + (1 if ok is None else ok.astype(jnp.int32))
    for line in (line_x, line_y, line_z):
        tell(barrier, line)

    lane = lax.broadcasted_iota(jnp.int32, (8, cz), 1)
    first, last_lane = lane == 0, lane == cz - 1
    ghost_lane = lane == jnp.where(gz == 0, 0, cz - 1)
    upward = 1 - 2 * gz
    beyond = (lax.rem(lane, SPAN) - 2) * upward >= 0
    beyond_x = (lax.rem(lax.rem(lane, 16), SPAN) - 2) * upward >= 0
    to_own = jnp.where(gz == 0, cz - 1, 1)

    def turn(v, shift):
        if isinstance(shift, int):
            shift = shift % cz
            return v if shift == 0 else pltpu.roll(v, shift, 1)
        return pltpu.roll(v, shift, 1)

    def edge(lines, x):
        return jnp.where(ghost_lane, turn(lines, lax.rem(2 * cz - SPAN * (x + 2) - 2 - gz, cz)), 0.0)

    def z_pair(v, e):
        return turn(jnp.where(first, e, v), cz - 1), turn(jnp.where(last_lane, e, v), 1)

    def pack(acc, v, x):
        return jnp.where(lax.div(lane, SPAN) == x + 2, turn(v, lax.rem(SPAN * (x + 2) + 3 - gz, cz)), acc)

    def tile_of(k, x, m, r):
        return field[k, x + XO, m, pl.ds(YO + r, 8), :]

    def over_x(body, carry, unroll):
        def block(b, carry):
            for u in range(unroll):
                carry = body(b * unroll + u, carry)
            return carry

        return lax.fori_loop(0, cx // unroll, block, carry)

    def pack_all(read, write):
        def planes(x, acc):
            return tuple(pack(a, read(x, m, t), x) for a, (m, t) in zip(acc, order))

        order = [(m, t) for m in range(MODELS) for t in range(tiles)]
        for a, (m, t) in zip(over_x(planes, (zero,) * len(order), PACK), order):
            write(m, t, a)

    def pack_field(k):
        def write(m, t, v):
            z_own[k, m, pl.ds(YO + 8 * t, 8), :] = v

        pack_all(lambda x, m, t: tile_of(k, x, m, 8 * t), write)
        high, low = zero, zero
        for m in range(MODELS):
            for t in range(tiles):
                i = m * tiles + t
                v, mine = z_own[k, m, pl.ds(YO + 8 * t, 8), :], lax.div(lane, 16) == i
                high = jnp.where(mine, turn(v, 16 * i - SPAN * cx), high)
                low = jnp.where(mine, turn(v, 16 * i - 2 * SPAN), low)
        x_own[k, 0] = high
        x_own[k, 1] = low

    def join_z(k):
        low, high = [jnp.where(beyond_x, x_got[k, side, 1], turn(x_got[k, side, 0], to_own)) for side in range(2)]

        def inside(m, r):
            return jnp.where(beyond, z_got[k, m, pl.ds(r, 8), :], turn(z_own[k, m, pl.ds(r, 8), :], to_own))

        def with_x(v, before, after):
            return jnp.where(lane < 2 * SPAN, before, jnp.where(lane < SPAN * (cx + 2), v, after))

        for m in range(MODELS):
            for t in range(tiles):
                i = m * tiles + t
                z_field[min(k, 1), m, pl.ds(YO + 8 * t, 8), :] = with_x(
                    inside(m, YO + 8 * t), turn(low, -16 * i), turn(high, SPAN * (cx + 2) - 16 * i))
            for r, oy in ((0, 1), (YO + cy, -1)):
                before, after = [turn(jnp.broadcast_to(corner[k, corners.index((ox, oy, 1)), m, pl.ds(0, 1), :], (8, cz)),
                                      -ox * SPAN * cx) for ox in (1, -1)]
                z_field[min(k, 1), m, pl.ds(r, 8), :] = with_x(inside(m, r), before, after)

    def cross_part(a, b, i):
        j, l = (i + 1) % 3, (i + 2) % 3
        return a[j] * b[l] - a[l] * b[j]

    def flux_part(g1, g2, which):
        crossed = [None if i == which else cross_part(g1, g2, i) for i in range(3)]
        return [(cross_part(g2, crossed, i), cross_part(crossed, g1, i)) for i in (range(3) if which is None else [which])]

    for copy in loads[:MODELS]:
        copy.wait()
    pack_field(0)
    pl.semaphore_wait(barrier, expected)
    start_copies(0, through_z)
    start_copies(0, plain)
    tell(enter_sem.at[0], line_y)
    for copy in loads[MODELS:]:
        copy.wait()
    for a, array in enumerate((wgt, tgt)):
        def write(m, t, v, a=a):
            z_fixed[0, a, m, pl.ds(8 * t, 8), :] = v

        pack_all(lambda x, m, t, array=array: array[m, x, pl.ds(YO + 8 * t, 8), :], write)
    fixed = [fixed_message(j) for j in range(5)]
    for copy, sends, _ in fixed:
        guarded(sends, copy.start)
    wait_copies(0, through_z)
    join_z(0)
    wait_copies(0, plain)
    pl.semaphore_wait(enter_sem.at[0], len(line_y))
    tell(enter_sem.at[1], line_z)
    for copy, _, receives in fixed:
        guarded(receives, copy.wait_recv)

    for k in range(1, ITERS + 1):
        final = k == ITERS
        for j in range(wide):
            grads = []
            for m in range(MODELS):
                here = z_field[0, m, pl.ds(YO - 1 + 8 * j, 8), :]
                grads.append([turn(here, -SPAN) - turn(here, SPAN),
                              z_field[0, m, pl.ds(YO + 8 * j, 8), :] - z_field[0, m, pl.ds(YO - 2 + 8 * j, 8), :],
                              turn(here, -1) - turn(here, 1)])
            for i, parts in enumerate(flux_part(grads[0], grads[1], None)):
                for m in range(MODELS):
                    z_flux[i, m, pl.ds(YO - 1 + 8 * j, 8), :] = parts[m]

        for x in (-1, cx + 1):
            for j in range(wide):
                grads = []
                for m in range(MODELS):
                    here = tile_of(0, x, m, 8 * j - 1)
                    up, down = z_pair(here, edge(z_field[0, m, pl.ds(YO - 1 + 8 * j, 8), :], x))
                    grads.append([tile_of(0, x + 1, m, 8 * j - 1) - tile_of(0, x - 1, m, 8 * j - 1),
                                  tile_of(0, x, m, 8 * j) - tile_of(0, x, m, 8 * j - 2), up - down])
                parts = flux_part(grads[0], grads[1], 0)[0]
                for m in range(MODELS):
                    flux0[x + 1, m, pl.ds(YO - 1 + 8 * j, 8), :] = parts[m]

        def fluxes(x, carry):
            for j in range(wide):
                grads = []
                at = pl.ds(YO - 1 + 8 * j, 8)
                for m in range(MODELS):
                    here = tile_of(0, x, m, 8 * j - 1)
                    up, down = z_pair(here, edge(z_field[0, m, at, :], x))
                    xp, xm = tile_of(0, x + 1, m, 8 * j - 1), tile_of(0, x - 1, m, 8 * j - 1)
                    yp, ym = tile_of(0, x, m, 8 * j), tile_of(0, x, m, 8 * j - 2)
                    grads.append([xp - xm, yp - ym, up - down])
                    smooth = 6.0 * here - ((xp + xm) + (yp + ym) + (up + down))
                    base[m, x, at, :] = wgt[m, x, at, :] * (here - tgt[m, x, at, :]) + smooth
                parts = flux_part(grads[0], grads[1], None)
                for m in range(MODELS):
                    flux0[x + 1, m, at, :] = parts[0][m]
                    flux1[x, m, at, :] = parts[1][m]
                    flux2[x, m, at, :] = parts[2][m]
            return carry

        fluxes(cx, 0)
        over_x(fluxes, 0, FLUX)

        def no_plane(x):
            for m in range(MODELS):
                for r in range(0, rows, 8):
                    flux0[x + 1, m, pl.ds(r, 8), :] = zero

        def no_row(y):
            for x in range(cx + 1):
                for m in range(MODELS):
                    flux1[x, m, pl.ds(YO + y, 1), :] = zero[0:1]

        pl.when(gx == 0)(lambda: no_plane(-1))
        pl.when(gx == nx - 1)(lambda: no_plane(cx))
        pl.when(gy == 0)(lambda: no_row(-1))
        pl.when(gy == ny - 1)(lambda: no_row(cy))

        def gradient(x, m, r):
            at = pl.ds(YO + r, 8)
            here = flux2[x, m, at, :]
            up, down = z_pair(here, edge(z_flux[2, m, at, :], x))
            div = (flux0[x + 2, m, at, :] - flux0[x, m, at, :]
                   + (flux1[x, m, pl.ds(YO + r + 1, 8), :] - flux1[x, m, pl.ds(YO + r - 1, 8), :]) + (up - down))
            return base[m, x, at, :] + KAPPA * div

        def gradients(x, norm):
            for t in range(tiles):
                for m in range(MODELS):
                    grad = gradient(x, m, 8 * t)
                    field[k, x + XO, m, pl.ds(YO + 8 * t, 8), :] = grad
                    norm = norm + grad * grad
            for m in range(MODELS):
                grad = gradient(x, m, cy)[0:1]
                field[k, x + XO, m, pl.ds(YO + cy, 1), :] = jnp.where(gy < ny - 1, grad, 0.0)
            return norm

        norm = over_x(gradients, zero, GRADIENT)

        if final:
            start_copies(k, [0, 2], True)
        for t in range(tiles):
            for m in range(MODELS):
                field[k, cx + XO, m, pl.ds(YO + 8 * t, 8), :] = jnp.where(gx < nx - 1, gradient(cx, m, 8 * t), 0.0)
        for t in range(tiles):
            for m in range(MODELS):
                def shifted(ref, i, dy=0):
                    return ref[i, m, pl.ds(YO + 8 * t + dy, 8), :]

                here, f0, f2 = shifted(z_field, 0), shifted(z_flux, 0), shifted(z_flux, 2)
                div = (turn(f0, -SPAN) - turn(f0, SPAN) + (shifted(z_flux, 1, 1) - shifted(z_flux, 1, -1))
                       + (turn(f2, -1) - turn(f2, 1)))
                around = ((turn(here, -SPAN) + turn(here, SPAN)) + (shifted(z_field, 0, 1) + shifted(z_field, 0, -1))
                          + (turn(here, -1) + turn(here, 1)))
                misfit = z_fixed[1, 0, m, pl.ds(8 * t, 8), :] * (here - z_fixed[1, 1, m, pl.ds(8 * t, 8), :])
                z_grad[m, pl.ds(YO + 8 * t, 8), :] = misfit + (6.0 * here - around) + KAPPA * div

        inside_up = (gz == 0).astype(jnp.float32)

        def curves(x, curve):
            for t in range(tiles):
                for m in range(MODELS):
                    here = tile_of(k, x, m, 8 * t)
                    e = edge(z_grad[m, pl.ds(YO + 8 * t, 8), :], x) * inside_up
                    up = turn(jnp.where(first, e, here), cz - 1)
                    pairs = tile_of(k, x + 1, m, 8 * t) + tile_of(k, x, m, 8 * t + 1) + up
                    curve = curve + here * ((wgt[m, x, pl.ds(YO + 8 * t, 8), :] + 6.0) * here - 2.0 * pairs)
            return curve

        curve = over_x(curves, zero, CURVE)

        def fold(v):
            v = jnp.sum(v, axis=0, keepdims=True)
            return v + turn(v, cz // 2)

        both = jnp.where(lane[0:1] < cz // 2, fold(norm), fold(curve))
        own[k - 1] = both
        got[k - 1, pl.ds(len(others), 1), :] = both
        if k == 1:
            pl.semaphore_wait(enter_sem.at[1], len(line_z))
        start_sum(k - 1)
        if final:
            wait_copies(k, [0, 2], True)

            def applies(x, carry):
                for t in range(tiles):
                    for m in range(MODELS):
                        here = tile_of(k, x, m, 8 * t)
                        up, down = z_pair(here, edge(z_grad[m, pl.ds(YO + 8 * t, 8), :], x))
                        around = ((tile_of(k, x + 1, m, 8 * t) + tile_of(k, x - 1, m, 8 * t))
                                  + (tile_of(k, x, m, 8 * t + 1) + tile_of(k, x, m, 8 * t - 1)) + (up + down))
                        applied_out[m, x, pl.ds(8 * t, 8), :] = (
                            wgt[m, x, pl.ds(YO + 8 * t, 8), :] * here + (6.0 * here - around))
                return carry

            over_x(applies, 0, APPLY)
        else:
            start_copies(k, plain)
            pack_field(k)
            start_copies(k, through_z)
            wait_copies(k, through_z)
            join_z(k)
            wait_copies(k, plain)
        whole_sum(k - 1).wait_recv()
        partial = [got[k - 1, pl.ds(r, 8), :] for r in range(0, len(others) + 1, 8)]
        while len(partial) > 1:
            partial = [sum(partial[i:i + 2]) for i in range(0, len(partial), 2)]
        half = lane < cz // 2
        sums = [jnp.sum(jnp.sum(jnp.where(half, *terms), axis=0, keepdims=True), axis=1, keepdims=True)
                for terms in ((partial[0], 0.0), (0.0, partial[0]))]
        alpha = jnp.broadcast_to(sums[0] / sums[1], (8, cz))

        if k == 1:
            wait_sent(0, plain + through_z)
            for copy, sends, _ in fixed:
                guarded(sends, copy.wait_send)
        if final:
            wait_sent(k, [0, 2], True)
        else:
            wait_sent(k, plain + through_z)
        whole_sum(k - 1).wait_send()

        if final:
            def step(x, carry):
                for m in range(MODELS):
                    for t in range(tiles):
                        updated[m, x, pl.ds(8 * t, 8), :] = tile_of(0, x, m, 8 * t) - alpha * tile_of(k, x, m, 8 * t)
                return carry

            over_x(step, 0, STEP)
        else:
            def step(x, carry):
                for m in range(MODELS):
                    for r in range(0, rows, 8):
                        field[0, x, m, pl.ds(r, 8), :] = (
                            field[0, x, m, pl.ds(r, 8), :] - alpha * field[k, x, m, pl.ds(r, 8), :])
                return carry

            lax.fori_loop(0, cx + LOW + HIGH, step, 0)
            for m in range(MODELS):
                for r in range(0, rows, 8):
                    z_field[0, m, pl.ds(r, 8), :] = z_field[0, m, pl.ds(r, 8), :] - alpha * z_field[1, m, pl.ds(r, 8), :]


def solution(mesh):
    sizes = (mesh.shape["gx"], mesh.shape["gy"], mesh.shape["gz"])
    nx, ny, nz = sizes

    def local(models, targets, weights):
        _, cx, cy, cz = models.shape
        assert nz == 2 and nx % 4 == 0 and cy % 8 == 0
        assert SPAN * (cx + 4) <= cz and 16 * MODELS * (cy // 8) <= cz
        f32 = jnp.float32
        rows = YO + cy + 8

        def vmem(*shape):
            return pltpu.VMEM(shape, f32)

        return pl.pallas_call(
            functools.partial(kernel, sizes),
            out_shape=[jax.ShapeDtypeStruct(models.shape, f32)] * 2,
            in_specs=[pl.BlockSpec(memory_space=pltpu.HBM)] * 3,
            out_specs=[pl.BlockSpec(memory_space=pltpu.VMEM)] * 2,
            scratch_shapes=[
                vmem(ITERS + 1, cx + LOW + HIGH, MODELS, rows, cz),
                vmem(MODELS, cx + 1, rows, cz),
                vmem(MODELS, cx + 1, rows, cz),
                vmem(MODELS, cx + 1, rows, cz),
                vmem(cx + 3, MODELS, rows, cz),
                vmem(cx + 1, MODELS, rows + 8, cz),
                vmem(cx + 1, MODELS, rows, cz),
                vmem(ITERS + 1, MODELS, rows, cz),
                vmem(ITERS + 1, MODELS, rows, cz),
                vmem(2, MODELS, rows, cz),
                vmem(3, MODELS, rows, cz),
                vmem(MODELS, rows, cz),
                vmem(2, 2, MODELS, cy, cz),
                vmem(ITERS + 1, 2, 8, cz),
                vmem(ITERS + 1, 2, 2, 8, cz),
                vmem(ITERS + 1, 4, MODELS, 8, cz),
                vmem(ITERS, 1, cz),
                vmem(ITERS, nx * ny * nz, cz),
                pltpu.SemaphoreType.DMA((4,)),
                pltpu.SemaphoreType.DMA((ITERS + 1, 21)),
                pltpu.SemaphoreType.DMA((ITERS + 1, 21)),
                pltpu.SemaphoreType.DMA((5,)),
                pltpu.SemaphoreType.DMA((5,)),
                pltpu.SemaphoreType.DMA((ITERS,)),
                pltpu.SemaphoreType.DMA((ITERS,)),
                pltpu.SemaphoreType.REGULAR((2,)),
            ],
            compiler_params=pltpu.CompilerParams(
                collective_id=0, has_side_effects=True, vmem_limit_bytes=24 * 2**20),
        )(*[pltpu.with_memory_space_constraint(a, pltpu.HBM) for a in (models, targets, weights)])

    spec = P(None, "gx", "gy", "gz")
    return jax.shard_map(local, mesh=mesh, in_specs=(spec,) * 3, out_specs=(spec,) * 2, check_vma=False)
```

```python
import functools

import jax
import jax.numpy as jnp
from jax import lax
from jax.experimental import pallas as pl
from jax.experimental.pallas import tpu as pltpu
from jax.sharding import PartitionSpec as P

ITERS = 3
MESH = pl.DeviceIdType.MESH
MODELS = 2
XO = 2
YO = 8
LOW, HIGH = 2, 3
SPAN = 5
FLUX, GRADIENT, CURVE, PACK, APPLY, STEP = 4, 4, 8, 4, 4, 4
KAPPA = 0.05 * -2.0 * 0.5 * 0.125


def kernel(sizes, models, targets, weights, updated, applied_out,
           field, tgt, wgt, base, flux0, flux1, flux2, z_own, z_got, z_field, z_flux, z_grad, z_fixed,
           x_own, x_got, corner, own, got,
           load_sem, send_sem, recv_sem, fixed_send, fixed_recv, sum_send, sum_recv, enter_sem):
    nx, ny, nz = sizes
    _, cx, cy, cz = updated.shape
    tiles = cy // 8
    rows = field.shape[3]
    wide = tiles + 1
    gx, gy, gz = lax.axis_index("gx"), lax.axis_index("gy"), lax.axis_index("gz")

    faces = [(1, 0, 0), (-1, 0, 0), (0, 1, 0), (0, -1, 0), (1, 1, 0), (1, -1, 0), (-1, 1, 0), (-1, -1, 0)]
    z_faces = [(0, 0, 1), (1, 0, 0), (-1, 0, 0), (1, 0, 1), (-1, 0, 1), (0, 1, 0), (0, -1, 0), (0, 1, 1), (0, -1, 1),
               (1, 1, 1), (1, -1, 1), (-1, 1, 1), (-1, -1, 1)]
    corners = z_faces[9:]

    def there(ox, oy):
        ok = None
        for place, step, count in ((gx, ox, nx), (gy, oy, ny)):
            if step != 0:
                here = place < count - 1 if step > 0 else place > 0
                ok = here if ok is None else jnp.logical_and(ok, here)
        return ok

    def guarded(ok, action):
        if ok is None:
            action()
        else:
            pl.when(ok)(action)

    def device(ox, oy, oz):
        return {"gx": gx + ox, "gy": gy + oy, "gz": gz + oz - 2 * oz * gz}

    def slices(step, offset, count, skip, depth):
        if step > 0:
            return pl.ds(offset + count - LOW, LOW), pl.ds(offset - LOW, LOW)
        if step < 0:
            return pl.ds(offset + skip, depth - skip), pl.ds(offset + count + skip, depth - skip)
        return pl.ds(offset, count), pl.ds(offset, count)

    def message(k, j, last=False):
        if j < len(faces):
            ox, oy, oz = faces[j]
            if last:
                x_src, x_dst = (pl.ds(XO + cx - 1, 1), pl.ds(XO - 1, 1)) if ox else (pl.ds(XO, cx),) * 2
                y_src, y_dst = (pl.ds(YO + cy - 1, 1), pl.ds(YO - 1, 1)) if oy else (pl.ds(YO, cy),) * 2
            else:
                edge_of = ox != 0 and oy != 0
                skip, depth = (0, 2) if edge_of else (0 if k == 0 else 1, HIGH)
                x_src, x_dst = slices(ox, XO, cx, skip, depth)
                y_src, y_dst = slices(oy, YO, cy, skip, depth)
            src, dst = field.at[k, x_src, :, y_src, :], field.at[k, x_dst, :, y_dst, :]
        else:
            ox, oy, oz = offset = z_faces[j - len(faces)]
            y_src, y_dst = slices(oy, YO, cy, 0, 2)
            into = z_got if oz else z_own
            if ox and oy:
                line = YO + cy - 1 if oy > 0 else YO
                src, dst = z_own.at[k, :, pl.ds(line, 1), :], corner.at[k, corners.index(offset), :, pl.ds(0, 1), :]
            elif ox:
                src, dst = x_own.at[k, 0 if ox > 0 else 1], x_got.at[k, 0 if ox > 0 else 1, oz]
            else:
                src, dst = z_own.at[k, :, y_src, :], into.at[k, :, y_dst, :]
        return pltpu.make_async_remote_copy(
            src_ref=src, dst_ref=dst, send_sem=send_sem.at[k, j], recv_sem=recv_sem.at[k, j],
            device_id=device(ox, oy, oz), device_id_type=MESH)

    everything = faces + z_faces
    plain = list(range(len(faces)))
    through_z = list(range(len(faces), len(everything)))

    def start_copies(k, which, last=False):
        for j in which:
            guarded(there(*everything[j][:2]), lambda j=j: message(k, j, last).start())

    def wait_copies(k, which, last=False):
        for j in which:
            ox, oy, _ = everything[j]
            guarded(there(-ox, -oy), lambda j=j: message(k, j, last).wait_recv())

    def wait_sent(k, which, last=False):
        for j in which:
            guarded(there(*everything[j][:2]), lambda j=j: message(k, j, last).wait_send())

    def fixed_message(j):
        array = (wgt, tgt)[j % 2]
        if j < 2:
            ox, oy, oz = -1, 0, 0
            src, dst = array.at[:, pl.ds(0, 1), pl.ds(YO, cy), :], array.at[:, pl.ds(cx, 1), pl.ds(YO, cy), :]
        elif j < 4:
            ox, oy, oz = 0, -1, 0
            src, dst = array.at[:, pl.ds(0, cx), pl.ds(YO, 1), :], array.at[:, pl.ds(0, cx), pl.ds(YO + cy, 1), :]
        else:
            ox, oy, oz = 0, 0, 1
            src, dst = z_fixed.at[0], z_fixed.at[1]
        return pltpu.make_async_remote_copy(
            src_ref=src, dst_ref=dst, send_sem=fixed_send.at[j], recv_sem=fixed_recv.at[j],
            device_id=device(ox, oy, oz), device_id_type=MESH), there(ox, oy), there(-ox, -oy)

    pair, quad, chip_z = lax.rem(gx, 2), lax.rem(lax.div(gx, 2), 2), lax.div(gx, 4)
    turns_z = nx // 4

    def hops(offset):
        x, z, h, q, c = offset
        return min(x, ny - x) + min(z, turns_z - z) + (1 if q else 2 * h), c

    others = [(x, z, h, q, c) for x in range(ny) for z in range(turns_z) for h in range(nz) for q in range(2) for c in range(2)]
    others = sorted(others, key=hops, reverse=True)[:-1]
    place_x = [lax.rem(gy + x, ny) if x else gy for x in range(ny)]
    place_h = [gz, 1 - gz]
    place_gx = {(z, q, c): 4 * (lax.rem(chip_z + z, turns_z) if z else chip_z) + 2 * (1 - quad if q else quad) + (1 - pair if c else pair)
                for z in range(turns_z) for q in range(2) for c in range(2)}

    def start_sum(k):
        for j, (x, z, h, q, c) in enumerate(others):
            pltpu.make_async_remote_copy(
                src_ref=own.at[k], dst_ref=got.at[k, pl.ds(j, 1)], send_sem=sum_send.at[k], recv_sem=sum_recv.at[k],
                device_id={"gx": place_gx[z, q, c], "gy": place_x[x], "gz": place_h[h]}, device_id_type=MESH).start()

    def whole_sum(k):
        landed = got.at[k, pl.ds(0, len(others))]
        return pltpu.make_async_remote_copy(
            src_ref=landed, dst_ref=landed, send_sem=sum_send.at[k], recv_sem=sum_recv.at[k],
            device_id={"gx": gx, "gy": gy, "gz": 1 - gz}, device_id_type=MESH)

    def on_line(x, y, z):
        return {"gx": x, "gy": y, "gz": z}

    line_x = [on_line(gx + c - 2 * c * pair, lax.rem(gy + s, ny), gz)
              for s in range(ny) for c in range(2) if (c, s) != (0, 0)]
    line_y = [on_line(gx + 2 * h - 4 * h * quad, gy, gz + s - 2 * s * gz)
              for s in range(nz) for h in range(2) if (h, s) != (0, 0)]
    line_z = [on_line(lax.rem(gx + 4 * s, nx), gy, gz) for s in range(1, nx // 4)]

    def tell(sem, line):
        for device in line:
            pl.semaphore_signal(sem, 1, device_id=device, device_id_type=MESH)

    inner = pl.ds(YO, cy)
    loads = [pltpu.make_async_copy(models.at[m], field.at[0, pl.ds(XO, cx), m, inner, :], load_sem.at[m]) for m in range(MODELS)]
    loads.append(pltpu.make_async_copy(targets, tgt.at[:, pl.ds(0, cx), inner, :], load_sem.at[2]))
    loads.append(pltpu.make_async_copy(weights, wgt.at[:, pl.ds(0, cx), inner, :], load_sem.at[3]))
    for copy in loads:
        copy.start()

    zero = jnp.zeros((8, cz), jnp.float32)

    def clear_planes(start, count, side):
        for k in range(ITERS + 1):
            for x in range(start, start + count):
                for m in range(MODELS):
                    for r in range(0, rows, 8):
                        field[k, x, m, pl.ds(r, 8), :] = zero
            for oz in range(2):
                x_got[k, side, oz] = zero

    def clear_rows(start):
        def clear(x, _):
            for k in range(ITERS + 1):
                for m in range(MODELS):
                    field[k, x, m, pl.ds(start, 8), :] = zero
            return 0

        lax.fori_loop(0, cx + LOW + HIGH, clear, 0)
        for k in range(ITERS + 1):
            for m in range(MODELS):
                z_own[k, m, pl.ds(start, 8), :] = zero
                z_got[k, m, pl.ds(start, 8), :] = zero

    def clear_corner(j):
        for k in range(ITERS + 1):
            for m in range(MODELS):
                corner[k, j, m] = zero

    for j, (ox, oy, _) in enumerate(corners):
        pl.when(jnp.logical_not(there(-ox, -oy)))(functools.partial(clear_corner, j))
    pl.when(gx == 0)(lambda: clear_planes(0, LOW, 0))
    pl.when(gx == nx - 1)(lambda: clear_planes(XO + cx, HIGH, 1))
    pl.when(gy == 0)(lambda: clear_rows(0))
    pl.when(gy == ny - 1)(lambda: clear_rows(rows - 8))

    barrier = pltpu.get_barrier_semaphore()
    expected = len(line_x) + len(line_y) + len(line_z)
    for ox, oy, oz in dict.fromkeys(everything):
        ok = there(ox, oy)
        guarded(ok, lambda ox=ox, oy=oy, oz=oz: pl.semaphore_signal(
            barrier, 1, device_id=device(ox, oy, oz), device_id_type=MESH))
        expected = expected + (1 if ok is None else ok.astype(jnp.int32))
    for line in (line_x, line_y, line_z):
        tell(barrier, line)

    lane = lax.broadcasted_iota(jnp.int32, (8, cz), 1)
    first, last_lane = lane == 0, lane == cz - 1
    end_lane = (1 - gz) * (cz - 1)
    ghost_lane = lane == end_lane
    upward = 1 - 2 * gz
    beyond = (lax.rem(lane, SPAN) - 2) * upward >= 0
    beyond_x = (lax.rem(lax.rem(lane, 16), SPAN) - 2) * upward >= 0
    to_own = jnp.where(gz == 0, cz - 1, 1)

    def turn(v, shift):
        if isinstance(shift, int):
            shift = shift % cz
            return v if shift == 0 else pltpu.roll(v, shift, 1)
        return pltpu.roll(v, shift, 1)

    def edge(lines, x):
        return jnp.where(ghost_lane, turn(lines, lax.rem(cz + end_lane - SPAN * (x + 2) - 2, cz)), 0.0)

    def z_pair(v, e):
        return jnp.where(last_lane, e, turn(v, cz - 1)), jnp.where(first, e, turn(v, 1))

    def pack(acc, v, x):
        return jnp.where(lax.div(lane, SPAN) == x + 2, turn(v, lax.rem(SPAN * (x + 2) + 3 - gz, cz)), acc)

    def tile_of(k, x, m, r):
        return field[k, x + XO, m, pl.ds(YO + r, 8), :]

    def over_x(body, carry, unroll):
        def block(b, carry):
            for u in range(unroll):
                carry = body(b * unroll + u, carry)
            return carry

        return lax.fori_loop(0, cx // unroll, block, carry)

    def pack_all(read, write):
        def planes(x, acc):
            return tuple(pack(a, read(x, m, t), x) for a, (m, t) in zip(acc, order))

        order = [(m, t) for m in range(MODELS) for t in range(tiles)]
        for a, (m, t) in zip(over_x(planes, (zero,) * len(order), PACK), order):
            write(m, t, a)

    def pack_field(k):
        def write(m, t, v):
            z_own[k, m, pl.ds(YO + 8 * t, 8), :] = v

        pack_all(lambda x, m, t: tile_of(k, x, m, 8 * t), write)
        high, low = zero, zero
        for m in range(MODELS):
            for t in range(tiles):
                i = m * tiles + t
                v, mine = z_own[k, m, pl.ds(YO + 8 * t, 8), :], lax.div(lane, 16) == i
                high = jnp.where(mine, turn(v, 16 * i - SPAN * cx), high)
                low = jnp.where(mine, turn(v, 16 * i - 2 * SPAN), low)
        x_own[k, 0] = high
        x_own[k, 1] = low

    def join_z(k):
        low, high = [jnp.where(beyond_x, x_got[k, side, 1], turn(x_got[k, side, 0], to_own)) for side in range(2)]

        def inside(m, r):
            return jnp.where(beyond, z_got[k, m, pl.ds(r, 8), :], turn(z_own[k, m, pl.ds(r, 8), :], to_own))

        def with_x(v, before, after):
            return jnp.where(lane < 2 * SPAN, before, jnp.where(lane < SPAN * (cx + 2), v, after))

        for m in range(MODELS):
            for t in range(tiles):
                i = m * tiles + t
                z_field[min(k, 1), m, pl.ds(YO + 8 * t, 8), :] = with_x(
                    inside(m, YO + 8 * t), turn(low, -16 * i), turn(high, SPAN * (cx + 2) - 16 * i))
            for r, oy in ((0, 1), (YO + cy, -1)):
                before, after = [turn(jnp.broadcast_to(corner[k, corners.index((ox, oy, 1)), m, pl.ds(0, 1), :], (8, cz)),
                                      -ox * SPAN * cx) for ox in (1, -1)]
                z_field[min(k, 1), m, pl.ds(r, 8), :] = with_x(inside(m, r), before, after)

    def cross_part(a, b, i):
        j, l = (i + 1) % 3, (i + 2) % 3
        return a[j] * b[l] - a[l] * b[j]

    def flux_part(g1, g2, which):
        crossed = [None if i == which else cross_part(g1, g2, i) for i in range(3)]
        return [(cross_part(g2, crossed, i), cross_part(crossed, g1, i)) for i in (range(3) if which is None else [which])]

    for copy in loads[:MODELS]:
        copy.wait()
    pack_field(0)
    pl.semaphore_wait(barrier, expected)
    start_copies(0, through_z)
    start_copies(0, plain)
    tell(enter_sem.at[0], line_y)
    for copy in loads[MODELS:]:
        copy.wait()
    for a, array in enumerate((wgt, tgt)):
        def write(m, t, v, a=a):
            z_fixed[0, a, m, pl.ds(8 * t, 8), :] = v

        pack_all(lambda x, m, t, array=array: array[m, x, pl.ds(YO + 8 * t, 8), :], write)
    fixed = [fixed_message(j) for j in range(5)]
    for copy, sends, _ in fixed:
        guarded(sends, copy.start)
    wait_copies(0, through_z)
    join_z(0)
    wait_copies(0, plain)
    pl.semaphore_wait(enter_sem.at[0], len(line_y))
    tell(enter_sem.at[1], line_z)
    for copy, _, receives in fixed:
        guarded(receives, copy.wait_recv)

    for k in range(1, ITERS + 1):
        final = k == ITERS
        for j in range(wide):
            grads = []
            for m in range(MODELS):
                here = z_field[0, m, pl.ds(YO - 1 + 8 * j, 8), :]
                grads.append([turn(here, -SPAN) - turn(here, SPAN),
                              z_field[0, m, pl.ds(YO + 8 * j, 8), :] - z_field[0, m, pl.ds(YO - 2 + 8 * j, 8), :],
                              turn(here, -1) - turn(here, 1)])
            for i, parts in enumerate(flux_part(grads[0], grads[1], None)):
                for m in range(MODELS):
                    z_flux[i, m, pl.ds(YO - 1 + 8 * j, 8), :] = parts[m]

        for x in (-1, cx + 1):
            for j in range(wide):
                grads = []
                for m in range(MODELS):
                    here = tile_of(0, x, m, 8 * j - 1)
                    up, down = z_pair(here, edge(z_field[0, m, pl.ds(YO - 1 + 8 * j, 8), :], x))
                    grads.append([tile_of(0, x + 1, m, 8 * j - 1) - tile_of(0, x - 1, m, 8 * j - 1),
                                  tile_of(0, x, m, 8 * j) - tile_of(0, x, m, 8 * j - 2), up - down])
                parts = flux_part(grads[0], grads[1], 0)[0]
                for m in range(MODELS):
                    flux0[x + 1, m, pl.ds(YO - 1 + 8 * j, 8), :] = parts[m]

        def fluxes(x, carry):
            for j in range(wide):
                grads = []
                at = pl.ds(YO - 1 + 8 * j, 8)
                for m in range(MODELS):
                    here = tile_of(0, x, m, 8 * j - 1)
                    up, down = z_pair(here, edge(z_field[0, m, at, :], x))
                    xp, xm = tile_of(0, x + 1, m, 8 * j - 1), tile_of(0, x - 1, m, 8 * j - 1)
                    yp, ym = tile_of(0, x, m, 8 * j), tile_of(0, x, m, 8 * j - 2)
                    grads.append([xp - xm, yp - ym, up - down])
                    smooth = 6.0 * here - ((xp + xm) + (yp + ym) + (up + down))
                    base[m, x, at, :] = wgt[m, x, at, :] * (here - tgt[m, x, at, :]) + smooth
                parts = flux_part(grads[0], grads[1], None)
                for m in range(MODELS):
                    flux0[x + 1, m, at, :] = parts[0][m]
                    flux1[x, m, at, :] = parts[1][m]
                    flux2[x, m, at, :] = parts[2][m]
            return carry

        fluxes(cx, 0)
        over_x(fluxes, 0, FLUX)

        def no_plane(x):
            for m in range(MODELS):
                for r in range(0, rows, 8):
                    flux0[x + 1, m, pl.ds(r, 8), :] = zero

        def no_row(y):
            for x in range(cx + 1):
                for m in range(MODELS):
                    flux1[x, m, pl.ds(YO + y, 1), :] = zero[0:1]

        pl.when(gx == 0)(lambda: no_plane(-1))
        pl.when(gx == nx - 1)(lambda: no_plane(cx))
        pl.when(gy == 0)(lambda: no_row(-1))
        pl.when(gy == ny - 1)(lambda: no_row(cy))

        def gradient(x, m, r):
            at = pl.ds(YO + r, 8)
            here = flux2[x, m, at, :]
            up, down = z_pair(here, edge(z_flux[2, m, at, :], x))
            div = (flux0[x + 2, m, at, :] - flux0[x, m, at, :]
                   + (flux1[x, m, pl.ds(YO + r + 1, 8), :] - flux1[x, m, pl.ds(YO + r - 1, 8), :]) + (up - down))
            return base[m, x, at, :] + KAPPA * div

        def gradients(x, norm):
            for t in range(tiles):
                for m in range(MODELS):
                    grad = gradient(x, m, 8 * t)
                    field[k, x + XO, m, pl.ds(YO + 8 * t, 8), :] = grad
                    norm = norm + grad * grad
            for m in range(MODELS):
                grad = gradient(x, m, cy)[0:1]
                field[k, x + XO, m, pl.ds(YO + cy, 1), :] = jnp.where(gy < ny - 1, grad, 0.0)
            return norm

        norm = over_x(gradients, zero, GRADIENT)

        if final:
            start_copies(k, [0, 2], True)
        for t in range(tiles):
            for m in range(MODELS):
                field[k, cx + XO, m, pl.ds(YO + 8 * t, 8), :] = jnp.where(gx < nx - 1, gradient(cx, m, 8 * t), 0.0)
        for t in range(tiles):
            for m in range(MODELS):
                def shifted(ref, i, dy=0):
                    return ref[i, m, pl.ds(YO + 8 * t + dy, 8), :]

                here, f0, f2 = shifted(z_field, 0), shifted(z_flux, 0), shifted(z_flux, 2)
                div = (turn(f0, -SPAN) - turn(f0, SPAN) + (shifted(z_flux, 1, 1) - shifted(z_flux, 1, -1))
                       + (turn(f2, -1) - turn(f2, 1)))
                around = ((turn(here, -SPAN) + turn(here, SPAN)) + (shifted(z_field, 0, 1) + shifted(z_field, 0, -1))
                          + (turn(here, -1) + turn(here, 1)))
                misfit = z_fixed[1, 0, m, pl.ds(8 * t, 8), :] * (here - z_fixed[1, 1, m, pl.ds(8 * t, 8), :])
                z_grad[m, pl.ds(YO + 8 * t, 8), :] = misfit + (6.0 * here - around) + KAPPA * div

        inside_up = (gz == 0).astype(jnp.float32)

        def curves(x, curve):
            for t in range(tiles):
                for m in range(MODELS):
                    here = tile_of(k, x, m, 8 * t)
                    e = edge(z_grad[m, pl.ds(YO + 8 * t, 8), :], x) * inside_up
                    up = jnp.where(last_lane, e, turn(here, cz - 1))
                    pairs = tile_of(k, x + 1, m, 8 * t) + tile_of(k, x, m, 8 * t + 1) + up
                    curve = curve + here * ((wgt[m, x, pl.ds(YO + 8 * t, 8), :] + 6.0) * here - 2.0 * pairs)
            return curve

        curve = over_x(curves, zero, CURVE)

        def fold(v):
            v = jnp.sum(v, axis=0, keepdims=True)
            return v + turn(v, cz // 2)

        both = jnp.where(lane[0:1] < cz // 2, fold(norm), fold(curve))
        own[k - 1] = both
        got[k - 1, pl.ds(len(others), 1), :] = both
        if k == 1:
            pl.semaphore_wait(enter_sem.at[1], len(line_z))
        start_sum(k - 1)
        if final:
            wait_copies(k, [0, 2], True)

            def applies(x, carry):
                for t in range(tiles):
                    for m in range(MODELS):
                        here = tile_of(k, x, m, 8 * t)
                        up, down = z_pair(here, edge(z_grad[m, pl.ds(YO + 8 * t, 8), :], x))
                        around = ((tile_of(k, x + 1, m, 8 * t) + tile_of(k, x - 1, m, 8 * t))
                                  + (tile_of(k, x, m, 8 * t + 1) + tile_of(k, x, m, 8 * t - 1)) + (up + down))
                        applied_out[m, x, pl.ds(8 * t, 8), :] = (
                            wgt[m, x, pl.ds(YO + 8 * t, 8), :] * here + (6.0 * here - around))
                return carry

            over_x(applies, 0, APPLY)
        else:
            start_copies(k, plain)
            pack_field(k)
            start_copies(k, through_z)
            wait_copies(k, through_z)
            join_z(k)
            wait_copies(k, plain)
        whole_sum(k - 1).wait_recv()
        partial = [got[k - 1, pl.ds(r, 8), :] for r in range(0, len(others) + 1, 8)]
        while len(partial) > 1:
            partial = [sum(partial[i:i + 2]) for i in range(0, len(partial), 2)]
        half = lane < cz // 2
        sums = [jnp.sum(jnp.sum(jnp.where(half, *terms), axis=0, keepdims=True), axis=1, keepdims=True)
                for terms in ((partial[0], 0.0), (0.0, partial[0]))]
        alpha = jnp.broadcast_to(sums[0] / sums[1], (8, cz))

        if k == 1:
            wait_sent(0, plain + through_z)
            for copy, sends, _ in fixed:
                guarded(sends, copy.wait_send)
        if final:
            wait_sent(k, [0, 2], True)
        else:
            wait_sent(k, plain + through_z)
        whole_sum(k - 1).wait_send()

        if final:
            def step(x, carry):
                for m in range(MODELS):
                    for t in range(tiles):
                        updated[m, x, pl.ds(8 * t, 8), :] = tile_of(0, x, m, 8 * t) - alpha * tile_of(k, x, m, 8 * t)
                return carry

            over_x(step, 0, STEP)
        else:
            def step(x, carry):
                for m in range(MODELS):
                    for r in range(0, rows, 8):
                        field[0, x, m, pl.ds(r, 8), :] = (
                            field[0, x, m, pl.ds(r, 8), :] - alpha * field[k, x, m, pl.ds(r, 8), :])
                return carry

            lax.fori_loop(0, cx + LOW + HIGH, step, 0)
            for m in range(MODELS):
                for r in range(0, rows, 8):
                    z_field[0, m, pl.ds(r, 8), :] = z_field[0, m, pl.ds(r, 8), :] - alpha * z_field[1, m, pl.ds(r, 8), :]


def solution(mesh):
    sizes = (mesh.shape["gx"], mesh.shape["gy"], mesh.shape["gz"])
    nx, ny, nz = sizes

    def local(models, targets, weights):
        _, cx, cy, cz = models.shape
        assert nz == 2 and nx % 4 == 0 and cy % 8 == 0
        assert SPAN * (cx + 4) <= cz and 16 * MODELS * (cy // 8) <= cz
        f32 = jnp.float32
        rows = YO + cy + 8

        def vmem(*shape):
            return pltpu.VMEM(shape, f32)

        return pl.pallas_call(
            functools.partial(kernel, sizes),
            out_shape=[jax.ShapeDtypeStruct(models.shape, f32)] * 2,
            in_specs=[pl.BlockSpec(memory_space=pltpu.HBM)] * 3,
            out_specs=[pl.BlockSpec(memory_space=pltpu.VMEM)] * 2,
            scratch_shapes=[
                vmem(ITERS + 1, cx + LOW + HIGH, MODELS, rows, cz),
                vmem(MODELS, cx + 1, rows, cz),
                vmem(MODELS, cx + 1, rows, cz),
                vmem(MODELS, cx + 1, rows, cz),
                vmem(cx + 3, MODELS, rows, cz),
                vmem(cx + 1, MODELS, rows + 8, cz),
                vmem(cx + 1, MODELS, rows, cz),
                vmem(ITERS + 1, MODELS, rows, cz),
                vmem(ITERS + 1, MODELS, rows, cz),
                vmem(2, MODELS, rows, cz),
                vmem(3, MODELS, rows, cz),
                vmem(MODELS, rows, cz),
                vmem(2, 2, MODELS, cy, cz),
                vmem(ITERS + 1, 2, 8, cz),
                vmem(ITERS + 1, 2, 2, 8, cz),
                vmem(ITERS + 1, 4, MODELS, 8, cz),
                vmem(ITERS, 1, cz),
                vmem(ITERS, nx * ny * nz, cz),
                pltpu.SemaphoreType.DMA((4,)),
                pltpu.SemaphoreType.DMA((ITERS + 1, 21)),
                pltpu.SemaphoreType.DMA((ITERS + 1, 21)),
                pltpu.SemaphoreType.DMA((5,)),
                pltpu.SemaphoreType.DMA((5,)),
                pltpu.SemaphoreType.DMA((ITERS,)),
                pltpu.SemaphoreType.DMA((ITERS,)),
                pltpu.SemaphoreType.REGULAR((2,)),
            ],
            compiler_params=pltpu.CompilerParams(
                collective_id=0, has_side_effects=True, vmem_limit_bytes=24 * 2**20),
        )(*[pltpu.with_memory_space_constraint(a, pltpu.HBM) for a in (models, targets, weights)])

    spec = P(None, "gx", "gy", "gz")
    return jax.shard_map(local, mesh=mesh, in_specs=(spec,) * 3, out_specs=(spec,) * 2, check_vma=False)
```

```python
import functools

import jax
import jax.numpy as jnp
from jax import lax
from jax.experimental import pallas as pl
from jax.experimental.pallas import tpu as pltpu
from jax.sharding import PartitionSpec as P

ITERS = 3
MESH = pl.DeviceIdType.MESH
MODELS = 2
XO = 2
YO = 8
LOW, HIGH = 2, 3
SPAN = 5
FLUX, GRADIENT, CURVE, PACK, APPLY, STEP = 4, 4, 8, 4, 4, 4
KAPPA = 0.05 * -2.0 * 0.5 * 0.125


def kernel(sizes, models, targets, weights, updated, applied_out,
           field, tgt, wgt, base, flux0, flux1, flux2, z_own, z_got, z_field, z_flux, z_grad, z_fixed,
           x_own, x_got, corner, own, got,
           load_sem, send_sem, recv_sem, fixed_send, fixed_recv, sum_send, sum_recv, enter_sem):
    nx, ny, nz = sizes
    _, cx, cy, cz = updated.shape
    tiles = cy // 8
    rows = field.shape[3]
    wide = tiles + 1
    gx, gy, gz = lax.axis_index("gx"), lax.axis_index("gy"), lax.axis_index("gz")

    faces = [(1, 0, 0), (-1, 0, 0), (0, 1, 0), (0, -1, 0), (1, 1, 0), (1, -1, 0), (-1, 1, 0), (-1, -1, 0)]
    z_faces = [(0, 0, 1), (1, 0, 0), (-1, 0, 0), (1, 0, 1), (-1, 0, 1), (0, 1, 0), (0, -1, 0), (0, 1, 1), (0, -1, 1),
               (1, 1, 1), (1, -1, 1), (-1, 1, 1), (-1, -1, 1)]
    corners = z_faces[9:]

    def there(ox, oy):
        ok = None
        for place, step, count in ((gx, ox, nx), (gy, oy, ny)):
            if step != 0:
                here = place < count - 1 if step > 0 else place > 0
                ok = here if ok is None else jnp.logical_and(ok, here)
        return ok

    def guarded(ok, action):
        if ok is None:
            action()
        else:
            pl.when(ok)(action)

    def device(ox, oy, oz):
        return {"gx": gx + ox, "gy": gy + oy, "gz": gz + oz - 2 * oz * gz}

    def slices(step, offset, count, skip, depth):
        if step > 0:
            return pl.ds(offset + count - LOW, LOW), pl.ds(offset - LOW, LOW)
        if step < 0:
            return pl.ds(offset + skip, depth - skip), pl.ds(offset + count + skip, depth - skip)
        return pl.ds(offset, count), pl.ds(offset, count)

    def message(k, j, last=False):
        if j < len(faces):
            ox, oy, oz = faces[j]
            if last:
                x_src, x_dst = (pl.ds(XO + cx - 1, 1), pl.ds(XO - 1, 1)) if ox else (pl.ds(XO, cx),) * 2
                y_src, y_dst = (pl.ds(YO + cy - 1, 1), pl.ds(YO - 1, 1)) if oy else (pl.ds(YO, cy),) * 2
            else:
                edge_of = ox != 0 and oy != 0
                skip, depth = (0, 2) if edge_of else (0 if k == 0 else 1, HIGH)
                x_src, x_dst = slices(ox, XO, cx, skip, depth)
                y_src, y_dst = slices(oy, YO, cy, skip, depth)
            src, dst = field.at[k, x_src, :, y_src, :], field.at[k, x_dst, :, y_dst, :]
        else:
            ox, oy, oz = offset = z_faces[j - len(faces)]
            y_src, y_dst = slices(oy, YO, cy, 0, 2)
            into = z_got if oz else z_own
            if ox and oy:
                line = YO + cy - 1 if oy > 0 else YO
                src, dst = z_own.at[k, :, pl.ds(line, 1), :], corner.at[k, corners.index(offset), :, pl.ds(0, 1), :]
            elif ox:
                src, dst = x_own.at[k, 0 if ox > 0 else 1], x_got.at[k, 0 if ox > 0 else 1, oz]
            else:
                src, dst = z_own.at[k, :, y_src, :], into.at[k, :, y_dst, :]
        return pltpu.make_async_remote_copy(
            src_ref=src, dst_ref=dst, send_sem=send_sem.at[k, j], recv_sem=recv_sem.at[k, j],
            device_id=device(ox, oy, oz), device_id_type=MESH)

    everything = faces + z_faces
    plain = list(range(len(faces)))
    through_z = list(range(len(faces), len(everything)))

    def start_copies(k, which, last=False):
        for j in which:
            guarded(there(*everything[j][:2]), lambda j=j: message(k, j, last).start())

    def wait_copies(k, which, last=False):
        for j in which:
            ox, oy, _ = everything[j]
            guarded(there(-ox, -oy), lambda j=j: message(k, j, last).wait_recv())

    def wait_sent(k, which, last=False):
        for j in which:
            guarded(there(*everything[j][:2]), lambda j=j: message(k, j, last).wait_send())

    def fixed_message(j):
        array = (wgt, tgt)[j % 2]
        if j < 2:
            ox, oy, oz = -1, 0, 0
            src, dst = array.at[:, pl.ds(0, 1), pl.ds(YO, cy), :], array.at[:, pl.ds(cx, 1), pl.ds(YO, cy), :]
        elif j < 4:
            ox, oy, oz = 0, -1, 0
            src, dst = array.at[:, pl.ds(0, cx), pl.ds(YO, 1), :], array.at[:, pl.ds(0, cx), pl.ds(YO + cy, 1), :]
        else:
            ox, oy, oz = 0, 0, 1
            src, dst = z_fixed.at[0], z_fixed.at[1]
        return pltpu.make_async_remote_copy(
            src_ref=src, dst_ref=dst, send_sem=fixed_send.at[j], recv_sem=fixed_recv.at[j],
            device_id=device(ox, oy, oz), device_id_type=MESH), there(ox, oy), there(-ox, -oy)

    pair, quad, chip_z = lax.rem(gx, 2), lax.rem(lax.div(gx, 2), 2), lax.div(gx, 4)
    turns_z = nx // 4

    def hops(offset):
        x, z, h, q, c = offset
        return min(x, ny - x) + min(z, turns_z - z) + (1 if q else 2 * h), c

    others = [(x, z, h, q, c) for x in range(ny) for z in range(turns_z) for h in range(nz) for q in range(2) for c in range(2)]
    others = sorted(others, key=hops, reverse=True)[:-1]
    place_x = [lax.rem(gy + x, ny) if x else gy for x in range(ny)]
    place_h = [gz, 1 - gz]
    place_gx = {(z, q, c): 4 * (lax.rem(chip_z + z, turns_z) if z else chip_z) + 2 * (1 - quad if q else quad) + (1 - pair if c else pair)
                for z in range(turns_z) for q in range(2) for c in range(2)}

    def start_sum(k, which):
        for j in which:
            x, z, h, q, c = others[j]
            pltpu.make_async_remote_copy(
                src_ref=own.at[k], dst_ref=got.at[k, pl.ds(j, 1)], send_sem=sum_send.at[k], recv_sem=sum_recv.at[k],
                device_id={"gx": place_gx[z, q, c], "gy": place_x[x], "gz": place_h[h]}, device_id_type=MESH).start()

    def whole_sum(k):
        landed = got.at[k, pl.ds(0, len(others))]
        return pltpu.make_async_remote_copy(
            src_ref=landed, dst_ref=landed, send_sem=sum_send.at[k], recv_sem=sum_recv.at[k],
            device_id={"gx": gx, "gy": gy, "gz": 1 - gz}, device_id_type=MESH)

    def on_line(x, y, z):
        return {"gx": x, "gy": y, "gz": z}

    line_x = [on_line(gx + c - 2 * c * pair, lax.rem(gy + s, ny), gz)
              for s in range(ny) for c in range(2) if (c, s) != (0, 0)]
    line_y = [on_line(gx + 2 * h - 4 * h * quad, gy, gz + s - 2 * s * gz)
              for s in range(nz) for h in range(2) if (h, s) != (0, 0)]
    line_z = [on_line(lax.rem(gx + 4 * s, nx), gy, gz) for s in range(1, nx // 4)]

    def tell(sem, line):
        for device in line:
            pl.semaphore_signal(sem, 1, device_id=device, device_id_type=MESH)

    inner = pl.ds(YO, cy)
    loads = [pltpu.make_async_copy(models.at[m], field.at[0, pl.ds(XO, cx), m, inner, :], load_sem.at[m]) for m in range(MODELS)]
    loads.append(pltpu.make_async_copy(targets, tgt.at[:, pl.ds(0, cx), inner, :], load_sem.at[2]))
    loads.append(pltpu.make_async_copy(weights, wgt.at[:, pl.ds(0, cx), inner, :], load_sem.at[3]))
    for copy in loads:
        copy.start()

    zero = jnp.zeros((8, cz), jnp.float32)

    def clear_planes(start, count, side):
        for k in range(ITERS + 1):
            for x in range(start, start + count):
                for m in range(MODELS):
                    for r in range(0, rows, 8):
                        field[k, x, m, pl.ds(r, 8), :] = zero
            for oz in range(2):
                x_got[k, side, oz] = zero

    def clear_rows(start):
        def clear(x, _):
            for k in range(ITERS + 1):
                for m in range(MODELS):
                    field[k, x, m, pl.ds(start, 8), :] = zero
            return 0

        lax.fori_loop(0, cx + LOW + HIGH, clear, 0)
        for k in range(ITERS + 1):
            for m in range(MODELS):
                z_own[k, m, pl.ds(start, 8), :] = zero
                z_got[k, m, pl.ds(start, 8), :] = zero

    def clear_corner(j):
        for k in range(ITERS + 1):
            for m in range(MODELS):
                corner[k, j, m] = zero

    for j, (ox, oy, _) in enumerate(corners):
        pl.when(jnp.logical_not(there(-ox, -oy)))(functools.partial(clear_corner, j))
    pl.when(gx == 0)(lambda: clear_planes(0, LOW, 0))
    pl.when(gx == nx - 1)(lambda: clear_planes(XO + cx, HIGH, 1))
    pl.when(gy == 0)(lambda: clear_rows(0))
    pl.when(gy == ny - 1)(lambda: clear_rows(rows - 8))

    barrier = pltpu.get_barrier_semaphore()
    expected = len(line_x) + len(line_y) + len(line_z)
    for ox, oy, oz in dict.fromkeys(everything):
        ok = there(ox, oy)
        guarded(ok, lambda ox=ox, oy=oy, oz=oz: pl.semaphore_signal(
            barrier, 1, device_id=device(ox, oy, oz), device_id_type=MESH))
        expected = expected + (1 if ok is None else ok.astype(jnp.int32))
    for line in (line_x, line_y, line_z):
        tell(barrier, line)

    lane = lax.broadcasted_iota(jnp.int32, (8, cz), 1)
    first, last_lane = lane == 0, lane == cz - 1
    end_lane = (1 - gz) * (cz - 1)
    ghost_lane = lane == end_lane
    upward = 1 - 2 * gz
    beyond = (lax.rem(lane, SPAN) - 2) * upward >= 0
    beyond_x = (lax.rem(lax.rem(lane, 16), SPAN) - 2) * upward >= 0
    to_own = jnp.where(gz == 0, cz - 1, 1)

    def turn(v, shift):
        if isinstance(shift, int):
            shift = shift % cz
            return v if shift == 0 else pltpu.roll(v, shift, 1)
        return pltpu.roll(v, shift, 1)

    def edge(lines, x):
        return jnp.where(ghost_lane, turn(lines, lax.rem(cz + end_lane - SPAN * (x + 2) - 2, cz)), 0.0)

    def z_pair(v, e):
        return jnp.where(last_lane, e, turn(v, cz - 1)), jnp.where(first, e, turn(v, 1))

    def pack(acc, v, x):
        return jnp.where(lax.div(lane, SPAN) == x + 2, turn(v, lax.rem(SPAN * (x + 2) + 3 - gz, cz)), acc)

    def tile_of(k, x, m, r):
        return field[k, x + XO, m, pl.ds(YO + r, 8), :]

    def over_x(body, carry, unroll):
        def block(b, carry):
            for u in range(unroll):
                carry = body(b * unroll + u, carry)
            return carry

        return lax.fori_loop(0, cx // unroll, block, carry)

    def pack_all(read, write):
        def planes(x, acc):
            return tuple(pack(a, read(x, m, t), x) for a, (m, t) in zip(acc, order))

        order = [(m, t) for m in range(MODELS) for t in range(tiles)]
        for a, (m, t) in zip(over_x(planes, (zero,) * len(order), PACK), order):
            write(m, t, a)

    def pack_field(k):
        def write(m, t, v):
            z_own[k, m, pl.ds(YO + 8 * t, 8), :] = v

        pack_all(lambda x, m, t: tile_of(k, x, m, 8 * t), write)
        high, low = zero, zero
        for m in range(MODELS):
            for t in range(tiles):
                i = m * tiles + t
                v, mine = z_own[k, m, pl.ds(YO + 8 * t, 8), :], lax.div(lane, 16) == i
                high = jnp.where(mine, turn(v, 16 * i - SPAN * cx), high)
                low = jnp.where(mine, turn(v, 16 * i - 2 * SPAN), low)
        x_own[k, 0] = high
        x_own[k, 1] = low

    def join_z(k):
        low, high = [jnp.where(beyond_x, x_got[k, side, 1], turn(x_got[k, side, 0], to_own)) for side in range(2)]

        def inside(m, r):
            return jnp.where(beyond, z_got[k, m, pl.ds(r, 8), :], turn(z_own[k, m, pl.ds(r, 8), :], to_own))

        def with_x(v, before, after):
            return jnp.where(lane < 2 * SPAN, before, jnp.where(lane < SPAN * (cx + 2), v, after))

        for m in range(MODELS):
            for t in range(tiles):
                i = m * tiles + t
                z_field[min(k, 1), m, pl.ds(YO + 8 * t, 8), :] = with_x(
                    inside(m, YO + 8 * t), turn(low, -16 * i), turn(high, SPAN * (cx + 2) - 16 * i))
            for r, oy in ((0, 1), (YO + cy, -1)):
                before, after = [turn(jnp.broadcast_to(corner[k, corners.index((ox, oy, 1)), m, pl.ds(0, 1), :], (8, cz)),
                                      -ox * SPAN * cx) for ox in (1, -1)]
                z_field[min(k, 1), m, pl.ds(r, 8), :] = with_x(inside(m, r), before, after)

    def cross_part(a, b, i):
        j, l = (i + 1) % 3, (i + 2) % 3
        return a[j] * b[l] - a[l] * b[j]

    def flux_part(g1, g2, which):
        crossed = [None if i == which else cross_part(g1, g2, i) for i in range(3)]
        return [(cross_part(g2, crossed, i), cross_part(crossed, g1, i)) for i in (range(3) if which is None else [which])]

    for copy in loads[:MODELS]:
        copy.wait()
    pack_field(0)
    pl.semaphore_wait(barrier, expected)
    start_copies(0, through_z)
    start_copies(0, plain)
    tell(enter_sem.at[0], line_y)
    for copy in loads[MODELS:]:
        copy.wait()
    for a, array in enumerate((wgt, tgt)):
        def write(m, t, v, a=a):
            z_fixed[0, a, m, pl.ds(8 * t, 8), :] = v

        pack_all(lambda x, m, t, array=array: array[m, x, pl.ds(YO + 8 * t, 8), :], write)
    fixed = [fixed_message(j) for j in range(5)]
    for copy, sends, _ in fixed:
        guarded(sends, copy.start)
    wait_copies(0, through_z)
    join_z(0)
    wait_copies(0, plain)
    pl.semaphore_wait(enter_sem.at[0], len(line_y))
    tell(enter_sem.at[1], line_z)
    for copy, _, receives in fixed:
        guarded(receives, copy.wait_recv)

    for k in range(1, ITERS + 1):
        final = k == ITERS
        for j in range(wide):
            grads = []
            for m in range(MODELS):
                here = z_field[0, m, pl.ds(YO - 1 + 8 * j, 8), :]
                grads.append([turn(here, -SPAN) - turn(here, SPAN),
                              z_field[0, m, pl.ds(YO + 8 * j, 8), :] - z_field[0, m, pl.ds(YO - 2 + 8 * j, 8), :],
                              turn(here, -1) - turn(here, 1)])
            for i, parts in enumerate(flux_part(grads[0], grads[1], None)):
                for m in range(MODELS):
                    z_flux[i, m, pl.ds(YO - 1 + 8 * j, 8), :] = parts[m]

        for x in (-1, cx + 1):
            for j in range(wide):
                grads = []
                for m in range(MODELS):
                    here = tile_of(0, x, m, 8 * j - 1)
                    up, down = z_pair(here, edge(z_field[0, m, pl.ds(YO - 1 + 8 * j, 8), :], x))
                    grads.append([tile_of(0, x + 1, m, 8 * j - 1) - tile_of(0, x - 1, m, 8 * j - 1),
                                  tile_of(0, x, m, 8 * j) - tile_of(0, x, m, 8 * j - 2), up - down])
                parts = flux_part(grads[0], grads[1], 0)[0]
                for m in range(MODELS):
                    flux0[x + 1, m, pl.ds(YO - 1 + 8 * j, 8), :] = parts[m]

        def fluxes(x, carry):
            for j in range(wide):
                grads = []
                at = pl.ds(YO - 1 + 8 * j, 8)
                for m in range(MODELS):
                    here = tile_of(0, x, m, 8 * j - 1)
                    up, down = z_pair(here, edge(z_field[0, m, at, :], x))
                    xp, xm = tile_of(0, x + 1, m, 8 * j - 1), tile_of(0, x - 1, m, 8 * j - 1)
                    yp, ym = tile_of(0, x, m, 8 * j), tile_of(0, x, m, 8 * j - 2)
                    grads.append([xp - xm, yp - ym, up - down])
                    smooth = 6.0 * here - ((xp + xm) + (yp + ym) + (up + down))
                    base[m, x, at, :] = wgt[m, x, at, :] * (here - tgt[m, x, at, :]) + smooth
                parts = flux_part(grads[0], grads[1], None)
                for m in range(MODELS):
                    flux0[x + 1, m, at, :] = parts[0][m]
                    flux1[x, m, at, :] = parts[1][m]
                    flux2[x, m, at, :] = parts[2][m]
            return carry

        fluxes(cx, 0)
        over_x(fluxes, 0, FLUX)

        def no_plane(x):
            for m in range(MODELS):
                for r in range(0, rows, 8):
                    flux0[x + 1, m, pl.ds(r, 8), :] = zero

        def no_row(y):
            for x in range(cx + 1):
                for m in range(MODELS):
                    flux1[x, m, pl.ds(YO + y, 1), :] = zero[0:1]

        pl.when(gx == 0)(lambda: no_plane(-1))
        pl.when(gx == nx - 1)(lambda: no_plane(cx))
        pl.when(gy == 0)(lambda: no_row(-1))
        pl.when(gy == ny - 1)(lambda: no_row(cy))

        def gradient(x, m, r):
            at = pl.ds(YO + r, 8)
            here = flux2[x, m, at, :]
            up, down = z_pair(here, edge(z_flux[2, m, at, :], x))
            div = (flux0[x + 2, m, at, :] - flux0[x, m, at, :]
                   + (flux1[x, m, pl.ds(YO + r + 1, 8), :] - flux1[x, m, pl.ds(YO + r - 1, 8), :]) + (up - down))
            return base[m, x, at, :] + KAPPA * div

        def gradients(x, norm):
            for t in range(tiles):
                for m in range(MODELS):
                    grad = gradient(x, m, 8 * t)
                    field[k, x + XO, m, pl.ds(YO + 8 * t, 8), :] = grad
                    norm = norm + grad * grad
            for m in range(MODELS):
                grad = gradient(x, m, cy)[0:1]
                field[k, x + XO, m, pl.ds(YO + cy, 1), :] = jnp.where(gy < ny - 1, grad, 0.0)
            return norm

        norm = over_x(gradients, zero, GRADIENT)

        if final:
            start_copies(k, [0, 2], True)
        for t in range(tiles):
            for m in range(MODELS):
                field[k, cx + XO, m, pl.ds(YO + 8 * t, 8), :] = jnp.where(gx < nx - 1, gradient(cx, m, 8 * t), 0.0)
        for t in range(tiles):
            for m in range(MODELS):
                def shifted(ref, i, dy=0):
                    return ref[i, m, pl.ds(YO + 8 * t + dy, 8), :]

                here, f0, f2 = shifted(z_field, 0), shifted(z_flux, 0), shifted(z_flux, 2)
                div = (turn(f0, -SPAN) - turn(f0, SPAN) + (shifted(z_flux, 1, 1) - shifted(z_flux, 1, -1))
                       + (turn(f2, -1) - turn(f2, 1)))
                around = ((turn(here, -SPAN) + turn(here, SPAN)) + (shifted(z_field, 0, 1) + shifted(z_field, 0, -1))
                          + (turn(here, -1) + turn(here, 1)))
                misfit = z_fixed[1, 0, m, pl.ds(8 * t, 8), :] * (here - z_fixed[1, 1, m, pl.ds(8 * t, 8), :])
                z_grad[m, pl.ds(YO + 8 * t, 8), :] = misfit + (6.0 * here - around) + KAPPA * div

        inside_up = (gz == 0).astype(jnp.float32)

        def curves(x, curve):
            for t in range(tiles):
                for m in range(MODELS):
                    here = tile_of(k, x, m, 8 * t)
                    e = edge(z_grad[m, pl.ds(YO + 8 * t, 8), :], x) * inside_up
                    up = jnp.where(last_lane, e, turn(here, cz - 1))
                    pairs = tile_of(k, x + 1, m, 8 * t) + tile_of(k, x, m, 8 * t + 1) + up
                    curve = curve + here * ((wgt[m, x, pl.ds(YO + 8 * t, 8), :] + 6.0) * here - 2.0 * pairs)
            return curve

        curve = over_x(curves, zero, CURVE)

        def fold(v):
            v = jnp.sum(v, axis=0, keepdims=True)
            return v + turn(v, cz // 2)

        both = jnp.where(lane[0:1] < cz // 2, fold(norm), fold(curve))
        own[k - 1] = both
        got[k - 1, pl.ds(len(others), 1), :] = both
        if k == 1:
            pl.semaphore_wait(enter_sem.at[1], len(line_z))
        far_ones = len(others) * 2 // 3
        start_sum(k - 1, range(far_ones))
        if not final:
            start_copies(k, plain)
            pack_field(k)
            start_copies(k, through_z)
        start_sum(k - 1, range(far_ones, len(others)))
        if final:
            wait_copies(k, [0, 2], True)

            def applies(x, carry):
                for t in range(tiles):
                    for m in range(MODELS):
                        here = tile_of(k, x, m, 8 * t)
                        up, down = z_pair(here, edge(z_grad[m, pl.ds(YO + 8 * t, 8), :], x))
                        around = ((tile_of(k, x + 1, m, 8 * t) + tile_of(k, x - 1, m, 8 * t))
                                  + (tile_of(k, x, m, 8 * t + 1) + tile_of(k, x, m, 8 * t - 1)) + (up + down))
                        applied_out[m, x, pl.ds(8 * t, 8), :] = (
                            wgt[m, x, pl.ds(YO + 8 * t, 8), :] * here + (6.0 * here - around))
                return carry

            over_x(applies, 0, APPLY)
        else:
            wait_copies(k, through_z)
            join_z(k)
            wait_copies(k, plain)
        whole_sum(k - 1).wait_recv()
        partial = [got[k - 1, pl.ds(r, 8), :] for r in range(0, len(others) + 1, 8)]
        while len(partial) > 1:
            partial = [sum(partial[i:i + 2]) for i in range(0, len(partial), 2)]
        half = lane < cz // 2
        sums = [jnp.sum(jnp.sum(jnp.where(half, *terms), axis=0, keepdims=True), axis=1, keepdims=True)
                for terms in ((partial[0], 0.0), (0.0, partial[0]))]
        alpha = jnp.broadcast_to(sums[0] / sums[1], (8, cz))

        if k == 1:
            wait_sent(0, plain + through_z)
            for copy, sends, _ in fixed:
                guarded(sends, copy.wait_send)
        if final:
            wait_sent(k, [0, 2], True)
        else:
            wait_sent(k, plain + through_z)
        whole_sum(k - 1).wait_send()

        if final:
            def step(x, carry):
                for m in range(MODELS):
                    for t in range(tiles):
                        updated[m, x, pl.ds(8 * t, 8), :] = tile_of(0, x, m, 8 * t) - alpha * tile_of(k, x, m, 8 * t)
                return carry

            over_x(step, 0, STEP)
        else:
            def step(x, carry):
                for m in range(MODELS):
                    for r in range(0, rows, 8):
                        field[0, x, m, pl.ds(r, 8), :] = (
                            field[0, x, m, pl.ds(r, 8), :] - alpha * field[k, x, m, pl.ds(r, 8), :])
                return carry

            lax.fori_loop(0, cx + LOW + HIGH, step, 0)
            for m in range(MODELS):
                for r in range(0, rows, 8):
                    z_field[0, m, pl.ds(r, 8), :] = z_field[0, m, pl.ds(r, 8), :] - alpha * z_field[1, m, pl.ds(r, 8), :]


def store(updated, applied, updated_out, applied_out, sems):
    copies = [pltpu.make_async_copy(updated, updated_out, sems.at[0]), pltpu.make_async_copy(applied, applied_out, sems.at[1])]
    for copy in copies:
        copy.start()
    for copy in copies:
        copy.wait()


def solution(mesh):
    sizes = (mesh.shape["gx"], mesh.shape["gy"], mesh.shape["gz"])
    nx, ny, nz = sizes

    def local(models, targets, weights):
        _, cx, cy, cz = models.shape
        assert nz == 2 and nx % 4 == 0 and cy % 8 == 0
        assert SPAN * (cx + 4) <= cz and 16 * MODELS * (cy // 8) <= cz
        f32 = jnp.float32
        rows = YO + cy + 8

        def vmem(*shape):
            return pltpu.VMEM(shape, f32)

        results = pl.pallas_call(
            functools.partial(kernel, sizes),
            out_shape=[jax.ShapeDtypeStruct(models.shape, f32)] * 2,
            in_specs=[pl.BlockSpec(memory_space=pltpu.HBM)] * 3,
            out_specs=[pl.BlockSpec(memory_space=pltpu.VMEM)] * 2,
            scratch_shapes=[
                vmem(ITERS + 1, cx + LOW + HIGH, MODELS, rows, cz),
                vmem(MODELS, cx + 1, rows, cz),
                vmem(MODELS, cx + 1, rows, cz),
                vmem(MODELS, cx + 1, rows, cz),
                vmem(cx + 3, MODELS, rows, cz),
                vmem(cx + 1, MODELS, rows + 8, cz),
                vmem(cx + 1, MODELS, rows, cz),
                vmem(ITERS + 1, MODELS, rows, cz),
                vmem(ITERS + 1, MODELS, rows, cz),
                vmem(2, MODELS, rows, cz),
                vmem(3, MODELS, rows, cz),
                vmem(MODELS, rows, cz),
                vmem(2, 2, MODELS, cy, cz),
                vmem(ITERS + 1, 2, 8, cz),
                vmem(ITERS + 1, 2, 2, 8, cz),
                vmem(ITERS + 1, 4, MODELS, 8, cz),
                vmem(ITERS, 1, cz),
                vmem(ITERS, nx * ny * nz, cz),
                pltpu.SemaphoreType.DMA((4,)),
                pltpu.SemaphoreType.DMA((ITERS + 1, 21)),
                pltpu.SemaphoreType.DMA((ITERS + 1, 21)),
                pltpu.SemaphoreType.DMA((5,)),
                pltpu.SemaphoreType.DMA((5,)),
                pltpu.SemaphoreType.DMA((ITERS,)),
                pltpu.SemaphoreType.DMA((ITERS,)),
                pltpu.SemaphoreType.REGULAR((2,)),
            ],
            compiler_params=pltpu.CompilerParams(
                collective_id=0, has_side_effects=True, vmem_limit_bytes=24 * 2**20),
        )(*[pltpu.with_memory_space_constraint(a, pltpu.HBM) for a in (models, targets, weights)])
        return pl.pallas_call(
            store,
            out_shape=[jax.ShapeDtypeStruct(models.shape, f32)] * 2,
            in_specs=[pl.BlockSpec(memory_space=pltpu.VMEM)] * 2,
            out_specs=[pl.BlockSpec(memory_space=pltpu.HBM)] * 2,
            scratch_shapes=[pltpu.SemaphoreType.DMA((2,))],
        )(*[pltpu.with_memory_space_constraint(a, pltpu.VMEM) for a in results])

    spec = P(None, "gx", "gy", "gz")
    return jax.shard_map(local, mesh=mesh, in_specs=(spec,) * 3, out_specs=(spec,) * 2, check_vma=False)
```

```python
import functools

import jax
import jax.numpy as jnp
from jax import lax
from jax.experimental import pallas as pl
from jax.experimental.pallas import tpu as pltpu
from jax.sharding import PartitionSpec as P

ITERS = 3
MESH = pl.DeviceIdType.MESH
MODELS = 2
XO = 2
YO = 8
LOW, HIGH = 2, 3
SPAN = 5
FLUX, GRADIENT, CURVE, PACK, APPLY, STEP = 4, 4, 16, 4, 4, 8
KAPPA = 0.05 * -2.0 * 0.5 * 0.125


def kernel(sizes, models, targets, weights, updated, applied_out,
           field, tgt, wgt, base, flux0, flux1, flux2, z_own, z_got, z_field, z_flux, z_grad, z_fixed,
           x_own, x_got, corner, own, got,
           load_sem, send_sem, recv_sem, fixed_send, fixed_recv, sum_send, sum_recv, enter_sem):
    nx, ny, nz = sizes
    _, cx, cy, cz = updated.shape
    tiles = cy // 8
    rows = field.shape[3]
    wide = tiles + 1
    gx, gy, gz = lax.axis_index("gx"), lax.axis_index("gy"), lax.axis_index("gz")

    faces = [(1, 0, 0), (-1, 0, 0), (0, 1, 0), (0, -1, 0), (1, 1, 0), (1, -1, 0), (-1, 1, 0), (-1, -1, 0)]
    z_faces = [(0, 0, 1), (1, 0, 0), (-1, 0, 0), (1, 0, 1), (-1, 0, 1), (0, 1, 0), (0, -1, 0), (0, 1, 1), (0, -1, 1),
               (1, 1, 1), (1, -1, 1), (-1, 1, 1), (-1, -1, 1)]
    corners = z_faces[9:]

    def there(ox, oy):
        ok = None
        for place, step, count in ((gx, ox, nx), (gy, oy, ny)):
            if step != 0:
                here = place < count - 1 if step > 0 else place > 0
                ok = here if ok is None else jnp.logical_and(ok, here)
        return ok

    def guarded(ok, action):
        if ok is None:
            action()
        else:
            pl.when(ok)(action)

    def device(ox, oy, oz):
        return {"gx": gx + ox, "gy": gy + oy, "gz": gz + oz - 2 * oz * gz}

    def slices(step, offset, count, skip, depth):
        if step > 0:
            return pl.ds(offset + count - LOW, LOW), pl.ds(offset - LOW, LOW)
        if step < 0:
            return pl.ds(offset + skip, depth - skip), pl.ds(offset + count + skip, depth - skip)
        return pl.ds(offset, count), pl.ds(offset, count)

    def message(k, j, last=False):
        if j < len(faces):
            ox, oy, oz = faces[j]
            if last:
                x_src, x_dst = (pl.ds(XO + cx - 1, 1), pl.ds(XO - 1, 1)) if ox else (pl.ds(XO, cx),) * 2
                y_src, y_dst = (pl.ds(YO + cy - 1, 1), pl.ds(YO - 1, 1)) if oy else (pl.ds(YO, cy),) * 2
            else:
                edge_of = ox != 0 and oy != 0
                skip, depth = (0, 2) if edge_of else (0 if k == 0 else 1, HIGH)
                x_src, x_dst = slices(ox, XO, cx, skip, depth)
                y_src, y_dst = slices(oy, YO, cy, skip, depth)
            src, dst = field.at[k, x_src, :, y_src, :], field.at[k, x_dst, :, y_dst, :]
        else:
            ox, oy, oz = offset = z_faces[j - len(faces)]
            y_src, y_dst = slices(oy, YO, cy, 0, 2)
            into = z_got if oz else z_own
            if ox and oy:
                line = YO + cy - 1 if oy > 0 else YO
                src, dst = z_own.at[k, :, pl.ds(line, 1), :], corner.at[k, corners.index(offset), :, pl.ds(0, 1), :]
            elif ox:
                src, dst = x_own.at[k, 0 if ox > 0 else 1], x_got.at[k, 0 if ox > 0 else 1, oz]
            else:
                src, dst = z_own.at[k, :, y_src, :], into.at[k, :, y_dst, :]
        return pltpu.make_async_remote_copy(
            src_ref=src, dst_ref=dst, send_sem=send_sem.at[k, j], recv_sem=recv_sem.at[k, j],
            device_id=device(ox, oy, oz), device_id_type=MESH)

    everything = faces + z_faces
    plain = list(range(len(faces)))
    through_z = list(range(len(faces), len(everything)))

    def start_copies(k, which, last=False):
        for j in which:
            guarded(there(*everything[j][:2]), lambda j=j: message(k, j, last).start())

    def wait_copies(k, which, last=False):
        for j in which:
            ox, oy, _ = everything[j]
            guarded(there(-ox, -oy), lambda j=j: message(k, j, last).wait_recv())

    def wait_sent(k, which, last=False):
        for j in which:
            guarded(there(*everything[j][:2]), lambda j=j: message(k, j, last).wait_send())

    def fixed_message(j):
        array = (wgt, tgt)[j % 2]
        if j < 2:
            ox, oy, oz = -1, 0, 0
            src, dst = array.at[:, pl.ds(0, 1), pl.ds(YO, cy), :], array.at[:, pl.ds(cx, 1), pl.ds(YO, cy), :]
        elif j < 4:
            ox, oy, oz = 0, -1, 0
            src, dst = array.at[:, pl.ds(0, cx), pl.ds(YO, 1), :], array.at[:, pl.ds(0, cx), pl.ds(YO + cy, 1), :]
        else:
            ox, oy, oz = 0, 0, 1
            src, dst = z_fixed.at[0], z_fixed.at[1]
        return pltpu.make_async_remote_copy(
            src_ref=src, dst_ref=dst, send_sem=fixed_send.at[j], recv_sem=fixed_recv.at[j],
            device_id=device(ox, oy, oz), device_id_type=MESH), there(ox, oy), there(-ox, -oy)

    pair, quad, chip_z = lax.rem(gx, 2), lax.rem(lax.div(gx, 2), 2), lax.div(gx, 4)
    turns_z = nx // 4

    def hops(offset):
        x, z, h, q, c = offset
        return min(x, ny - x) + min(z, turns_z - z) + (1 if q else 2 * h), c

    others = [(x, z, h, q, c) for x in range(ny) for z in range(turns_z) for h in range(nz) for q in range(2) for c in range(2)]
    others = sorted(others, key=hops, reverse=True)[:-1]
    place_x = [lax.rem(gy + x, ny) if x else gy for x in range(ny)]
    place_h = [gz, 1 - gz]
    place_gx = {(z, q, c): 4 * (lax.rem(chip_z + z, turns_z) if z else chip_z) + 2 * (1 - quad if q else quad) + (1 - pair if c else pair)
                for z in range(turns_z) for q in range(2) for c in range(2)}

    def start_sum(k, which):
        for j in which:
            x, z, h, q, c = others[j]
            pltpu.make_async_remote_copy(
                src_ref=own.at[k], dst_ref=got.at[k, pl.ds(j, 1)], send_sem=sum_send.at[k], recv_sem=sum_recv.at[k],
                device_id={"gx": place_gx[z, q, c], "gy": place_x[x], "gz": place_h[h]}, device_id_type=MESH).start()

    def whole_sum(k):
        landed = got.at[k, pl.ds(0, len(others))]
        return pltpu.make_async_remote_copy(
            src_ref=landed, dst_ref=landed, send_sem=sum_send.at[k], recv_sem=sum_recv.at[k],
            device_id={"gx": gx, "gy": gy, "gz": 1 - gz}, device_id_type=MESH)

    def on_line(x, y, z):
        return {"gx": x, "gy": y, "gz": z}

    line_x = [on_line(gx + c - 2 * c * pair, lax.rem(gy + s, ny), gz)
              for s in range(ny) for c in range(2) if (c, s) != (0, 0)]
    line_y = [on_line(gx + 2 * h - 4 * h * quad, gy, gz + s - 2 * s * gz)
              for s in range(nz) for h in range(2) if (h, s) != (0, 0)]
    line_z = [on_line(lax.rem(gx + 4 * s, nx), gy, gz) for s in range(1, nx // 4)]

    def tell(sem, line):
        for device in line:
            pl.semaphore_signal(sem, 1, device_id=device, device_id_type=MESH)

    inner = pl.ds(YO, cy)
    loads = [pltpu.make_async_copy(models.at[m], field.at[0, pl.ds(XO, cx), m, inner, :], load_sem.at[m]) for m in range(MODELS)]
    loads.append(pltpu.make_async_copy(targets, tgt.at[:, pl.ds(0, cx), inner, :], load_sem.at[2]))
    loads.append(pltpu.make_async_copy(weights, wgt.at[:, pl.ds(0, cx), inner, :], load_sem.at[3]))
    for copy in loads:
        copy.start()

    zero = jnp.zeros((8, cz), jnp.float32)

    def clear_planes(start, count, side):
        for k in range(ITERS + 1):
            for x in range(start, start + count):
                for m in range(MODELS):
                    for r in range(0, rows, 8):
                        field[k, x, m, pl.ds(r, 8), :] = zero
            for oz in range(2):
                x_got[k, side, oz] = zero

    def clear_rows(start):
        def clear(x, _):
            for k in range(ITERS + 1):
                for m in range(MODELS):
                    field[k, x, m, pl.ds(start, 8), :] = zero
            return 0

        lax.fori_loop(0, cx + LOW + HIGH, clear, 0)
        for k in range(ITERS + 1):
            for m in range(MODELS):
                z_own[k, m, pl.ds(start, 8), :] = zero
                z_got[k, m, pl.ds(start, 8), :] = zero

    def clear_corner(j):
        for k in range(ITERS + 1):
            for m in range(MODELS):
                corner[k, j, m] = zero

    for j, (ox, oy, _) in enumerate(corners):
        pl.when(jnp.logical_not(there(-ox, -oy)))(functools.partial(clear_corner, j))
    pl.when(gx == 0)(lambda: clear_planes(0, LOW, 0))
    pl.when(gx == nx - 1)(lambda: clear_planes(XO + cx, HIGH, 1))
    pl.when(gy == 0)(lambda: clear_rows(0))
    pl.when(gy == ny - 1)(lambda: clear_rows(rows - 8))

    barrier = pltpu.get_barrier_semaphore()
    expected = len(line_x) + len(line_y) + len(line_z)
    for ox, oy, oz in dict.fromkeys(everything):
        ok = there(ox, oy)
        guarded(ok, lambda ox=ox, oy=oy, oz=oz: pl.semaphore_signal(
            barrier, 1, device_id=device(ox, oy, oz), device_id_type=MESH))
        expected = expected + (1 if ok is None else ok.astype(jnp.int32))
    for line in (line_x, line_y, line_z):
        tell(barrier, line)

    lane = lax.broadcasted_iota(jnp.int32, (8, cz), 1)
    first, last_lane = lane == 0, lane == cz - 1
    end_lane = (1 - gz) * (cz - 1)
    ghost_lane = lane == end_lane
    upward = 1 - 2 * gz
    beyond = (lax.rem(lane, SPAN) - 2) * upward >= 0
    beyond_x = (lax.rem(lax.rem(lane, 16), SPAN) - 2) * upward >= 0
    to_own = jnp.where(gz == 0, cz - 1, 1)

    def turn(v, shift):
        if isinstance(shift, int):
            shift = shift % cz
            return v if shift == 0 else pltpu.roll(v, shift, 1)
        return pltpu.roll(v, shift, 1)

    def edge(lines, x):
        return jnp.where(ghost_lane, turn(lines, lax.rem(cz + end_lane - SPAN * (x + 2) - 2, cz)), 0.0)

    def z_pair(v, e):
        return jnp.where(last_lane, e, turn(v, cz - 1)), jnp.where(first, e, turn(v, 1))

    def pack(acc, v, x):
        return jnp.where(lax.div(lane, SPAN) == x + 2, turn(v, lax.rem(SPAN * (x + 2) + 3 - gz, cz)), acc)

    def tile_of(k, x, m, r):
        return field[k, x + XO, m, pl.ds(YO + r, 8), :]

    def over_x(body, carry, unroll):
        def block(b, carry):
            for u in range(unroll):
                carry = body(b * unroll + u, carry)
            return carry

        return lax.fori_loop(0, cx // unroll, block, carry)

    def pack_all(read, write):
        def planes(x, acc):
            return tuple(pack(a, read(x, m, t), x) for a, (m, t) in zip(acc, order))

        order = [(m, t) for m in range(MODELS) for t in range(tiles)]
        for a, (m, t) in zip(over_x(planes, (zero,) * len(order), PACK), order):
            write(m, t, a)

    def pack_field(k):
        def write(m, t, v):
            z_own[k, m, pl.ds(YO + 8 * t, 8), :] = v

        pack_all(lambda x, m, t: tile_of(k, x, m, 8 * t), write)
        high, low = zero, zero
        for m in range(MODELS):
            for t in range(tiles):
                i = m * tiles + t
                v, mine = z_own[k, m, pl.ds(YO + 8 * t, 8), :], lax.div(lane, 16) == i
                high = jnp.where(mine, turn(v, 16 * i - SPAN * cx), high)
                low = jnp.where(mine, turn(v, 16 * i - 2 * SPAN), low)
        x_own[k, 0] = high
        x_own[k, 1] = low

    def join_z(k):
        low, high = [jnp.where(beyond_x, x_got[k, side, 1], turn(x_got[k, side, 0], to_own)) for side in range(2)]

        def inside(m, r):
            return jnp.where(beyond, z_got[k, m, pl.ds(r, 8), :], turn(z_own[k, m, pl.ds(r, 8), :], to_own))

        def with_x(v, before, after):
            return jnp.where(lane < 2 * SPAN, before, jnp.where(lane < SPAN * (cx + 2), v, after))

        for m in range(MODELS):
            for t in range(tiles):
                i = m * tiles + t
                z_field[min(k, 1), m, pl.ds(YO + 8 * t, 8), :] = with_x(
                    inside(m, YO + 8 * t), turn(low, -16 * i), turn(high, SPAN * (cx + 2) - 16 * i))
            for r, oy in ((0, 1), (YO + cy, -1)):
                before, after = [turn(jnp.broadcast_to(corner[k, corners.index((ox, oy, 1)), m, pl.ds(0, 1), :], (8, cz)),
                                      -ox * SPAN * cx) for ox in (1, -1)]
                z_field[min(k, 1), m, pl.ds(r, 8), :] = with_x(inside(m, r), before, after)

    def cross_part(a, b, i):
        j, l = (i + 1) % 3, (i + 2) % 3
        return a[j] * b[l] - a[l] * b[j]

    def flux_part(g1, g2, which):
        crossed = [None if i == which else cross_part(g1, g2, i) for i in range(3)]
        return [(cross_part(g2, crossed, i), cross_part(crossed, g1, i)) for i in (range(3) if which is None else [which])]

    for copy in loads[:MODELS]:
        copy.wait()
    pack_field(0)
    pl.semaphore_wait(barrier, expected)
    start_copies(0, through_z)
    start_copies(0, plain)
    tell(enter_sem.at[0], line_y)
    for copy in loads[MODELS:]:
        copy.wait()
    for a, array in enumerate((wgt, tgt)):
        def write(m, t, v, a=a):
            z_fixed[0, a, m, pl.ds(8 * t, 8), :] = v

        pack_all(lambda x, m, t, array=array: array[m, x, pl.ds(YO + 8 * t, 8), :], write)
    fixed = [fixed_message(j) for j in range(5)]
    for copy, sends, _ in fixed:
        guarded(sends, copy.start)
    wait_copies(0, through_z)
    join_z(0)
    wait_copies(0, plain)
    pl.semaphore_wait(enter_sem.at[0], len(line_y))
    tell(enter_sem.at[1], line_z)
    for copy, _, receives in fixed:
        guarded(receives, copy.wait_recv)

    for k in range(1, ITERS + 1):
        final = k == ITERS
        for j in range(wide):
            grads = []
            for m in range(MODELS):
                here = z_field[0, m, pl.ds(YO - 1 + 8 * j, 8), :]
                grads.append([turn(here, -SPAN) - turn(here, SPAN),
                              z_field[0, m, pl.ds(YO + 8 * j, 8), :] - z_field[0, m, pl.ds(YO - 2 + 8 * j, 8), :],
                              turn(here, -1) - turn(here, 1)])
            for i, parts in enumerate(flux_part(grads[0], grads[1], None)):
                for m in range(MODELS):
                    z_flux[i, m, pl.ds(YO - 1 + 8 * j, 8), :] = parts[m]

        for x in (-1, cx + 1):
            for j in range(wide):
                grads = []
                for m in range(MODELS):
                    here = tile_of(0, x, m, 8 * j - 1)
                    up, down = z_pair(here, edge(z_field[0, m, pl.ds(YO - 1 + 8 * j, 8), :], x))
                    grads.append([tile_of(0, x + 1, m, 8 * j - 1) - tile_of(0, x - 1, m, 8 * j - 1),
                                  tile_of(0, x, m, 8 * j) - tile_of(0, x, m, 8 * j - 2), up - down])
                parts = flux_part(grads[0], grads[1], 0)[0]
                for m in range(MODELS):
                    flux0[x + 1, m, pl.ds(YO - 1 + 8 * j, 8), :] = parts[m]

        def fluxes(x, carry):
            for j in range(wide):
                grads = []
                at = pl.ds(YO - 1 + 8 * j, 8)
                for m in range(MODELS):
                    here = tile_of(0, x, m, 8 * j - 1)
                    up, down = z_pair(here, edge(z_field[0, m, at, :], x))
                    xp, xm = tile_of(0, x + 1, m, 8 * j - 1), tile_of(0, x - 1, m, 8 * j - 1)
                    yp, ym = tile_of(0, x, m, 8 * j), tile_of(0, x, m, 8 * j - 2)
                    grads.append([xp - xm, yp - ym, up - down])
                    smooth = 6.0 * here - ((xp + xm) + (yp + ym) + (up + down))
                    base[m, x, at, :] = wgt[m, x, at, :] * (here - tgt[m, x, at, :]) + smooth
                parts = flux_part(grads[0], grads[1], None)
                for m in range(MODELS):
                    flux0[x + 1, m, at, :] = parts[0][m]
                    flux1[x, m, at, :] = parts[1][m]
                    flux2[x, m, at, :] = parts[2][m]
            return carry

        fluxes(cx, 0)
        over_x(fluxes, 0, FLUX)

        def no_plane(x):
            for m in range(MODELS):
                for r in range(0, rows, 8):
                    flux0[x + 1, m, pl.ds(r, 8), :] = zero

        def no_row(y):
            for x in range(cx + 1):
                for m in range(MODELS):
                    flux1[x, m, pl.ds(YO + y, 1), :] = zero[0:1]

        pl.when(gx == 0)(lambda: no_plane(-1))
        pl.when(gx == nx - 1)(lambda: no_plane(cx))
        pl.when(gy == 0)(lambda: no_row(-1))
        pl.when(gy == ny - 1)(lambda: no_row(cy))

        def gradient(x, m, r):
            at = pl.ds(YO + r, 8)
            here = flux2[x, m, at, :]
            up, down = z_pair(here, edge(z_flux[2, m, at, :], x))
            div = (flux0[x + 2, m, at, :] - flux0[x, m, at, :]
                   + (flux1[x, m, pl.ds(YO + r + 1, 8), :] - flux1[x, m, pl.ds(YO + r - 1, 8), :]) + (up - down))
            return base[m, x, at, :] + KAPPA * div

        def gradients(x, norm):
            for t in range(tiles):
                for m in range(MODELS):
                    grad = gradient(x, m, 8 * t)
                    field[k, x + XO, m, pl.ds(YO + 8 * t, 8), :] = grad
                    norm = norm + grad * grad
            for m in range(MODELS):
                grad = gradient(x, m, cy)[0:1]
                field[k, x + XO, m, pl.ds(YO + cy, 1), :] = jnp.where(gy < ny - 1, grad, 0.0)
            return norm

        norm = over_x(gradients, zero, GRADIENT)

        if final:
            start_copies(k, [0, 2], True)
        for t in range(tiles):
            for m in range(MODELS):
                field[k, cx + XO, m, pl.ds(YO + 8 * t, 8), :] = jnp.where(gx < nx - 1, gradient(cx, m, 8 * t), 0.0)
        for t in range(tiles):
            for m in range(MODELS):
                def shifted(ref, i, dy=0):
                    return ref[i, m, pl.ds(YO + 8 * t + dy, 8), :]

                here, f0, f2 = shifted(z_field, 0), shifted(z_flux, 0), shifted(z_flux, 2)
                div = (turn(f0, -SPAN) - turn(f0, SPAN) + (shifted(z_flux, 1, 1) - shifted(z_flux, 1, -1))
                       + (turn(f2, -1) - turn(f2, 1)))
                around = ((turn(here, -SPAN) + turn(here, SPAN)) + (shifted(z_field, 0, 1) + shifted(z_field, 0, -1))
                          + (turn(here, -1) + turn(here, 1)))
                misfit = z_fixed[1, 0, m, pl.ds(8 * t, 8), :] * (here - z_fixed[1, 1, m, pl.ds(8 * t, 8), :])
                z_grad[m, pl.ds(YO + 8 * t, 8), :] = misfit + (6.0 * here - around) + KAPPA * div

        inside_up = (gz == 0).astype(jnp.float32)

        def curves(x, curve):
            for t in range(tiles):
                for m in range(MODELS):
                    here = tile_of(k, x, m, 8 * t)
                    e = edge(z_grad[m, pl.ds(YO + 8 * t, 8), :], x) * inside_up
                    up = jnp.where(last_lane, e, turn(here, cz - 1))
                    pairs = tile_of(k, x + 1, m, 8 * t) + tile_of(k, x, m, 8 * t + 1) + up
                    curve = curve + here * ((wgt[m, x, pl.ds(YO + 8 * t, 8), :] + 6.0) * here - 2.0 * pairs)
            return curve

        curve = over_x(curves, zero, CURVE)

        def fold(v):
            v = jnp.sum(v, axis=0, keepdims=True)
            return v + turn(v, cz // 2)

        both = jnp.where(lane[0:1] < cz // 2, fold(norm), fold(curve))
        own[k - 1] = both
        got[k - 1, pl.ds(len(others), 1), :] = both
        if k == 1:
            pl.semaphore_wait(enter_sem.at[1], len(line_z))
        far_ones = len(others) * 2 // 3
        start_sum(k - 1, range(far_ones))
        if not final:
            start_copies(k, plain)
            pack_field(k)
            start_copies(k, through_z)
        start_sum(k - 1, range(far_ones, len(others)))
        if final:
            wait_copies(k, [0, 2], True)

            def applies(x, carry):
                for t in range(tiles):
                    for m in range(MODELS):
                        here = tile_of(k, x, m, 8 * t)
                        up, down = z_pair(here, edge(z_grad[m, pl.ds(YO + 8 * t, 8), :], x))
                        around = ((tile_of(k, x + 1, m, 8 * t) + tile_of(k, x - 1, m, 8 * t))
                                  + (tile_of(k, x, m, 8 * t + 1) + tile_of(k, x, m, 8 * t - 1)) + (up + down))
                        applied_out[m, x, pl.ds(8 * t, 8), :] = (
                            wgt[m, x, pl.ds(YO + 8 * t, 8), :] * here + (6.0 * here - around))
                return carry

            over_x(applies, 0, APPLY)
        else:
            wait_copies(k, through_z)
            join_z(k)
            wait_copies(k, plain)
        if k == 1:
            wait_sent(0, plain + through_z)
            for copy, sends, _ in fixed:
                guarded(sends, copy.wait_send)
        if final:
            wait_sent(k, [0, 2], True)
        else:
            wait_sent(k, plain + through_z)
        whole_sum(k - 1).wait_send()
        whole_sum(k - 1).wait_recv()
        partial = [got[k - 1, pl.ds(r, 8), :] for r in range(0, len(others) + 1, 8)]
        while len(partial) > 1:
            partial = [sum(partial[i:i + 2]) for i in range(0, len(partial), 2)]
        half = lane < cz // 2
        sums = [jnp.sum(jnp.sum(jnp.where(half, *terms), axis=0, keepdims=True), axis=1, keepdims=True)
                for terms in ((partial[0], 0.0), (0.0, partial[0]))]
        alpha = jnp.broadcast_to(sums[0] / sums[1], (8, cz))

        if final:
            def step(x, carry):
                for m in range(MODELS):
                    for t in range(tiles):
                        updated[m, x, pl.ds(8 * t, 8), :] = tile_of(0, x, m, 8 * t) - alpha * tile_of(k, x, m, 8 * t)
                return carry

            over_x(step, 0, STEP)
        else:
            def step(b, carry):
                for x in range(3):
                    for m in range(MODELS):
                        for r in range(0, rows, 8):
                            field[0, 3 * b + x, m, pl.ds(r, 8), :] = (
                                field[0, 3 * b + x, m, pl.ds(r, 8), :] - alpha * field[k, 3 * b + x, m, pl.ds(r, 8), :])
                return carry

            lax.fori_loop(0, (cx + LOW + HIGH) // 3, step, 0)
            for m in range(MODELS):
                for r in range(0, rows, 8):
                    z_field[0, m, pl.ds(r, 8), :] = z_field[0, m, pl.ds(r, 8), :] - alpha * z_field[1, m, pl.ds(r, 8), :]


def store(updated, applied, updated_out, applied_out, sems):
    copies = [pltpu.make_async_copy(updated, updated_out, sems.at[0]), pltpu.make_async_copy(applied, applied_out, sems.at[1])]
    for copy in copies:
        copy.start()
    for copy in copies:
        copy.wait()


def solution(mesh):
    sizes = (mesh.shape["gx"], mesh.shape["gy"], mesh.shape["gz"])
    nx, ny, nz = sizes

    def local(models, targets, weights):
        _, cx, cy, cz = models.shape
        assert nz == 2 and nx % 4 == 0 and cy % 8 == 0
        assert (cx + LOW + HIGH) % 3 == 0 and SPAN * (cx + 4) <= cz and 16 * MODELS * (cy // 8) <= cz
        f32 = jnp.float32
        rows = YO + cy + 8

        def vmem(*shape):
            return pltpu.VMEM(shape, f32)

        results = pl.pallas_call(
            functools.partial(kernel, sizes),
            out_shape=[jax.ShapeDtypeStruct(models.shape, f32)] * 2,
            in_specs=[pl.BlockSpec(memory_space=pltpu.HBM)] * 3,
            out_specs=[pl.BlockSpec(memory_space=pltpu.VMEM)] * 2,
            scratch_shapes=[
                vmem(ITERS + 1, cx + LOW + HIGH, MODELS, rows, cz),
                vmem(MODELS, cx + 1, rows, cz),
                vmem(MODELS, cx + 1, rows, cz),
                vmem(MODELS, cx + 1, rows, cz),
                vmem(cx + 3, MODELS, rows, cz),
                vmem(cx + 1, MODELS, rows + 8, cz),
                vmem(cx + 1, MODELS, rows, cz),
                vmem(ITERS + 1, MODELS, rows, cz),
                vmem(ITERS + 1, MODELS, rows, cz),
                vmem(2, MODELS, rows, cz),
                vmem(3, MODELS, rows, cz),
                vmem(MODELS, rows, cz),
                vmem(2, 2, MODELS, cy, cz),
                vmem(ITERS + 1, 2, 8, cz),
                vmem(ITERS + 1, 2, 2, 8, cz),
                vmem(ITERS + 1, 4, MODELS, 8, cz),
                vmem(ITERS, 1, cz),
                vmem(ITERS, nx * ny * nz, cz),
                pltpu.SemaphoreType.DMA((4,)),
                pltpu.SemaphoreType.DMA((ITERS + 1, 21)),
                pltpu.SemaphoreType.DMA((ITERS + 1, 21)),
                pltpu.SemaphoreType.DMA((5,)),
                pltpu.SemaphoreType.DMA((5,)),
                pltpu.SemaphoreType.DMA((ITERS,)),
                pltpu.SemaphoreType.DMA((ITERS,)),
                pltpu.SemaphoreType.REGULAR((2,)),
            ],
            compiler_params=pltpu.CompilerParams(
                collective_id=0, has_side_effects=True, vmem_limit_bytes=24 * 2**20),
        )(*[pltpu.with_memory_space_constraint(a, pltpu.HBM) for a in (models, targets, weights)])
        return pl.pallas_call(
            store,
            out_shape=[jax.ShapeDtypeStruct(models.shape, f32)] * 2,
            in_specs=[pl.BlockSpec(memory_space=pltpu.VMEM)] * 2,
            out_specs=[pl.BlockSpec(memory_space=pltpu.HBM)] * 2,
            scratch_shapes=[pltpu.SemaphoreType.DMA((2,))],
        )(*[pltpu.with_memory_space_constraint(a, pltpu.VMEM) for a in results])

    spec = P(None, "gx", "gy", "gz")
    return jax.shard_map(local, mesh=mesh, in_specs=(spec,) * 3, out_specs=(spec,) * 2, check_vma=False)
```

```python
import functools

import jax
import jax.numpy as jnp
from jax import lax
from jax.experimental import pallas as pl
from jax.experimental.pallas import tpu as pltpu
from jax.sharding import PartitionSpec as P

ITERS = 3
MESH = pl.DeviceIdType.MESH
MODELS = 2
XO = 2
YO = 8
LOW, HIGH = 2, 3
SPAN = 5
FLUX, GRADIENT, CURVE, PACK, APPLY, STEP = 4, 4, 16, 8, 4, 8
KAPPA = 0.05 * -2.0 * 0.5 * 0.125


def kernel(sizes, models, targets, weights, updated, applied_out,
           field, tgt, wgt, base, flux0, flux1, flux2, z_own, z_got, z_field, z_flux, z_grad, z_fixed,
           x_own, x_got, corner, own, got,
           load_sem, send_sem, recv_sem, fixed_send, fixed_recv, sum_send, sum_recv, enter_sem):
    nx, ny, nz = sizes
    _, cx, cy, cz = updated.shape
    tiles = cy // 8
    rows = field.shape[3]
    wide = tiles + 1
    gx, gy, gz = lax.axis_index("gx"), lax.axis_index("gy"), lax.axis_index("gz")

    faces = [(1, 0, 0), (-1, 0, 0), (0, 1, 0), (0, -1, 0), (1, 1, 0), (1, -1, 0), (-1, 1, 0), (-1, -1, 0)]
    z_faces = [(0, 0, 1), (1, 0, 0), (-1, 0, 0), (1, 0, 1), (-1, 0, 1), (0, 1, 0), (0, -1, 0), (0, 1, 1), (0, -1, 1),
               (1, 1, 1), (1, -1, 1), (-1, 1, 1), (-1, -1, 1)]
    corners = z_faces[9:]

    def there(ox, oy):
        ok = None
        for place, step, count in ((gx, ox, nx), (gy, oy, ny)):
            if step != 0:
                here = place < count - 1 if step > 0 else place > 0
                ok = here if ok is None else jnp.logical_and(ok, here)
        return ok

    def guarded(ok, action):
        if ok is None:
            action()
        else:
            pl.when(ok)(action)

    def device(ox, oy, oz):
        return {"gx": gx + ox, "gy": gy + oy, "gz": gz + oz - 2 * oz * gz}

    def slices(step, offset, count, skip, depth):
        if step > 0:
            return pl.ds(offset + count - LOW, LOW), pl.ds(offset - LOW, LOW)
        if step < 0:
            return pl.ds(offset + skip, depth - skip), pl.ds(offset + count + skip, depth - skip)
        return pl.ds(offset, count), pl.ds(offset, count)

    def message(k, j, last=False):
        if j < len(faces):
            ox, oy, oz = faces[j]
            if last:
                x_src, x_dst = (pl.ds(XO + cx - 1, 1), pl.ds(XO - 1, 1)) if ox else (pl.ds(XO, cx),) * 2
                y_src, y_dst = (pl.ds(YO + cy - 1, 1), pl.ds(YO - 1, 1)) if oy else (pl.ds(YO, cy),) * 2
            else:
                edge_of = ox != 0 and oy != 0
                skip, depth = (0, 2) if edge_of else (0 if k == 0 else 1, HIGH)
                x_src, x_dst = slices(ox, XO, cx, skip, depth)
                y_src, y_dst = slices(oy, YO, cy, skip, depth)
            src, dst = field.at[k, x_src, :, y_src, :], field.at[k, x_dst, :, y_dst, :]
        else:
            ox, oy, oz = offset = z_faces[j - len(faces)]
            y_src, y_dst = slices(oy, YO, cy, 0, 2)
            into = z_got if oz else z_own
            if ox and oy:
                line = YO + cy - 1 if oy > 0 else YO
                src, dst = z_own.at[k, :, pl.ds(line, 1), :], corner.at[k, corners.index(offset), :, pl.ds(0, 1), :]
            elif ox:
                src, dst = x_own.at[k, 0 if ox > 0 else 1], x_got.at[k, 0 if ox > 0 else 1, oz]
            else:
                src, dst = z_own.at[k, :, y_src, :], into.at[k, :, y_dst, :]
        return pltpu.make_async_remote_copy(
            src_ref=src, dst_ref=dst, send_sem=send_sem.at[k, j], recv_sem=recv_sem.at[k, j],
            device_id=device(ox, oy, oz), device_id_type=MESH)

    everything = faces + z_faces
    plain = list(range(len(faces)))
    through_z = list(range(len(faces), len(everything)))

    def start_copies(k, which, last=False):
        for j in which:
            guarded(there(*everything[j][:2]), lambda j=j: message(k, j, last).start())

    def wait_copies(k, which, last=False):
        for j in which:
            ox, oy, _ = everything[j]
            guarded(there(-ox, -oy), lambda j=j: message(k, j, last).wait_recv())

    def wait_sent(k, which, last=False):
        for j in which:
            guarded(there(*everything[j][:2]), lambda j=j: message(k, j, last).wait_send())

    def fixed_message(j):
        array = (wgt, tgt)[j % 2]
        if j < 2:
            ox, oy, oz = -1, 0, 0
            src, dst = array.at[:, pl.ds(0, 1), pl.ds(YO, cy), :], array.at[:, pl.ds(cx, 1), pl.ds(YO, cy), :]
        elif j < 4:
            ox, oy, oz = 0, -1, 0
            src, dst = array.at[:, pl.ds(0, cx), pl.ds(YO, 1), :], array.at[:, pl.ds(0, cx), pl.ds(YO + cy, 1), :]
        else:
            ox, oy, oz = 0, 0, 1
            src, dst = z_fixed.at[0], z_fixed.at[1]
        return pltpu.make_async_remote_copy(
            src_ref=src, dst_ref=dst, send_sem=fixed_send.at[j], recv_sem=fixed_recv.at[j],
            device_id=device(ox, oy, oz), device_id_type=MESH), there(ox, oy), there(-ox, -oy)

    pair, quad, chip_z = lax.rem(gx, 2), lax.rem(lax.div(gx, 2), 2), lax.div(gx, 4)
    turns_z = nx // 4

    def hops(offset):
        x, z, h, q, c = offset
        return min(x, ny - x) + min(z, turns_z - z) + (1 if q else 2 * h), c

    others = [(x, z, h, q, c) for x in range(ny) for z in range(turns_z) for h in range(nz) for q in range(2) for c in range(2)]
    others = sorted(others, key=hops, reverse=True)[:-1]
    place_x = [lax.rem(gy + x, ny) if x else gy for x in range(ny)]
    place_h = [gz, 1 - gz]
    place_gx = {(z, q, c): 4 * (lax.rem(chip_z + z, turns_z) if z else chip_z) + 2 * (1 - quad if q else quad) + (1 - pair if c else pair)
                for z in range(turns_z) for q in range(2) for c in range(2)}

    def start_sum(k, which):
        for j in which:
            x, z, h, q, c = others[j]
            pltpu.make_async_remote_copy(
                src_ref=own.at[k], dst_ref=got.at[k, pl.ds(j, 1)], send_sem=sum_send.at[k], recv_sem=sum_recv.at[k],
                device_id={"gx": place_gx[z, q, c], "gy": place_x[x], "gz": place_h[h]}, device_id_type=MESH).start()

    def whole_sum(k):
        landed = got.at[k, pl.ds(0, len(others))]
        return pltpu.make_async_remote_copy(
            src_ref=landed, dst_ref=landed, send_sem=sum_send.at[k], recv_sem=sum_recv.at[k],
            device_id={"gx": gx, "gy": gy, "gz": 1 - gz}, device_id_type=MESH)

    def on_line(x, y, z):
        return {"gx": x, "gy": y, "gz": z}

    line_x = [on_line(gx + c - 2 * c * pair, lax.rem(gy + s, ny), gz)
              for s in range(ny) for c in range(2) if (c, s) != (0, 0)]
    line_y = [on_line(gx + 2 * h - 4 * h * quad, gy, gz + s - 2 * s * gz)
              for s in range(nz) for h in range(2) if (h, s) != (0, 0)]
    line_z = [on_line(lax.rem(gx + 4 * s, nx), gy, gz) for s in range(1, nx // 4)]

    def tell(sem, line):
        for device in line:
            pl.semaphore_signal(sem, 1, device_id=device, device_id_type=MESH)

    inner = pl.ds(YO, cy)
    loads = [pltpu.make_async_copy(models.at[m], field.at[0, pl.ds(XO, cx), m, inner, :], load_sem.at[m]) for m in range(MODELS)]
    loads.append(pltpu.make_async_copy(targets, tgt.at[:, pl.ds(0, cx), inner, :], load_sem.at[2]))
    loads.append(pltpu.make_async_copy(weights, wgt.at[:, pl.ds(0, cx), inner, :], load_sem.at[3]))
    for copy in loads:
        copy.start()

    zero = jnp.zeros((8, cz), jnp.float32)

    def clear_planes(start, count, side):
        for k in range(ITERS + 1):
            for x in range(start, start + count):
                for m in range(MODELS):
                    for r in range(0, rows, 8):
                        field[k, x, m, pl.ds(r, 8), :] = zero
            for oz in range(2):
                x_got[k, side, oz] = zero

    def clear_rows(start):
        def clear(x, _):
            for k in range(ITERS + 1):
                for m in range(MODELS):
                    field[k, x, m, pl.ds(start, 8), :] = zero
            return 0

        lax.fori_loop(0, cx + LOW + HIGH, clear, 0)
        for k in range(ITERS + 1):
            for m in range(MODELS):
                z_own[k, m, pl.ds(start, 8), :] = zero
                z_got[k, m, pl.ds(start, 8), :] = zero

    def clear_corner(j):
        for k in range(ITERS + 1):
            for m in range(MODELS):
                corner[k, j, m] = zero

    for j, (ox, oy, _) in enumerate(corners):
        pl.when(jnp.logical_not(there(-ox, -oy)))(functools.partial(clear_corner, j))
    pl.when(gx == 0)(lambda: clear_planes(0, LOW, 0))
    pl.when(gx == nx - 1)(lambda: clear_planes(XO + cx, HIGH, 1))
    pl.when(gy == 0)(lambda: clear_rows(0))
    pl.when(gy == ny - 1)(lambda: clear_rows(rows - 8))

    barrier = pltpu.get_barrier_semaphore()
    expected = len(line_x) + len(line_y) + len(line_z)
    for ox, oy, oz in dict.fromkeys(everything):
        ok = there(ox, oy)
        guarded(ok, lambda ox=ox, oy=oy, oz=oz: pl.semaphore_signal(
            barrier, 1, device_id=device(ox, oy, oz), device_id_type=MESH))
        expected = expected + (1 if ok is None else ok.astype(jnp.int32))
    for line in (line_x, line_y, line_z):
        tell(barrier, line)

    lane = lax.broadcasted_iota(jnp.int32, (8, cz), 1)
    first, last_lane = lane == 0, lane == cz - 1
    end_lane = (1 - gz) * (cz - 1)
    ghost_lane = lane == end_lane
    upward = 1 - 2 * gz
    beyond = (lax.rem(lane, SPAN) - 2) * upward >= 0
    beyond_x = (lax.rem(lax.rem(lane, 16), SPAN) - 2) * upward >= 0
    to_own = jnp.where(gz == 0, cz - 1, 1)

    def turn(v, shift):
        if isinstance(shift, int):
            shift = shift % cz
            return v if shift == 0 else pltpu.roll(v, shift, 1)
        return pltpu.roll(v, shift, 1)

    def edge(lines, x):
        return jnp.where(ghost_lane, turn(lines, lax.rem(cz + end_lane - SPAN * (x + 2) - 2, cz)), 0.0)

    def z_pair(v, e):
        return jnp.where(last_lane, e, turn(v, cz - 1)), jnp.where(first, e, turn(v, 1))

    def pack(acc, v, x):
        return jnp.where(lax.div(lane, SPAN) == x + 2, turn(v, lax.rem(SPAN * (x + 2) + 3 - gz, cz)), acc)

    def tile_of(k, x, m, r):
        return field[k, x + XO, m, pl.ds(YO + r, 8), :]

    def over_x(body, carry, unroll):
        def block(b, carry):
            for u in range(unroll):
                carry = body(b * unroll + u, carry)
            return carry

        return lax.fori_loop(0, cx // unroll, block, carry)

    def pack_all(read, write):
        def planes(x, acc):
            return tuple(pack(a, read(x, m, t), x) for a, (m, t) in zip(acc, order))

        order = [(m, t) for m in range(MODELS) for t in range(tiles)]
        for a, (m, t) in zip(over_x(planes, (zero,) * len(order), PACK), order):
            write(m, t, a)

    def pack_field(k):
        def write(m, t, v):
            z_own[k, m, pl.ds(YO + 8 * t, 8), :] = v

        pack_all(lambda x, m, t: tile_of(k, x, m, 8 * t), write)
        high, low = zero, zero
        for m in range(MODELS):
            for t in range(tiles):
                i = m * tiles + t
                v, mine = z_own[k, m, pl.ds(YO + 8 * t, 8), :], lax.div(lane, 16) == i
                high = jnp.where(mine, turn(v, 16 * i - SPAN * cx), high)
                low = jnp.where(mine, turn(v, 16 * i - 2 * SPAN), low)
        x_own[k, 0] = high
        x_own[k, 1] = low

    def join_z(k):
        low, high = [jnp.where(beyond_x, x_got[k, side, 1], turn(x_got[k, side, 0], to_own)) for side in range(2)]

        def inside(m, r):
            return jnp.where(beyond, z_got[k, m, pl.ds(r, 8), :], turn(z_own[k, m, pl.ds(r, 8), :], to_own))

        def with_x(v, before, after):
            return jnp.where(lane < 2 * SPAN, before, jnp.where(lane < SPAN * (cx + 2), v, after))

        for m in range(MODELS):
            for t in range(tiles):
                i = m * tiles + t
                z_field[min(k, 1), m, pl.ds(YO + 8 * t, 8), :] = with_x(
                    inside(m, YO + 8 * t), turn(low, -16 * i), turn(high, SPAN * (cx + 2) - 16 * i))
            for r, oy in ((0, 1), (YO + cy, -1)):
                before, after = [turn(jnp.broadcast_to(corner[k, corners.index((ox, oy, 1)), m, pl.ds(0, 1), :], (8, cz)),
                                      -ox * SPAN * cx) for ox in (1, -1)]
                z_field[min(k, 1), m, pl.ds(r, 8), :] = with_x(inside(m, r), before, after)

    def cross_part(a, b, i):
        j, l = (i + 1) % 3, (i + 2) % 3
        return a[j] * b[l] - a[l] * b[j]

    def flux_part(g1, g2, which):
        crossed = [None if i == which else cross_part(g1, g2, i) for i in range(3)]
        return [(cross_part(g2, crossed, i), cross_part(crossed, g1, i)) for i in (range(3) if which is None else [which])]

    for copy in loads[:MODELS]:
        copy.wait()
    pack_field(0)
    pl.semaphore_wait(barrier, expected)
    start_copies(0, through_z)
    start_copies(0, plain)
    tell(enter_sem.at[0], line_y)
    for copy in loads[MODELS:]:
        copy.wait()
    for a, array in enumerate((wgt, tgt)):
        def write(m, t, v, a=a):
            z_fixed[0, a, m, pl.ds(8 * t, 8), :] = v

        pack_all(lambda x, m, t, array=array: array[m, x, pl.ds(YO + 8 * t, 8), :], write)
    fixed = [fixed_message(j) for j in range(5)]
    for copy, sends, _ in fixed:
        guarded(sends, copy.start)
    wait_copies(0, through_z)
    join_z(0)
    wait_copies(0, plain)
    pl.semaphore_wait(enter_sem.at[0], len(line_y))
    tell(enter_sem.at[1], line_z)
    for copy, _, receives in fixed:
        guarded(receives, copy.wait_recv)

    for k in range(1, ITERS + 1):
        final = k == ITERS
        for j in range(wide):
            grads = []
            for m in range(MODELS):
                here = z_field[0, m, pl.ds(YO - 1 + 8 * j, 8), :]
                grads.append([turn(here, -SPAN) - turn(here, SPAN),
                              z_field[0, m, pl.ds(YO + 8 * j, 8), :] - z_field[0, m, pl.ds(YO - 2 + 8 * j, 8), :],
                              turn(here, -1) - turn(here, 1)])
            for i, parts in enumerate(flux_part(grads[0], grads[1], None)):
                for m in range(MODELS):
                    z_flux[i, m, pl.ds(YO - 1 + 8 * j, 8), :] = parts[m]

        for x in (-1, cx + 1):
            for j in range(wide):
                grads = []
                for m in range(MODELS):
                    here = tile_of(0, x, m, 8 * j - 1)
                    up, down = z_pair(here, edge(z_field[0, m, pl.ds(YO - 1 + 8 * j, 8), :], x))
                    grads.append([tile_of(0, x + 1, m, 8 * j - 1) - tile_of(0, x - 1, m, 8 * j - 1),
                                  tile_of(0, x, m, 8 * j) - tile_of(0, x, m, 8 * j - 2), up - down])
                parts = flux_part(grads[0], grads[1], 0)[0]
                for m in range(MODELS):
                    flux0[x + 1, m, pl.ds(YO - 1 + 8 * j, 8), :] = parts[m]

        def fluxes(x, carry):
            for j in range(wide):
                grads = []
                at = pl.ds(YO - 1 + 8 * j, 8)
                for m in range(MODELS):
                    here = tile_of(0, x, m, 8 * j - 1)
                    up, down = z_pair(here, edge(z_field[0, m, at, :], x))
                    xp, xm = tile_of(0, x + 1, m, 8 * j - 1), tile_of(0, x - 1, m, 8 * j - 1)
                    yp, ym = tile_of(0, x, m, 8 * j), tile_of(0, x, m, 8 * j - 2)
                    grads.append([xp - xm, yp - ym, up - down])
                    smooth = 6.0 * here - ((xp + xm) + (yp + ym) + (up + down))
                    base[m, x, at, :] = wgt[m, x, at, :] * (here - tgt[m, x, at, :]) + smooth
                parts = flux_part(grads[0], grads[1], None)
                for m in range(MODELS):
                    flux0[x + 1, m, at, :] = parts[0][m]
                    flux1[x, m, at, :] = parts[1][m]
                    flux2[x, m, at, :] = parts[2][m]
            return carry

        fluxes(cx, 0)
        over_x(fluxes, 0, FLUX)

        def no_plane(x):
            for m in range(MODELS):
                for r in range(0, rows, 8):
                    flux0[x + 1, m, pl.ds(r, 8), :] = zero

        def no_row(y):
            for x in range(cx + 1):
                for m in range(MODELS):
                    flux1[x, m, pl.ds(YO + y, 1), :] = zero[0:1]

        pl.when(gx == 0)(lambda: no_plane(-1))
        pl.when(gx == nx - 1)(lambda: no_plane(cx))
        pl.when(gy == 0)(lambda: no_row(-1))
        pl.when(gy == ny - 1)(lambda: no_row(cy))

        def gradient(x, m, r):
            at = pl.ds(YO + r, 8)
            here = flux2[x, m, at, :]
            up, down = z_pair(here, edge(z_flux[2, m, at, :], x))
            div = (flux0[x + 2, m, at, :] - flux0[x, m, at, :]
                   + (flux1[x, m, pl.ds(YO + r + 1, 8), :] - flux1[x, m, pl.ds(YO + r - 1, 8), :]) + (up - down))
            return base[m, x, at, :] + KAPPA * div

        def gradients(x, norm):
            for t in range(tiles):
                for m in range(MODELS):
                    grad = gradient(x, m, 8 * t)
                    field[k, x + XO, m, pl.ds(YO + 8 * t, 8), :] = grad
                    norm = norm + grad * grad
            for m in range(MODELS):
                grad = gradient(x, m, cy)[0:1]
                field[k, x + XO, m, pl.ds(YO + cy, 1), :] = jnp.where(gy < ny - 1, grad, 0.0)
            return norm

        norm = over_x(gradients, zero, GRADIENT)

        if final:
            start_copies(k, [0, 2], True)
        for t in range(tiles):
            for m in range(MODELS):
                field[k, cx + XO, m, pl.ds(YO + 8 * t, 8), :] = jnp.where(gx < nx - 1, gradient(cx, m, 8 * t), 0.0)
        for t in range(tiles):
            for m in range(MODELS):
                def shifted(ref, i, dy=0):
                    return ref[i, m, pl.ds(YO + 8 * t + dy, 8), :]

                here, f0, f2 = shifted(z_field, 0), shifted(z_flux, 0), shifted(z_flux, 2)
                div = (turn(f0, -SPAN) - turn(f0, SPAN) + (shifted(z_flux, 1, 1) - shifted(z_flux, 1, -1))
                       + (turn(f2, -1) - turn(f2, 1)))
                around = ((turn(here, -SPAN) + turn(here, SPAN)) + (shifted(z_field, 0, 1) + shifted(z_field, 0, -1))
                          + (turn(here, -1) + turn(here, 1)))
                misfit = z_fixed[1, 0, m, pl.ds(8 * t, 8), :] * (here - z_fixed[1, 1, m, pl.ds(8 * t, 8), :])
                z_grad[m, pl.ds(YO + 8 * t, 8), :] = misfit + (6.0 * here - around) + KAPPA * div

        inside_up = (gz == 0).astype(jnp.float32)

        def curves(x, curve):
            for t in range(tiles):
                for m in range(MODELS):
                    here = tile_of(k, x, m, 8 * t)
                    e = edge(z_grad[m, pl.ds(YO + 8 * t, 8), :], x) * inside_up
                    up = jnp.where(last_lane, e, turn(here, cz - 1))
                    pairs = tile_of(k, x + 1, m, 8 * t) + tile_of(k, x, m, 8 * t + 1) + up
                    curve = curve + here * ((wgt[m, x, pl.ds(YO + 8 * t, 8), :] + 6.0) * here - 2.0 * pairs)
            return curve

        curve = over_x(curves, zero, CURVE)

        def fold(v):
            v = jnp.sum(v, axis=0, keepdims=True)
            return v + turn(v, cz // 2)

        both = jnp.where(lane[0:1] < cz // 2, fold(norm), fold(curve))
        own[k - 1] = both
        got[k - 1, pl.ds(len(others), 1), :] = both
        if k == 1:
            pl.semaphore_wait(enter_sem.at[1], len(line_z))
        far_ones = len(others) * 2 // 3
        start_sum(k - 1, range(far_ones))
        if not final:
            start_copies(k, plain)
            pack_field(k)
            start_copies(k, through_z)
        start_sum(k - 1, range(far_ones, len(others)))
        if final:
            wait_copies(k, [0, 2], True)

            def applies(x, carry):
                for t in range(tiles):
                    for m in range(MODELS):
                        here = tile_of(k, x, m, 8 * t)
                        up, down = z_pair(here, edge(z_grad[m, pl.ds(YO + 8 * t, 8), :], x))
                        around = ((tile_of(k, x + 1, m, 8 * t) + tile_of(k, x - 1, m, 8 * t))
                                  + (tile_of(k, x, m, 8 * t + 1) + tile_of(k, x, m, 8 * t - 1)) + (up + down))
                        applied_out[m, x, pl.ds(8 * t, 8), :] = (
                            wgt[m, x, pl.ds(YO + 8 * t, 8), :] * here + (6.0 * here - around))
                return carry

            over_x(applies, 0, APPLY)
        else:
            wait_copies(k, through_z)
            join_z(k)
            wait_copies(k, plain)
        if k == 1:
            wait_sent(0, plain + through_z)
            for copy, sends, _ in fixed:
                guarded(sends, copy.wait_send)
        if final:
            wait_sent(k, [0, 2], True)
        else:
            wait_sent(k, plain + through_z)
        whole_sum(k - 1).wait_send()
        whole_sum(k - 1).wait_recv()
        partial = [got[k - 1, pl.ds(r, 8), :] for r in range(0, len(others) + 1, 8)]
        while len(partial) > 1:
            partial = [sum(partial[i:i + 2]) for i in range(0, len(partial), 2)]
        half = lane < cz // 2
        sums = [jnp.sum(jnp.sum(jnp.where(half, *terms), axis=0, keepdims=True), axis=1, keepdims=True)
                for terms in ((partial[0], 0.0), (0.0, partial[0]))]
        alpha = jnp.broadcast_to(sums[0] / sums[1], (8, cz))

        if final:
            def step(x, carry):
                for m in range(MODELS):
                    for t in range(tiles):
                        updated[m, x, pl.ds(8 * t, 8), :] = tile_of(0, x, m, 8 * t) - alpha * tile_of(k, x, m, 8 * t)
                return carry

            over_x(step, 0, STEP)
        else:
            def step(b, carry):
                for x in range(3):
                    for m in range(MODELS):
                        for r in range(0, rows, 8):
                            field[0, 3 * b + x, m, pl.ds(r, 8), :] = (
                                field[0, 3 * b + x, m, pl.ds(r, 8), :] - alpha * field[k, 3 * b + x, m, pl.ds(r, 8), :])
                return carry

            lax.fori_loop(0, (cx + LOW + HIGH) // 3, step, 0)
            for m in range(MODELS):
                for r in range(0, rows, 8):
                    z_field[0, m, pl.ds(r, 8), :] = z_field[0, m, pl.ds(r, 8), :] - alpha * z_field[1, m, pl.ds(r, 8), :]


def store(updated, applied, updated_out, applied_out, sems):
    copies = [pltpu.make_async_copy(updated, updated_out, sems.at[0]), pltpu.make_async_copy(applied, applied_out, sems.at[1])]
    for copy in copies:
        copy.start()
    for copy in copies:
        copy.wait()


def solution(mesh):
    sizes = (mesh.shape["gx"], mesh.shape["gy"], mesh.shape["gz"])
    nx, ny, nz = sizes

    def local(models, targets, weights):
        _, cx, cy, cz = models.shape
        assert nz == 2 and nx % 4 == 0 and cy % 8 == 0
        assert (cx + LOW + HIGH) % 3 == 0 and SPAN * (cx + 4) <= cz and 16 * MODELS * (cy // 8) <= cz
        f32 = jnp.float32
        rows = YO + cy + 8

        def vmem(*shape):
            return pltpu.VMEM(shape, f32)

        results = pl.pallas_call(
            functools.partial(kernel, sizes),
            out_shape=[jax.ShapeDtypeStruct(models.shape, f32)] * 2,
            in_specs=[pl.BlockSpec(memory_space=pltpu.HBM)] * 3,
            out_specs=[pl.BlockSpec(memory_space=pltpu.VMEM)] * 2,
            scratch_shapes=[
                vmem(ITERS + 1, cx + LOW + HIGH, MODELS, rows, cz),
                vmem(MODELS, cx + 1, rows, cz),
                vmem(MODELS, cx + 1, rows, cz),
                vmem(MODELS, cx + 1, rows, cz),
                vmem(cx + 3, MODELS, rows, cz),
                vmem(cx + 1, MODELS, rows + 8, cz),
                vmem(cx + 1, MODELS, rows, cz),
                vmem(ITERS + 1, MODELS, rows, cz),
                vmem(ITERS + 1, MODELS, rows, cz),
                vmem(2, MODELS, rows, cz),
                vmem(3, MODELS, rows, cz),
                vmem(MODELS, rows, cz),
                vmem(2, 2, MODELS, cy, cz),
                vmem(ITERS + 1, 2, 8, cz),
                vmem(ITERS + 1, 2, 2, 8, cz),
                vmem(ITERS + 1, 4, MODELS, 8, cz),
                vmem(ITERS, 1, cz),
                vmem(ITERS, nx * ny * nz, cz),
                pltpu.SemaphoreType.DMA((4,)),
                pltpu.SemaphoreType.DMA((ITERS + 1, 21)),
                pltpu.SemaphoreType.DMA((ITERS + 1, 21)),
                pltpu.SemaphoreType.DMA((5,)),
                pltpu.SemaphoreType.DMA((5,)),
                pltpu.SemaphoreType.DMA((ITERS,)),
                pltpu.SemaphoreType.DMA((ITERS,)),
                pltpu.SemaphoreType.REGULAR((2,)),
            ],
            compiler_params=pltpu.CompilerParams(
                collective_id=0, has_side_effects=True, vmem_limit_bytes=24 * 2**20),
        )(*[pltpu.with_memory_space_constraint(a, pltpu.HBM) for a in (models, targets, weights)])
        return pl.pallas_call(
            store,
            out_shape=[jax.ShapeDtypeStruct(models.shape, f32)] * 2,
            in_specs=[pl.BlockSpec(memory_space=pltpu.VMEM)] * 2,
            out_specs=[pl.BlockSpec(memory_space=pltpu.HBM)] * 2,
            scratch_shapes=[pltpu.SemaphoreType.DMA((2,))],
        )(*[pltpu.with_memory_space_constraint(a, pltpu.VMEM) for a in results])

    spec = P(None, "gx", "gy", "gz")
    return jax.shard_map(local, mesh=mesh, in_specs=(spec,) * 3, out_specs=(spec,) * 2, check_vma=False)
```
